128 devices in a mesh: group: 8 (over x, core), dev: 16 (over y, z).
Axes of the slice: x: 4, y: 4, z: 4, core: 2. Of those that a mesh axis runs over, the one named last changes fastest.
Arguments:
- images: bfloat16 [16384, 1152], P(('group', 'dev')), may hold values from -1 to 1
- texts: bfloat16 [16384, 1152], P(('group', 'dev')), may hold values from -1 to 1
- lang_order: int32 [16384], P(('group', 'dev')), may hold values from 0 to 2047, as said below
- position: int32 [16384], P(('group', 'dev')), may hold values from 0 to 2047, as said below
- logit_scale: float32 [1], replicated, may hold values from 8 to 24
- logit_bias: float32 [1], replicated, may hold values from -4 to -1
Outputs:
- image_grad: float32 [16384, 1152], P(('group', 'dev'))
- text_grad: float32 [16384, 1152], P(('group', 'dev'))
- loss: float32 [1], replicated
The draws below stay inside these ranges and needn't reach their ends.
Inputs may be any that keep to these rules, and one draw needn't show every extreme that they name: In each group of 2048 examples, lang_order is a permutation of the group-local indices; the 128 entries of one device name at most 16 examples held by any one device of the group, and exactly 16 for each device they name. position is the inverse of lang_order within each group.
All inputs are finite; a program needn't handle non-finite values.
Results may differ from the reference program's by a relative error of at most 0.00062.
Values may be sent and summed in bfloat16 or wider, within the bound.
A program may use at most 64 MiB of HBM per device.

```python
import math
import jax
import jax.numpy as jnp
from jax import lax

D = 1152
ROWS = 128
N_GROUP = 8
N_DEV = 16


def lang_maps(key):
    group_count = N_GROUP
    dev_count = N_DEV
    row_count = ROWS
    slot_depth = ROWS // 8
    per_source = row_count // slot_depth
    key_list = jax.random.split(jax.random.fold_in(key, 7), 4)
    shifts = jax.vmap(lambda subkey: jax.random.permutation(subkey, dev_count)[:per_source])(jax.random.split(key_list[0], group_count))
    relabel = jax.vmap(lambda subkey: jax.random.permutation(subkey, dev_count))(jax.random.split(key_list[1], group_count))
    within = jax.vmap(lambda subkey: jax.random.permutation(subkey, per_source))(jax.random.split(key_list[2], group_count * dev_count)).reshape(group_count, dev_count, per_source)
    scramble = jax.vmap(lambda subkey: jax.random.permutation(subkey, row_count))(jax.random.split(key_list[3], group_count * dev_count)).reshape(group_count, dev_count, row_count)
    span = dev_count * row_count
    place_ids = jnp.arange(span, dtype=jnp.int32)
    source = place_ids // row_count
    which = place_ids % row_count // slot_depth
    offset = place_ids % slot_depth
    group_ids = jnp.arange(group_count, dtype=jnp.int32)[:, None]
    pick = within[group_ids, source[None, :], which[None, :]]
    target_dev = (relabel[group_ids, source[None, :]] + jnp.take_along_axis(shifts, pick, axis=1)) % dev_count
    local = scramble[group_ids, target_dev, pick * slot_depth + offset[None, :]]
    ordering = (target_dev * row_count + local).astype(jnp.int32)
    inverse = jnp.zeros_like(ordering).at[group_ids, ordering].set(jnp.broadcast_to(place_ids[None, :], (group_count, span)))
    return (ordering.reshape(-1).astype(jnp.int32), inverse.reshape(-1).astype(jnp.int32))


def embed_parts(key):
    total = N_GROUP * N_DEV * ROWS
    mix_count = 8
    key_list = jax.random.split(jax.random.fold_in(key, 11), 7)
    root = jnp.float32(D) ** (-0.5)
    directions = jax.random.normal(key_list[0], (mix_count, D), jnp.float32) * root
    weights = jax.random.normal(key_list[1], (total, mix_count), jnp.float32) * jnp.float32(mix_count) ** (-0.5)
    cluster = jnp.dot(weights, directions, precision=jax.lax.Precision.HIGHEST)
    shared = jax.random.normal(key_list[2], (total, D), jnp.float32) * root
    img_noise = jax.random.normal(key_list[3], (total, D), jnp.float32) * root
    txt_noise = jax.random.normal(key_list[4], (total, D), jnp.float32) * root
    img_scale = jnp.exp(jax.random.uniform(key_list[5], (total, 1), jnp.float32, -0.6931472, 0.6931472))
    txt_scale = jnp.exp(jax.random.uniform(key_list[6], (total, 1), jnp.float32, -0.6931472, 0.6931472))
    cluster_weight = 0.63
    image_rows = (cluster_weight * cluster + 0.5 * shared + 0.6 * img_noise) * img_scale
    text_rows = (cluster_weight * cluster + 0.5 * shared + 0.6 * txt_noise) * txt_scale
    return (jnp.clip(image_rows, -1.0, 1.0), jnp.clip(text_rows, -1.0, 1.0))


def draw_lang_order(key, part):
    return lang_maps(key)[0]


def draw_position(key, part):
    return lang_maps(key)[1]


def draw_images(key, part):
    return embed_parts(key)[0].astype(jnp.bfloat16)


def draw_texts(key, part):
    total = N_GROUP * N_DEV * ROWS
    span = N_DEV * ROWS
    ordering = lang_maps(key)[0]
    text_rows = embed_parts(key)[1]
    starts = jnp.arange(total, dtype=jnp.int32) // span * span
    return text_rows[starts + ordering].astype(jnp.bfloat16)


def setup_inputs(seed: int = 0) -> dict:
    key_of = jax.random.split(jax.random.key(seed), 7)
    images = draw_images(jax.random.fold_in(key_of[6], 71), 0)
    texts = draw_texts(jax.random.fold_in(key_of[6], 71), 0)
    lang_order = draw_lang_order(jax.random.fold_in(key_of[6], 71), 0)
    position = draw_position(jax.random.fold_in(key_of[6], 71), 0)
    logit_scale = jnp.clip(jnp.exp(jax.random.uniform(key_of[4], (1,), jnp.float32, math.log(8.0), math.log(24.0))), 8.0, 24.0)
    logit_bias = jnp.clip(jax.random.uniform(key_of[5], (1,), jnp.float32, -4.0, -1.0), -4.0, -1.0)
    return dict(images=images, texts=texts, lang_order=lang_order, position=position, logit_scale=logit_scale, logit_bias=logit_bias)


EPSILON = 1e-06

def normalize(values):
    wide = values.astype(jnp.float32)
    recip = lax.rsqrt(lax.optimization_barrier(jnp.sum(wide * wide, axis=1, keepdims=True)) + EPSILON)
    return (wide * recip, recip)

def project_back(unit, recip, grad):
    return recip * (grad - unit * lax.optimization_barrier(jnp.sum(unit * grad, axis=1, keepdims=True)))

def reference(images, texts, lang_order, position, logit_scale, logit_bias):
    span = ROWS * N_DEV
    total = span * N_GROUP
    img_unit, img_recip = normalize(images)
    txt_unit, txt_recip = normalize(texts)
    img_half = img_unit.astype(jnp.bfloat16).astype(jnp.float32)
    txt_half = txt_unit.astype(jnp.bfloat16)
    starts = jnp.arange(total, dtype=jnp.int32) // span * span
    batch_text = txt_half[starts + position.astype(jnp.int32)].astype(jnp.float32)
    scale = logit_scale[0]
    bias = logit_bias[0]
    column_ids = jnp.arange(total, dtype=jnp.int32)

    def block(carry, block_index):
        dtext, loss_sum = carry
        rows_here = lax.dynamic_slice_in_dim(img_half, (block_index * span).astype(jnp.int32), span, 0)
        logits = scale * jnp.dot(rows_here, batch_text.T, precision=lax.Precision.HIGHEST, preferred_element_type=jnp.float32) + bias
        row_ids = block_index * span + jnp.arange(span, dtype=jnp.int32)
        sign = jnp.where(row_ids[:, None] == column_ids[None, :], jnp.float32(1.0), jnp.float32(-1.0))
        loss_sum = loss_sum + jnp.sum(-jax.nn.log_sigmoid(sign * logits))
        coeff = lax.optimization_barrier((-sign * jax.nn.sigmoid(-sign * logits)).astype(jnp.bfloat16))
        coeff = coeff.astype(jnp.float32)
        dimg_block = jnp.dot(coeff, batch_text, precision=lax.Precision.HIGHEST, preferred_element_type=jnp.float32)
        dtext = dtext + jnp.dot(coeff.T, rows_here, precision=lax.Precision.HIGHEST, preferred_element_type=jnp.float32)
        return ((dtext, loss_sum), dimg_block)
    init = (jnp.zeros((total, D), jnp.float32), jnp.zeros((), jnp.float32))
    (dtext, loss_sum), dimg_blocks = lax.scan(block, init, jnp.arange(N_GROUP, dtype=jnp.int32))
    dimg = scale * dimg_blocks.reshape(total, D)
    dtext = scale * dtext
    dtext_lang = dtext[starts + lang_order.astype(jnp.int32)]
    image_grad = project_back(img_unit, img_recip, dimg)
    text_grad = project_back(txt_unit, txt_recip, dtext_lang)
    loss = (loss_sum / (jnp.float32(total) * jnp.float32(total))).reshape(1)
    return (image_grad, text_grad, loss)
```

```python
import jax
import jax.numpy as jnp
from jax import lax
from jax.sharding import Mesh
from jax.sharding import PartitionSpec as P

DEV = ("dev_0", "dev_1")
GROUP = ("group_0", "group_1")
GROUP_DEV = ("group_0", "group_1", "dev_0", "dev_1")


EPSILON = 1e-06


def normalize(values):
    wide = values.astype(jnp.float32)
    recip = lax.rsqrt(jnp.sum(wide * wide, axis=1, keepdims=True) + EPSILON)
    return (wide * recip, recip)


def project_back(unit, recip, grad):
    return recip * (grad - unit * jnp.sum(unit * grad, axis=1, keepdims=True))


def per_device(images, texts, lang_order, position, logit_scale, logit_bias):
    row_count, width_count = images.shape
    dev_count = lax.axis_size(DEV)
    group_count = lax.axis_size(GROUP)
    scale = logit_scale[0]
    bias = logit_bias[0]
    span = row_count * dev_count
    group_index = lax.axis_index(GROUP)
    img_unit, img_recip = normalize(images)
    txt_unit, txt_recip = normalize(texts)
    img_block = lax.all_gather(img_unit.astype(jnp.bfloat16), DEV, axis=0, tiled=True)
    txt_block = lax.all_gather(txt_unit.astype(jnp.bfloat16), GROUP, axis=0, tiled=True)
    txt_ids = lax.all_gather(group_index * span + lang_order, GROUP, axis=0, tiled=True)
    img_ids = group_index * span + jnp.arange(span, dtype=jnp.int32)
    logits = (
        scale
        * lax.dot_general(
            img_block, txt_block, (((1,), (1,)), ((), ())), preferred_element_type=jnp.float32
        )
        + bias
    )
    sign = jnp.where(img_ids[:, None] == txt_ids[None, :], jnp.float32(1.0), jnp.float32(-1.0))
    loss_part = jnp.sum(-jax.nn.log_sigmoid(sign * logits))
    coeff = (-sign * jax.nn.sigmoid(-sign * logits)).astype(jnp.bfloat16)
    dimg_part = jnp.dot(coeff, txt_block, preferred_element_type=jnp.float32)
    dtext_part = lax.dot_general(
        coeff, img_block, (((0,), (0,)), ((), ())), preferred_element_type=jnp.float32
    )
    dimg = scale * lax.psum_scatter(dimg_part, DEV, scatter_dimension=0, tiled=True)
    dtext = scale * lax.psum_scatter(dtext_part, GROUP, scatter_dimension=0, tiled=True)
    total = jnp.float32(span * group_count)
    loss = (lax.psum(loss_part, GROUP_DEV) / (total * total)).reshape(1)
    return (
        project_back(img_unit, img_recip, dimg),
        project_back(txt_unit, txt_recip, dtext),
        loss,
    )


def solution(mesh):
    finer = Mesh(mesh.devices.reshape(4, 2, 4, 4), GROUP_DEV)
    return jax.shard_map(
        per_device,
        mesh=finer,
        in_specs=(P(GROUP_DEV, None), P(GROUP_DEV, None), P(GROUP_DEV), P(GROUP_DEV), P(), P()),
        out_specs=(P(GROUP_DEV, None), P(GROUP_DEV, None), P()),
        check_vma=False,
    )
```

```python
import jax
import jax.numpy as jnp
from jax import lax
from jax.experimental import pallas as pl
from jax.experimental.pallas import tpu as pltpu
from jax.sharding import Mesh
from jax.sharding import PartitionSpec as P

AXES = ("x", "core", "y", "z")
MESH = pl.DeviceIdType.MESH
EPSILON = 1e-06
ROWS = 128
BF16 = jnp.bfloat16
F32 = jnp.float32

PLACES = ((0, 0), (0, 1), (1, 0), (3, 0), (1, 1), (3, 1), (2, 0), (2, 1))
AT = {place: index for index, place in enumerate(PLACES)}
N_PLACE = len(PLACES)

GATHER = ("z", "plus_own", "minus_own", "plus_par", "minus_par", "plus_far", "minus_far")
REDUCE = ("far_plus", "far_minus", "near_plus", "near_minus", "relay_plus", "relay_minus", "z")
FLOWS = {}
for kind in ("img", "txt", "ids"):
    for name in GATHER:
        FLOWS[kind, name] = len(FLOWS)
for kind in ("dimg", "dimg_s", "dtxt", "dtxt_s"):
    for name in REDUCE:
        FLOWS[kind, name] = len(FLOWS)
for place in range(N_PLACE):
    FLOWS["share", place] = len(FLOWS)
for place in range(N_PLACE):
    FLOWS["swap", place] = len(FLOWS)
FLOWS["loss_core"] = len(FLOWS)
for axis in ("x", "y", "z"):
    for step in (1, 2, 3):
        FLOWS["loss", axis, step] = len(FLOWS)
N_FLOW = len(FLOWS)


def normalize(values):
    wide = values.astype(F32)
    recip = lax.rsqrt(jnp.sum(wide * wide, axis=1, keepdims=True) + EPSILON)
    return (wide * recip, recip)


def project_back(unit, recip, grad):
    return recip * (grad - unit * jnp.sum(unit * grad, axis=1, keepdims=True))


def kernel(
    img_in, txt_in, ids_in, scale_ref, bias_ref,
    img_out, txt_out, loss_out,
    img, txt, ids, dimg, swap, dtxt, coeff, sent, sent_s, got, got_s, loss_tile, loss_got,
    send_sem, recv_sem,
):
    x, core = lax.axis_index("x"), lax.axis_index("core")
    y, z = lax.axis_index("y"), lax.axis_index("z")
    other = {"core": 1 - core}
    z_img = z + 1 - 2 * lax.rem(z, 2)
    z_txt = 3 - z
    plus = {"img": {"x": lax.rem(x + 1, 4)}, "txt": {"y": lax.rem(y + 1, 4)}}
    minus = {"img": {"x": lax.rem(x + 3, 4)}, "txt": {"y": lax.rem(y + 3, 4)}}
    across = {"img": {"z": z_img}, "txt": {"z": z_txt}}

    started = []

    def copy(flow, src, dst, device):
        return pltpu.make_async_remote_copy(
            src_ref=src, dst_ref=dst, send_sem=send_sem.at[flow], recv_sem=recv_sem.at[flow],
            device_id=device, device_id_type=MESH,
        )

    barrier = pltpu.get_barrier_semaphore()
    peers = [other]
    for axis, here in (("x", x), ("y", y), ("z", z)):
        for step in (1, 2, 3):
            peers.append({axis: lax.rem(here + step, 4)})
    for peer in peers:
        pl.semaphore_signal(barrier, inc=1, device_id=peer, device_id_type=MESH)

    def img_rows(place, which):
        return pl.ds((2 * place + which) * ROWS, ROWS)

    def rows(place):
        return pl.ds(place * ROWS, ROWS)

    img[img_rows(0, 0), :] = normalize(img_in[...])[0].astype(BF16)
    txt[rows(0), :] = normalize(txt_in[...])[0].astype(BF16)
    ids[0] = ids_in[...]
    scale = scale_ref[0]
    bias = bias_ref[0]
    dtxt[...] = jnp.zeros_like(dtxt)
    loss_tile[0] = jnp.zeros_like(loss_tile[0])
    pl.semaphore_wait(barrier, len(peers))

    def block(kind, place):
        if kind == "img":
            return img.at[img_rows(place, 0), :]
        if kind == "txt":
            return txt.at[rows(place), :]
        return ids.at[place]

    def gather(kind, name):
        ring = "img" if kind == "img" else "txt"
        src, dst, device = {
            "z": ((0, 0), (0, 1), across[ring]),
            "plus_own": ((0, 0), (3, 0), plus[ring]),
            "minus_own": ((0, 0), (1, 0), minus[ring]),
            "plus_par": ((0, 1), (3, 1), plus[ring]),
            "minus_par": ((0, 1), (1, 1), minus[ring]),
            "plus_far": ((3, 0), (2, 0), plus[ring]),
            "minus_far": ((1, 1), (2, 1), minus[ring]),
        }[name]
        return copy(FLOWS[kind, name], block(kind, AT[src]), block(kind, AT[dst]), device)

    def share(place):
        return copy(
            FLOWS["share", place], img.at[img_rows(place, 0), :], img.at[img_rows(place, 1), :], other
        )

    def go(kind, name):
        descriptor = gather(kind, name)
        descriptor.start()
        started.append(descriptor)
        if kind == "txt":
            go("ids", name)

    def give(place):
        descriptor = share(AT[place])
        descriptor.start()
        started.append(descriptor)

    def come(kind, name):
        gather(kind, name).wait_recv()
        if kind == "txt":
            come("ids", name)

    for name in ("z", "plus_own", "minus_own"):
        go("img", name)
        go("txt", name)
    give((0, 0))
    come("img", "z")
    go("img", "plus_par")
    go("img", "minus_par")
    give((0, 1))
    come("txt", "z")
    go("txt", "plus_par")
    go("txt", "minus_par")
    come("img", "plus_own")
    go("img", "plus_far")
    give((3, 0))
    come("txt", "plus_own")
    go("txt", "plus_far")
    come("img", "minus_own")
    give((1, 0))
    come("txt", "minus_own")
    come("img", "minus_par")
    go("img", "minus_far")
    give((1, 1))
    come("txt", "minus_par")
    go("txt", "minus_far")
    come("img", "plus_par")
    give((3, 1))
    come("txt", "plus_par")
    come("img", "plus_far")
    give((2, 0))
    come("img", "minus_far")
    give((2, 1))
    come("txt", "plus_far")
    come("txt", "minus_far")
    for place in range(N_PLACE):
        share(place).wait_recv()

    row_iota = lax.broadcasted_iota(jnp.int32, (2 * ROWS, 1), 0)

    def give_back(place):
        flow = FLOWS["swap", 0] + place
        return copy(flow, dimg.at[img_rows(place, 1), :], swap.at[rows(place), :], other)

    def step(index, carry):
        place = N_PLACE - 1 - index
        start = pl.multiple_of(place * (2 * ROWS), 2 * ROWS)
        here = img[pl.ds(start, 2 * ROWS), :]
        owner = jnp.where(place == 0, y * 4 + z, y * 4 + z_img) * ROWS
        valid = jnp.logical_and(place < 2, row_iota < ROWS)
        row_ids = jnp.where(valid, owner + row_iota, -1)
        total = jnp.zeros((8, 128), F32)
        for part in range(4):
            columns = pl.ds(part * 256, 256)
            there = txt[columns, :]
            logits = scale * lax.dot_general(
                here, there, (((1,), (1,)), ((), ())), preferred_element_type=F32
            ) + bias
            column_ids = jnp.concatenate([ids[2 * part, 0:1, :], ids[2 * part + 1, 0:1, :]], axis=1)
            same = row_ids == column_ids
            logits = jnp.where(same, -logits, logits)
            small = jnp.exp(-jnp.abs(logits))
            one_plus = 1.0 + small
            recip = 1.0 / one_plus
            sigmoid = jnp.where(logits >= 0, recip, small * recip)
            log1p = jnp.where(
                small < 0.01,
                small * (1.0 - small * (0.5 - small * (1.0 / 3.0))),
                jnp.log(one_plus),
            )
            softplus = jnp.maximum(logits, 0.0) + log1p
            folded = jnp.sum(softplus.reshape(32, 8, 256), axis=0)
            total = total + folded[:, :128] + folded[:, 128:]
            half = jnp.where(same, -sigmoid, sigmoid).astype(BF16)
            coeff[:, columns] = half
            dtxt[columns, :] += lax.dot_general(
                half, here, (((0,), (0,)), ((), ())), preferred_element_type=F32
            )
        dimg[pl.ds(start, 2 * ROWS), :] = jnp.dot(coeff[...], txt[...], preferred_element_type=F32)
        loss_tile[0] += total
        give_back(place).start()
        return carry

    lax.fori_loop(0, N_PLACE, step, 0)

    eye = lax.broadcasted_iota(jnp.int32, (ROWS, ROWS), 0) == lax.broadcasted_iota(
        jnp.int32, (ROWS, ROWS), 1
    )

    def slot(kind, name):
        return REDUCE.index(name) + (0 if kind == "dimg" else len(REDUCE))

    def sum_ref(kind, place):
        if kind == "dimg":
            return dimg.at[img_rows(AT[place], 0), :]
        return dtxt.at[rows(AT[place]), :]

    def route(kind, name):
        ring = "img" if kind == "dimg" else "txt"
        if name == "z":
            return across[ring]
        return plus[ring] if name.endswith("plus") else minus[ring]

    def two(kind, name):
        s = slot(kind, name)
        device = route(kind, name)
        return (
            copy(FLOWS[kind, name], sent.at[s], got.at[s], device),
            copy(FLOWS[kind + "_s", name], sent_s.at[s], got_s.at[s], device),
        )

    def send(kind, name, place):
        ref = sum_ref(kind, place)
        s = slot(kind, name)
        top = jnp.maximum(jnp.max(jnp.abs(ref[...]), axis=1, keepdims=True), 1e-30)
        across_lanes = jnp.sum(jnp.where(eye, top * (1.0 / 32767.0), 0.0), axis=0, keepdims=True)
        sent_s[s] = jnp.broadcast_to(across_lanes, (8, ROWS))
        sent[s] = jnp.round(ref[...] * (32767.0 / top)).astype(jnp.int32).astype(jnp.int16)
        for descriptor in two(kind, name):
            descriptor.start()
            started.append(descriptor)

    def take(kind, name):
        s = slot(kind, name)
        for descriptor in two(kind, name):
            descriptor.wait_recv()
        unit = jnp.sum(jnp.where(eye, got_s[s, 0:1, :], 0.0), axis=1, keepdims=True)
        return got[s].astype(jnp.int32).astype(F32) * unit

    def merge(place):
        give_back(AT[place]).wait_recv()
        dimg[img_rows(AT[place], 0), :] += swap[rows(AT[place]), :]

    for place in ((2, 0), (2, 1), (1, 1), (3, 0), (1, 0), (3, 1), (0, 0), (0, 1)):
        merge(place)
    for name, place in (
        ("far_plus", (2, 0)), ("far_minus", (2, 1)), ("near_plus", (1, 1)), ("near_minus", (3, 0)),
    ):
        for kind in ("dtxt", "dimg"):
            send(kind, name, place)

    loss_copies = []

    def loss_over(axis, here, number):
        loss_got[number, here] = loss_tile[number]
        for stride in (1, 2, 3):
            descriptor = copy(
                FLOWS["loss", axis, stride], loss_tile.at[number], loss_got.at[number, here],
                {axis: lax.rem(here + stride, 4)},
            )
            descriptor.start()
            started.append(descriptor)
        for stride in (1, 2, 3):
            source = lax.rem(here + 4 - stride, 4)
            copy(
                FLOWS["loss", axis, stride], loss_tile.at[number], loss_got.at[number, source],
                {axis: lax.rem(here + stride, 4)},
            ).wait_recv()
        loss_tile[number + 1] = (loss_got[number, 0] + loss_got[number, 1]) + (
            loss_got[number, 2] + loss_got[number, 3]
        )

    descriptor = copy(FLOWS["loss_core"], loss_tile.at[0], loss_got.at[0, 0], other)
    descriptor.start()
    started.append(descriptor)
    descriptor.wait_recv()
    loss_tile[1] = loss_tile[0] + loss_got[0, 0]
    loss_over("x", x, 1)
    loss_over("y", y, 2)
    loss_over("z", z, 3)
    count = F32(ROWS * 128)
    loss_out[0] = jnp.sum(loss_tile[4]) / (count * count)

    for kind in ("dtxt", "dimg"):
        sum_ref(kind, (3, 1))[...] += take(kind, "far_minus")
        send(kind, "relay_minus", (3, 1))
        sum_ref(kind, (1, 0))[...] += take(kind, "far_plus")
        send(kind, "relay_plus", (1, 0))
    for kind in ("dtxt", "dimg"):
        ref = sum_ref(kind, (0, 1))
        ref[...] += take(kind, "near_plus")
        ref[...] += take(kind, "relay_minus")
        send(kind, "z", (0, 1))
    for kind in ("dtxt", "dimg"):
        ref = sum_ref(kind, (0, 0))
        ref[...] += take(kind, "near_minus")
        ref[...] += take(kind, "relay_plus")
    for kind, source, out in (("dtxt", txt_in, txt_out), ("dimg", img_in, img_out)):
        ref = sum_ref(kind, (0, 0))
        ref[...] = scale * (ref[...] + take(kind, "z"))
        unit, recip = normalize(source[...])
        out[...] = project_back(unit, recip, ref[...])

    for descriptor in started:
        descriptor.wait_send()
    for place in range(N_PLACE):
        give_back(place).wait_send()


def per_device(images, texts, lang_order, position, logit_scale, logit_bias):
    rows, width = images.shape
    ids = jnp.broadcast_to(lang_order[None, :], (8, rows))
    vmem = pl.BlockSpec(memory_space=pltpu.VMEM)
    smem = pl.BlockSpec(memory_space=pltpu.SMEM)
    return pl.pallas_call(
        kernel,
        out_shape=(
            jax.ShapeDtypeStruct((rows, width), F32),
            jax.ShapeDtypeStruct((rows, width), F32),
            jax.ShapeDtypeStruct((1,), F32),
        ),
        in_specs=[vmem, vmem, vmem, smem, smem],
        out_specs=(vmem, vmem, smem),
        scratch_shapes=[
            pltpu.VMEM((16 * rows, width), BF16),
            pltpu.VMEM((8 * rows, width), BF16),
            pltpu.VMEM((8, 8, rows), jnp.int32),
            pltpu.VMEM((16 * rows, width), F32),
            pltpu.VMEM((8 * rows, width), F32),
            pltpu.VMEM((8 * rows, width), F32),
            pltpu.VMEM((2 * rows, 8 * rows), BF16),
            pltpu.VMEM((14, rows, width), jnp.int16),
            pltpu.VMEM((14, 8, rows), F32),
            pltpu.VMEM((14, rows, width), jnp.int16),
            pltpu.VMEM((14, 8, rows), F32),
            pltpu.VMEM((5, 8, 128), F32),
            pltpu.VMEM((4, 4, 8, 128), F32),
            pltpu.SemaphoreType.DMA((N_FLOW,)),
            pltpu.SemaphoreType.DMA((N_FLOW,)),
        ],
        compiler_params=pltpu.CompilerParams(
            collective_id=0, has_side_effects=True, vmem_limit_bytes=62 * 1024 * 1024
        ),
        name="pair_grads",
    )(images, texts, ids, logit_scale, logit_bias)


def solution(mesh):
    finer = Mesh(mesh.devices.reshape(4, 2, 4, 4), AXES)
    return jax.shard_map(
        per_device,
        mesh=finer,
        in_specs=(P(AXES, None), P(AXES, None), P(AXES), P(AXES), P(), P()),
        out_specs=(P(AXES, None), P(AXES, None), P()),
        check_vma=False,
    )
```

```python
import jax
import jax.numpy as jnp
from jax import lax
from jax.experimental import pallas as pl
from jax.experimental.pallas import tpu as pltpu
from jax.sharding import Mesh
from jax.sharding import PartitionSpec as P

AXES = ("x", "core", "y", "z")
MESH = pl.DeviceIdType.MESH
EPSILON = 1e-06
ROWS = 128
BF16 = jnp.bfloat16
F32 = jnp.float32

PLACES = ((0, 0), (0, 1), (1, 0), (3, 0), (1, 1), (3, 1), (2, 0), (2, 1))
AT = {place: index for index, place in enumerate(PLACES)}
N_PLACE = len(PLACES)

HALVES = (0, 1)
HALF = ROWS // 2
GATHER = ("z", "plus_own", "minus_own", "plus_par", "minus_par", "plus_far", "minus_far")
REDUCE = ("far_plus", "far_minus", "near_plus", "near_minus", "relay_plus", "relay_minus", "z")
FLOWS = {}
for name in GATHER:
    FLOWS["ids", name] = len(FLOWS)
    for part in HALVES:
        for kind in ("img", "txt"):
            FLOWS[kind, name, part] = len(FLOWS)
for kind in ("dimg", "dimg_s", "dtxt", "dtxt_s"):
    for name in REDUCE:
        for part in HALVES:
            FLOWS[kind, name, part] = len(FLOWS)
for place in range(N_PLACE):
    FLOWS["share", place] = len(FLOWS)
for place in range(N_PLACE):
    FLOWS["swap", place] = len(FLOWS)
FLOWS["loss_core"] = len(FLOWS)
for axis in ("x", "y", "z"):
    for step in (1, 2, 3):
        FLOWS["loss", axis, step] = len(FLOWS)
N_FLOW = len(FLOWS)


def normalize(values):
    wide = values.astype(F32)
    recip = lax.rsqrt(jnp.sum(wide * wide, axis=1, keepdims=True) + EPSILON)
    return (wide * recip, recip)


def project_back(unit, recip, grad):
    return recip * (grad - unit * jnp.sum(unit * grad, axis=1, keepdims=True))


def tile_at(index):
    table = (
        (8, 4, lambda k: 7 - k // 4, lambda k: 3 - k % 4),
        (14, 1, lambda k: 5 - k, lambda k: 3),
        (20, 3, lambda k: 5 - k // 3, lambda k: 2 - k % 3),
        (24, 1, lambda k: 3 - k, lambda k: 2),
        (32, 2, lambda k: 3 - k // 2, lambda k: 1 - k % 2),
    )
    first = 0
    pair, group = jnp.int32(0), jnp.int32(0)
    for last, _, pair_of, group_of in table:
        inside = jnp.logical_and(index >= first, index < last)
        pair = jnp.where(inside, pair_of(index - first), pair)
        group = jnp.where(inside, group_of(index - first), group)
        first = last
    return pair, group


def kernel(
    img_in, txt_in, ids_in, scale_ref, bias_ref,
    img_out, txt_out, loss_out,
    img_raw, txt_raw, ids_raw,
    img, txt, ids, dimg, swap, dtxt, coeff, sent, sent_s, got, got_s, loss_tile, loss_got,
    load_sem, send_sem, recv_sem,
):
    x, core = lax.axis_index("x"), lax.axis_index("core")
    y, z = lax.axis_index("y"), lax.axis_index("z")
    other = {"core": 1 - core}
    z_img = z + 1 - 2 * lax.rem(z, 2)
    z_txt = 3 - z
    plus = {"img": {"x": lax.rem(x + 1, 4)}, "txt": {"y": lax.rem(y + 1, 4)}}
    minus = {"img": {"x": lax.rem(x + 3, 4)}, "txt": {"y": lax.rem(y + 3, 4)}}
    across = {"img": {"z": z_img}, "txt": {"z": z_txt}}

    loads = [
        pltpu.make_async_copy(src, dst, load_sem.at[number])
        for number, (src, dst) in enumerate(
            ((img_in, img_raw), (txt_in, txt_raw), (ids_in, ids_raw))
        )
    ]
    for load in loads:
        load.start()

    started = []

    def copy(flow, src, dst, device):
        return pltpu.make_async_remote_copy(
            src_ref=src, dst_ref=dst, send_sem=send_sem.at[flow], recv_sem=recv_sem.at[flow],
            device_id=device, device_id_type=MESH,
        )

    def launch(make):
        make().start()
        started.append(make)

    barrier = pltpu.get_barrier_semaphore()
    peers = [other]
    for axis, here in (("x", x), ("y", y), ("z", z)):
        for step in (1, 2, 3):
            peers.append({axis: lax.rem(here + step, 4)})
    for peer in peers:
        pl.semaphore_signal(barrier, inc=1, device_id=peer, device_id_type=MESH)

    def img_rows(place, which):
        return pl.ds((2 * place + which) * ROWS, ROWS)

    def rows(place):
        return pl.ds(place * ROWS, ROWS)

    for load in loads:
        load.wait()
    img[img_rows(0, 0), :] = normalize(img_raw[...])[0].astype(BF16)
    txt[rows(0), :] = normalize(txt_raw[...])[0].astype(BF16)
    ids[0] = jnp.broadcast_to(ids_raw[...], (8, ROWS))
    scale = scale_ref[0]
    bias = bias_ref[0]
    pl.semaphore_wait(barrier, len(peers))

    def gather(kind, name, part):
        ring = "img" if kind == "img" else "txt"
        src, dst, device = {
            "z": ((0, 0), (0, 1), across[ring]),
            "plus_own": ((0, 0), (3, 0), plus[ring]),
            "minus_own": ((0, 0), (1, 0), minus[ring]),
            "plus_par": ((0, 1), (3, 1), plus[ring]),
            "minus_par": ((0, 1), (1, 1), minus[ring]),
            "plus_far": ((3, 0), (2, 0), plus[ring]),
            "minus_far": ((1, 1), (2, 1), minus[ring]),
        }[name]
        src, dst = AT[src], AT[dst]
        if kind == "ids":
            return copy(FLOWS[kind, name], ids.at[src], ids.at[dst], device)
        ref, every = (img, 2) if kind == "img" else (txt, 1)
        return copy(
            FLOWS[kind, name, part],
            ref.at[pl.ds(src * every * ROWS + part * HALF, HALF), :],
            ref.at[pl.ds(dst * every * ROWS + part * HALF, HALF), :],
            device,
        )

    def share(place):
        return copy(
            FLOWS["share", place], img.at[img_rows(place, 0), :], img.at[img_rows(place, 1), :], other
        )

    def go(kind, name, part):
        launch(lambda: gather(kind, name, part))
        if kind == "txt" and part == 1:
            launch(lambda: gather("ids", name, 0))

    def give(place):
        launch(lambda: share(AT[place]))

    def come(kind, name, part):
        gather(kind, name, part).wait_recv()
        if kind == "txt" and part == 1:
            gather("ids", name, 0).wait_recv()

    for part in HALVES:
        for name in ("z", "plus_own", "minus_own"):
            go("img", name, part)
            go("txt", name, part)
    give((0, 0))
    dimg[...] = jnp.zeros_like(dimg)
    dtxt[...] = jnp.zeros_like(dtxt)
    loss_tile[0] = jnp.zeros_like(loss_tile[0])
    for part in HALVES:
        for kind in ("img", "txt"):
            come(kind, "z", part)
            go(kind, "plus_par", part)
            go(kind, "minus_par", part)
        for kind in ("img", "txt"):
            come(kind, "plus_own", part)
            go(kind, "plus_far", part)
    give((0, 1))
    give((3, 0))
    for part in HALVES:
        come("img", "minus_own", part)
        come("txt", "minus_own", part)
    give((1, 0))
    for part in HALVES:
        for kind in ("img", "txt"):
            come(kind, "minus_par", part)
            go(kind, "minus_far", part)
    give((1, 1))
    for part in HALVES:
        come("img", "plus_par", part)
        come("txt", "plus_par", part)
    give((3, 1))
    for name, place in (("plus_far", (2, 0)), ("minus_far", (2, 1))):
        for part in HALVES:
            come("img", name, part)
        give(place)
    for name in ("plus_far", "minus_far"):
        for part in HALVES:
            come("txt", name, part)
    for place in range(N_PLACE):
        share(place).wait_recv()

    eye = lax.broadcasted_iota(jnp.int32, (HALF, ROWS), 0) == lax.broadcasted_iota(
        jnp.int32, (HALF, ROWS), 1
    )

    def give_back(place):
        return copy(
            FLOWS["swap", place], dimg.at[img_rows(place, 1), :], swap.at[rows(place), :], other
        )

    def slot(kind, name, part):
        number = REDUCE.index(name) + (0 if kind == "dimg" else len(REDUCE))
        return number * 2 + part

    def sum_ref(kind, place, part):
        if kind == "dimg":
            return dimg.at[pl.ds(AT[place] * 2 * ROWS + part * HALF, HALF), :]
        return dtxt.at[pl.ds(AT[place] * ROWS + part * HALF, HALF), :]

    def route(kind, name):
        ring = "img" if kind == "dimg" else "txt"
        if name == "z":
            return across[ring]
        return plus[ring] if name.endswith("plus") else minus[ring]

    def values(kind, name, part):
        s = slot(kind, name, part)
        return copy(FLOWS[kind, name, part], sent.at[s], got.at[s], route(kind, name))

    def units(kind, name, part):
        s = slot(kind, name, part)
        return copy(FLOWS[kind + "_s", name, part], sent_s.at[s], got_s.at[s], route(kind, name))

    def send(kind, name, place, part):
        ref = sum_ref(kind, place, part)
        s = slot(kind, name, part)
        top = jnp.maximum(jnp.max(jnp.abs(ref[...]), axis=1, keepdims=True), 1e-30)
        across_lanes = jnp.sum(jnp.where(eye, top * (1.0 / 32767.0), 0.0), axis=0, keepdims=True)
        sent_s[s] = jnp.broadcast_to(across_lanes, (8, ROWS))
        sent[s] = jnp.round(ref[...] * (32767.0 / top)).astype(jnp.int32).astype(jnp.int16)
        launch(lambda: values(kind, name, part))
        launch(lambda: units(kind, name, part))

    def take(kind, name, part):
        s = slot(kind, name, part)
        values(kind, name, part).wait_recv()
        units(kind, name, part).wait_recv()
        unit = jnp.sum(jnp.where(eye, got_s[s, 0:1, :], 0.0), axis=1, keepdims=True)
        return got[s].astype(jnp.int32).astype(F32) * unit

    def add(kind, name, place, part):
        sum_ref(kind, place, part)[...] += take(kind, name, part)

    def merge(place):
        give_back(AT[place]).wait_recv()
        dimg[img_rows(AT[place], 0), :] += swap[rows(AT[place]), :]

    def relay(kind, way, place):
        for part in HALVES:
            add(kind, "far_" + way, place, part)
            send(kind, "relay_" + way, place, part)

    def send_all(kind, name, place):
        for part in HALVES:
            send(kind, name, place, part)

    row_iota = lax.broadcasted_iota(jnp.int32, (2 * ROWS, 1), 0)

    def spans(index):
        pair, group = tile_at(index)
        return (
            pair,
            pl.ds(pl.multiple_of(pair * (2 * ROWS), 2 * ROWS), 2 * ROWS),
            group,
            pl.ds(pl.multiple_of(group * (2 * ROWS), 2 * ROWS), 2 * ROWS),
        )

    def make_coeff(index):
        pair, here, group, there = spans(index)
        logits = scale * lax.dot_general(
            img[here, :], txt[there, :], (((1,), (1,)), ((), ())), preferred_element_type=F32
        ) + bias
        owner = jnp.where(pair == 0, y * 4 + z, y * 4 + z_img) * ROWS
        valid = jnp.logical_and(pair < 2, row_iota < ROWS)
        row_ids = jnp.where(valid, owner + row_iota, -1)
        column_ids = jnp.concatenate(
            [ids[2 * group, 0:1, :], ids[2 * group + 1, 0:1, :]], axis=1
        )
        same = row_ids == column_ids
        logits = jnp.where(same, -logits, logits)
        small = jnp.exp(-jnp.abs(logits))
        one_plus = 1.0 + small
        recip = 1.0 / one_plus
        sigmoid = jnp.where(logits >= 0, recip, small * recip)
        log1p = jnp.where(
            small < 0.01,
            small * (1.0 - small * (0.5 - small * (1.0 / 3.0))),
            jnp.log(one_plus),
        )
        softplus = jnp.maximum(logits, 0.0) + log1p
        folded = jnp.sum(softplus.reshape(32, 8, 256), axis=0)
        loss_tile[0] += folded[:, :128] + folded[:, 128:]
        coeff[lax.rem(index, 2)] = jnp.where(same, -sigmoid, sigmoid).astype(BF16)

    def use_coeff(index):
        _, here, _, there = spans(index)
        half = coeff[lax.rem(index, 2)]
        dimg[here, :] += jnp.dot(half, txt[there, :], preferred_element_type=F32)
        dtxt[there, :] += lax.dot_general(
            half, img[here, :], (((0,), (0,)), ((), ())), preferred_element_type=F32
        )

    def pass_back(place):
        launch(lambda: give_back(place))

    def far_dimg():
        merge((2, 1))
        send_all("dimg", "far_minus", (2, 1))
        merge((2, 0))
        send_all("dimg", "far_plus", (2, 0))

    def far_dtxt():
        send_all("dtxt", "far_minus", (2, 1))
        send_all("dtxt", "far_plus", (2, 0))

    def near_dimg():
        merge((1, 1))
        merge((3, 1))
        send_all("dimg", "near_plus", (1, 1))

    events = {
        3: lambda: pass_back(7),
        7: lambda: pass_back(6),
        10: far_dimg,
        13: far_dtxt,
        16: lambda: pass_back(5),
        19: lambda: pass_back(4),
        21: near_dimg,
        23: lambda: send_all("dtxt", "near_plus", (1, 1)),
        25: lambda: pass_back(3),
        27: lambda: pass_back(2),
        28: lambda: relay("dimg", "minus", (3, 1)),
        29: lambda: pass_back(1),
    }

    make_coeff(jnp.int32(0))

    def step(index, carry):
        make_coeff(index + 1)
        use_coeff(index)
        for moment, event in events.items():
            pl.when(index == moment)(event)
        return carry

    lax.fori_loop(0, 31, step, 0)
    use_coeff(jnp.int32(31))
    pass_back(0)

    def loss_send(axis, here, number):
        loss_got[number, here] = loss_tile[number]
        for stride in (1, 2, 3):
            launch(
                lambda stride=stride: copy(
                    FLOWS["loss", axis, stride], loss_tile.at[number], loss_got.at[number, here],
                    {axis: lax.rem(here + stride, 4)},
                )
            )

    def loss_take(axis, here, number):
        for stride in (1, 2, 3):
            source = lax.rem(here + 4 - stride, 4)
            copy(
                FLOWS["loss", axis, stride], loss_tile.at[number], loss_got.at[number, source],
                {axis: lax.rem(here + stride, 4)},
            ).wait_recv()
        loss_tile[number + 1] = (loss_got[number, 0] + loss_got[number, 1]) + (
            loss_got[number, 2] + loss_got[number, 3]
        )

    def loss_swap():
        return copy(FLOWS["loss_core"], loss_tile.at[0], loss_got.at[0, 0], other)

    launch(loss_swap)
    merge((3, 0))
    send_all("dimg", "near_minus", (3, 0))
    relay("dtxt", "minus", (3, 1))
    loss_swap().wait_recv()
    loss_tile[1] = loss_tile[0] + loss_got[0, 0]
    loss_send("x", x, 1)
    merge((1, 0))
    relay("dimg", "plus", (1, 0))
    relay("dtxt", "plus", (1, 0))
    send_all("dtxt", "near_minus", (3, 0))
    merge((0, 1))
    merge((0, 0))
    loss_take("x", x, 1)
    loss_send("y", y, 2)
    for kind in ("dimg", "dtxt"):
        for part in HALVES:
            add(kind, "near_plus", (0, 1), part)
    for kind in ("dimg", "dtxt"):
        for part in HALVES:
            add(kind, "relay_minus", (0, 1), part)
            send(kind, "z", (0, 1), part)
    loss_take("y", y, 2)
    loss_send("z", z, 3)
    for name in ("near_minus", "relay_plus"):
        for kind in ("dimg", "dtxt"):
            for part in HALVES:
                add(kind, name, (0, 0), part)
    loss_take("z", z, 3)
    count = F32(ROWS * 128)
    loss_out[0] = jnp.sum(loss_tile[4]) / (count * count)
    for kind, source, out in (("dimg", img_raw, img_out), ("dtxt", txt_raw, txt_out)):
        for part in HALVES:
            ref = sum_ref(kind, (0, 0), part)
            piece = pl.ds(part * HALF, HALF)
            ref[...] = scale * (ref[...] + take(kind, "z", part))
            unit, recip = normalize(source[piece, :])
            out[piece, :] = project_back(unit, recip, ref[...])

    for make in started:
        make().wait_send()


def per_device(images, texts, lang_order, position, logit_scale, logit_bias):
    rows, width = images.shape
    ids = lang_order.reshape(1, rows)
    whole = pl.BlockSpec(memory_space=pl.ANY)
    vmem = pl.BlockSpec(memory_space=pltpu.VMEM)
    smem = pl.BlockSpec(memory_space=pltpu.SMEM)
    return pl.pallas_call(
        kernel,
        out_shape=(
            jax.ShapeDtypeStruct((rows, width), F32),
            jax.ShapeDtypeStruct((rows, width), F32),
            jax.ShapeDtypeStruct((1,), F32),
        ),
        in_specs=[whole, whole, whole, smem, smem],
        out_specs=(vmem, vmem, smem),
        scratch_shapes=[
            pltpu.VMEM((rows, width), BF16),
            pltpu.VMEM((rows, width), BF16),
            pltpu.VMEM((1, rows), jnp.int32),
            pltpu.VMEM((16 * rows, width), BF16),
            pltpu.VMEM((8 * rows, width), BF16),
            pltpu.VMEM((8, 8, rows), jnp.int32),
            pltpu.VMEM((16 * rows, width), F32),
            pltpu.VMEM((8 * rows, width), F32),
            pltpu.VMEM((8 * rows, width), F32),
            pltpu.VMEM((2, 2 * rows, 2 * rows), BF16),
            pltpu.VMEM((28, HALF, width), jnp.int16),
            pltpu.VMEM((28, 8, rows), F32),
            pltpu.VMEM((28, HALF, width), jnp.int16),
            pltpu.VMEM((28, 8, rows), F32),
            pltpu.VMEM((5, 8, 128), F32),
            pltpu.VMEM((4, 4, 8, 128), F32),
            pltpu.SemaphoreType.DMA((3,)),
            pltpu.SemaphoreType.DMA((N_FLOW,)),
            pltpu.SemaphoreType.DMA((N_FLOW,)),
        ],
        compiler_params=pltpu.CompilerParams(
            collective_id=0, has_side_effects=True, vmem_limit_bytes=62 * 1024 * 1024
        ),
        name="pair_grads",
    )(images, texts, ids, logit_scale, logit_bias)


def solution(mesh):
    finer = Mesh(mesh.devices.reshape(4, 2, 4, 4), AXES)
    return jax.shard_map(
        per_device,
        mesh=finer,
        in_specs=(P(AXES, None), P(AXES, None), P(AXES), P(AXES), P(), P()),
        out_specs=(P(AXES, None), P(AXES, None), P()),
        check_vma=False,
    )
```

```python
import jax
import jax.numpy as jnp
from jax import lax
from jax.experimental import pallas as pl
from jax.experimental.pallas import tpu as pltpu
from jax.sharding import Mesh
from jax.sharding import PartitionSpec as P

AXES = ("x", "core", "y", "z")
MESH = pl.DeviceIdType.MESH
EPSILON = 1e-06
ROWS = 128
BF16 = jnp.bfloat16
F32 = jnp.float32

PLACES = ((0, 0), (0, 1), (1, 0), (3, 0), (1, 1), (3, 1), (2, 0), (2, 1))
AT = {place: index for index, place in enumerate(PLACES)}
N_PLACE = len(PLACES)

HALVES = (0, 1)
HALF = ROWS // 2
GATHER = ("z", "plus_own", "minus_own", "plus_par", "minus_par", "plus_far", "minus_far")
REDUCE = ("far_plus", "far_minus", "near_plus", "near_minus", "relay_plus", "relay_minus", "z")
FLOWS = {}
for name in GATHER:
    FLOWS["ids", name] = len(FLOWS)
    for part in HALVES:
        for kind in ("img", "txt"):
            FLOWS[kind, name, part] = len(FLOWS)
for kind in ("dimg", "dimg_s", "dtxt", "dtxt_s"):
    for name in REDUCE:
        for part in HALVES:
            FLOWS[kind, name, part] = len(FLOWS)
for place in range(N_PLACE):
    FLOWS["share", place] = len(FLOWS)
for place in range(N_PLACE):
    FLOWS["swap", place] = len(FLOWS)
FLOWS["loss_core"] = len(FLOWS)
for axis in ("x", "y", "z"):
    for step in (1, 2, 3):
        FLOWS["loss", axis, step] = len(FLOWS)
N_FLOW = len(FLOWS)


def normalize(values):
    wide = values.astype(F32)
    recip = lax.rsqrt(jnp.sum(wide * wide, axis=1, keepdims=True) + EPSILON)
    return (wide * recip, recip)


def project_back(unit, recip, grad):
    return recip * (grad - unit * jnp.sum(unit * grad, axis=1, keepdims=True))


def tile_at(index):
    table = (
        (8, 4, lambda k: 7 - k // 4, lambda k: 3 - k % 4),
        (14, 1, lambda k: 5 - k, lambda k: 3),
        (20, 3, lambda k: 5 - k // 3, lambda k: 2 - k % 3),
        (24, 1, lambda k: 3 - k, lambda k: 2),
    )
    first = 0
    pair, group = jnp.int32(0), jnp.int32(0)
    for last, _, pair_of, group_of in table:
        inside = jnp.logical_and(index >= first, index < last)
        pair = jnp.where(inside, pair_of(index - first), pair)
        group = jnp.where(inside, group_of(index - first), group)
        first = last
    return pair, group


def kernel(
    img_in, txt_in, ids_in, scale_ref, bias_ref,
    img_out, txt_out, loss_out,
    img_raw, txt_raw, ids_raw, scale_raw, bias_raw,
    img, txt, ids, dimg, swap, dtxt, even, odd, kept, sent, sent_s, got, got_s, loss_tile, loss_got,
    load_sem, send_sem, recv_sem,
):
    x, core = lax.axis_index("x"), lax.axis_index("core")
    y, z = lax.axis_index("y"), lax.axis_index("z")
    other = {"core": 1 - core}
    z_img = z + 1 - 2 * lax.rem(z, 2)
    z_txt = 3 - z
    plus = {"img": {"x": lax.rem(x + 1, 4)}, "txt": {"y": lax.rem(y + 1, 4)}}
    minus = {"img": {"x": lax.rem(x + 3, 4)}, "txt": {"y": lax.rem(y + 3, 4)}}
    across = {"img": {"z": z_img}, "txt": {"z": z_txt}}

    loads = [
        pltpu.make_async_copy(src, dst, load_sem.at[number])
        for number, (src, dst) in enumerate(
            (
                (img_in, img_raw), (txt_in, txt_raw), (ids_in, ids_raw),
                (scale_ref, scale_raw), (bias_ref, bias_raw),
            )
        )
    ]
    for load in loads:
        load.start()

    started = []

    def copy(flow, src, dst, device):
        return pltpu.make_async_remote_copy(
            src_ref=src, dst_ref=dst, send_sem=send_sem.at[flow], recv_sem=recv_sem.at[flow],
            device_id=device, device_id_type=MESH,
        )

    def launch(make):
        make().start()
        started.append(make)

    barrier = pltpu.get_barrier_semaphore()
    peers = [other]
    for axis, here in (("x", x), ("y", y), ("z", z)):
        for step in (1, 2, 3):
            peers.append({axis: lax.rem(here + step, 4)})
    for peer in peers:
        pl.semaphore_signal(barrier, inc=1, device_id=peer, device_id_type=MESH)

    def img_rows(place, which):
        return pl.ds((2 * place + which) * ROWS, ROWS)

    def rows(place):
        return pl.ds(place * ROWS, ROWS)

    for load in loads:
        load.wait()
    img[img_rows(0, 0), :] = normalize(img_raw[...])[0].astype(BF16)
    txt[rows(0), :] = normalize(txt_raw[...])[0].astype(BF16)
    ids[0] = jnp.broadcast_to(ids_raw[...], (8, ROWS))
    scale = scale_raw[0]
    bias = bias_raw[0]
    pl.semaphore_wait(barrier, len(peers))

    def gather(kind, name, part):
        ring = "img" if kind == "img" else "txt"
        src, dst, device = {
            "z": ((0, 0), (0, 1), across[ring]),
            "plus_own": ((0, 0), (3, 0), plus[ring]),
            "minus_own": ((0, 0), (1, 0), minus[ring]),
            "plus_par": ((0, 1), (3, 1), plus[ring]),
            "minus_par": ((0, 1), (1, 1), minus[ring]),
            "plus_far": ((3, 0), (2, 0), plus[ring]),
            "minus_far": ((1, 1), (2, 1), minus[ring]),
        }[name]
        src, dst = AT[src], AT[dst]
        if kind == "ids":
            return copy(FLOWS[kind, name], ids.at[src], ids.at[dst], device)
        ref, every = (img, 2) if kind == "img" else (txt, 1)
        return copy(
            FLOWS[kind, name, part],
            ref.at[pl.ds(src * every * ROWS + part * HALF, HALF), :],
            ref.at[pl.ds(dst * every * ROWS + part * HALF, HALF), :],
            device,
        )

    def share(place):
        return copy(
            FLOWS["share", place], img.at[img_rows(place, 0), :], img.at[img_rows(place, 1), :], other
        )

    def go(kind, name, part):
        launch(lambda: gather(kind, name, part))
        if kind == "txt" and part == 1:
            launch(lambda: gather("ids", name, 0))

    def give(place):
        launch(lambda: share(AT[place]))

    def come(kind, name, part):
        gather(kind, name, part).wait_recv()
        if kind == "txt" and part == 1:
            gather("ids", name, 0).wait_recv()

    row_iota = lax.broadcasted_iota(jnp.int32, (2 * ROWS, 1), 0)

    def span(number):
        return pl.ds(pl.multiple_of(number * (2 * ROWS), 2 * ROWS), 2 * ROWS)

    def make_coeff(pair, group):
        logits = scale * lax.dot_general(
            img[span(pair), :], txt[span(group), :], (((1,), (1,)), ((), ())),
            preferred_element_type=F32,
        ) + bias
        owner = jnp.where(pair == 0, y * 4 + z, y * 4 + z_img) * ROWS
        valid = jnp.logical_and(pair < 2, row_iota < ROWS)
        row_ids = jnp.where(valid, owner + row_iota, -1)
        column_ids = jnp.concatenate(
            [ids[2 * group, 0:1, :], ids[2 * group + 1, 0:1, :]], axis=1
        )
        same = row_ids == column_ids
        logits = jnp.where(same, -logits, logits)
        power = jnp.exp(logits)
        one_plus = 1.0 + power
        recip = 1.0 / one_plus
        sigmoid = power * recip
        softplus = jnp.log(one_plus) + (power - (one_plus - 1.0)) * recip
        folded = jnp.sum(softplus.reshape(32, 8, 256), axis=0)
        loss_tile[0] += folded[:, :128] + folded[:, 128:]
        return jnp.where(same, -sigmoid, sigmoid).astype(BF16)

    def use_coeff(half, pair, group):
        here, there = span(pair), span(group)
        dimg[here, :] += jnp.dot(half, txt[there, :], preferred_element_type=F32)
        dtxt[there, :] += lax.dot_general(
            half, img[here, :], (((0,), (0,)), ((), ())), preferred_element_type=F32
        )

    for part in HALVES:
        for name in ("z", "plus_own", "minus_own"):
            go("img", name, part)
            go("txt", name, part)
    give((0, 0))
    dimg[...] = jnp.zeros_like(dimg)
    dtxt[...] = jnp.zeros_like(dtxt)
    loss_tile[0] = jnp.zeros_like(loss_tile[0])
    for part in HALVES:
        for kind in ("img", "txt"):
            come(kind, "z", part)
            go(kind, "plus_par", part)
            go(kind, "minus_par", part)
        for kind in ("img", "txt"):
            come(kind, "plus_own", part)
            go(kind, "plus_far", part)
    give((0, 1))
    give((3, 0))
    for part in HALVES:
        come("img", "minus_own", part)
        come("txt", "minus_own", part)
    give((1, 0))

    for place in range(4):
        share(place).wait_recv()

    def early(index, carry):
        kept[index] = make_coeff(3 - index // 2, 1 - lax.rem(index, 2))
        return carry

    lax.fori_loop(0, 8, early, 0)
    for part in HALVES:
        for kind in ("img", "txt"):
            come(kind, "minus_par", part)
            go(kind, "minus_far", part)
    give((1, 1))
    for part in HALVES:
        come("img", "plus_par", part)
        come("txt", "plus_par", part)
    give((3, 1))
    for name, place in (("plus_far", (2, 0)), ("minus_far", (2, 1))):
        for part in HALVES:
            come("img", name, part)
        give(place)
    for name in ("plus_far", "minus_far"):
        for part in HALVES:
            come("txt", name, part)
    for place in range(4, N_PLACE):
        share(place).wait_recv()

    eye = lax.broadcasted_iota(jnp.int32, (HALF, ROWS), 0) == lax.broadcasted_iota(
        jnp.int32, (HALF, ROWS), 1
    )

    def give_back(place):
        return copy(
            FLOWS["swap", 0] + place, dimg.at[img_rows(place, 1), :], swap.at[rows(place), :], other
        )

    def slot(kind, name, part):
        number = REDUCE.index(name) + (0 if kind == "dimg" else len(REDUCE))
        return number * 2 + part

    def sum_ref(kind, place, part):
        if kind == "dimg":
            return dimg.at[pl.ds(AT[place] * 2 * ROWS + part * HALF, HALF), :]
        return dtxt.at[pl.ds(AT[place] * ROWS + part * HALF, HALF), :]

    def route(kind, name):
        ring = "img" if kind == "dimg" else "txt"
        if name == "z":
            return across[ring]
        return plus[ring] if name.endswith("plus") else minus[ring]

    def values(kind, name, part):
        s = slot(kind, name, part)
        return copy(FLOWS[kind, name, part], sent.at[s], got.at[s], route(kind, name))

    def units(kind, name, part):
        s = slot(kind, name, part)
        return copy(FLOWS[kind + "_s", name, part], sent_s.at[s], got_s.at[s], route(kind, name))

    def send(kind, name, place, part):
        ref = sum_ref(kind, place, part)
        s = slot(kind, name, part)
        top = jnp.maximum(jnp.max(jnp.abs(ref[...]), axis=1, keepdims=True), 1e-30)
        across_lanes = jnp.sum(jnp.where(eye, top * (1.0 / 32767.0), 0.0), axis=0, keepdims=True)
        sent_s[s] = jnp.broadcast_to(across_lanes, (8, ROWS))
        sent[s] = jnp.round(ref[...] * (32767.0 / top)).astype(jnp.int32).astype(jnp.int16)
        launch(lambda: values(kind, name, part))
        launch(lambda: units(kind, name, part))

    def take(kind, name, part):
        s = slot(kind, name, part)
        values(kind, name, part).wait_recv()
        units(kind, name, part).wait_recv()
        unit = jnp.sum(jnp.where(eye, got_s[s, 0:1, :], 0.0), axis=1, keepdims=True)
        return got[s].astype(jnp.int32).astype(F32) * unit

    def add(kind, name, place, part):
        sum_ref(kind, place, part)[...] += take(kind, name, part)

    def merge(place):
        give_back(AT[place]).wait_recv()
        dimg[img_rows(AT[place], 0), :] += swap[rows(AT[place]), :]

    def relay(kind, way, place):
        for part in HALVES:
            add(kind, "far_" + way, place, part)
            send(kind, "relay_" + way, place, part)

    def send_all(kind, name, place):
        for part in HALVES:
            send(kind, name, place, part)

    def pass_back(place):
        launch(lambda: give_back(place))

    def far_dimg():
        merge((2, 1))
        send_all("dimg", "far_minus", (2, 1))
        merge((2, 0))
        send_all("dimg", "far_plus", (2, 0))

    def far_dtxt():
        send_all("dtxt", "far_minus", (2, 1))
        send_all("dtxt", "far_plus", (2, 0))

    def loss_send(axis, here, number):
        loss_got[number, here] = loss_tile[number]
        for stride in (1, 2, 3):
            launch(
                lambda stride=stride: copy(
                    FLOWS["loss", axis, stride], loss_tile.at[number], loss_got.at[number, here],
                    {axis: lax.rem(here + stride, 4)},
                )
            )

    def loss_take(axis, here, number):
        for stride in (1, 2, 3):
            source = lax.rem(here + 4 - stride, 4)
            copy(
                FLOWS["loss", axis, stride], loss_tile.at[number], loss_got.at[number, source],
                {axis: lax.rem(here + stride, 4)},
            ).wait_recv()
        loss_tile[number + 1] = (loss_got[number, 0] + loss_got[number, 1]) + (
            loss_got[number, 2] + loss_got[number, 3]
        )

    def loss_swap():
        return copy(FLOWS["loss_core"], loss_tile.at[0], loss_got.at[0, 0], other)

    events = {
        1: lambda: pass_back(7),
        3: lambda: pass_back(6),
        5: far_dimg,
        6: far_dtxt,
        8: lambda: pass_back(5),
        9: lambda: pass_back(4),
    }

    def make(index, buffer):
        buffer[...] = make_coeff(*tile_at(index))

    def use(index, buffer):
        use_coeff(buffer[...], *tile_at(index))

    make(jnp.int32(0), even)

    def step(index, carry):
        make(2 * index + 1, odd)
        use(2 * index, even)
        make(2 * index + 2, even)
        use(2 * index + 1, odd)
        for moment, event in events.items():
            pl.when(index == moment)(event)
        return carry

    lax.fori_loop(0, 11, step, 0)
    make(jnp.int32(23), odd)
    launch(loss_swap)
    use(jnp.int32(22), even)
    use(jnp.int32(23), odd)

    merge((3, 1))
    relay("dimg", "minus", (3, 1))
    merge((1, 1))
    send_all("dimg", "near_plus", (1, 1))
    loss_swap().wait_recv()
    loss_tile[1] = loss_tile[0] + loss_got[0, 0]
    loss_send("y", y, 1)
    relay("dtxt", "minus", (3, 1))
    send_all("dtxt", "near_plus", (1, 1))

    def late(index, carry):
        use_coeff(kept[2 * index], 3 - index, 1)
        use_coeff(kept[2 * index + 1], 3 - index, 0)
        give_back(3 - index).start()
        return carry

    lax.fori_loop(0, 2, late, 0)
    loss_take("y", y, 1)
    loss_send("z", z, 2)
    lax.fori_loop(2, 4, late, 0)
    for place in range(4):
        started.append(lambda place=place: give_back(place))

    relay("dtxt", "plus", (1, 0))
    send_all("dtxt", "near_minus", (3, 0))
    merge((3, 0))
    send_all("dimg", "near_minus", (3, 0))
    merge((1, 0))
    relay("dimg", "plus", (1, 0))
    merge((0, 1))
    for kind in ("dimg", "dtxt"):
        for part in HALVES:
            add(kind, "near_plus", (0, 1), part)
    loss_take("z", z, 2)
    loss_send("x", x, 3)
    for kind in ("dimg", "dtxt"):
        for part in HALVES:
            add(kind, "relay_minus", (0, 1), part)
            send(kind, "z", (0, 1), part)
    merge((0, 0))
    for name in ("near_minus", "relay_plus"):
        for kind in ("dtxt", "dimg"):
            for part in HALVES:
                add(kind, name, (0, 0), part)
    loss_take("x", x, 3)
    count = F32(ROWS * 128)
    loss_out[0] = jnp.sum(loss_tile[4]) / (count * count)
    for kind, source, out in (("dimg", img_raw, img_out), ("dtxt", txt_raw, txt_out)):
        for part in HALVES:
            ref = sum_ref(kind, (0, 0), part)
            piece = pl.ds(part * HALF, HALF)
            ref[...] = scale * (ref[...] + take(kind, "z", part))
            unit, recip = normalize(source[piece, :])
            out[piece, :] = project_back(unit, recip, ref[...])

    for make in started:
        make().wait_send()


def per_device(images, texts, lang_order, position, logit_scale, logit_bias):
    rows, width = images.shape
    ids = lang_order.reshape(1, rows)
    whole = pl.BlockSpec(memory_space=pl.ANY)
    vmem = pl.BlockSpec(memory_space=pltpu.VMEM)
    smem = pl.BlockSpec(memory_space=pltpu.SMEM)
    return pl.pallas_call(
        kernel,
        out_shape=(
            jax.ShapeDtypeStruct((rows, width), F32),
            jax.ShapeDtypeStruct((rows, width), F32),
            jax.ShapeDtypeStruct((1,), F32),
        ),
        in_specs=[whole] * 5,
        out_specs=(vmem, vmem, smem),
        scratch_shapes=[
            pltpu.VMEM((rows, width), BF16),
            pltpu.VMEM((rows, width), BF16),
            pltpu.VMEM((1, rows), jnp.int32),
            pltpu.SMEM((1,), F32),
            pltpu.SMEM((1,), F32),
            pltpu.VMEM((16 * rows, width), BF16),
            pltpu.VMEM((8 * rows, width), BF16),
            pltpu.VMEM((8, 8, rows), jnp.int32),
            pltpu.VMEM((16 * rows, width), F32),
            pltpu.VMEM((8 * rows, width), F32),
            pltpu.VMEM((8 * rows, width), F32),
            pltpu.VMEM((2 * rows, 2 * rows), BF16),
            pltpu.VMEM((2 * rows, 2 * rows), BF16),
            pltpu.VMEM((8, 2 * rows, 2 * rows), BF16),
            pltpu.VMEM((28, HALF, width), jnp.int16),
            pltpu.VMEM((28, 8, rows), F32),
            pltpu.VMEM((28, HALF, width), jnp.int16),
            pltpu.VMEM((28, 8, rows), F32),
            pltpu.VMEM((5, 8, 128), F32),
            pltpu.VMEM((4, 4, 8, 128), F32),
            pltpu.SemaphoreType.DMA((5,)),
            pltpu.SemaphoreType.DMA((N_FLOW,)),
            pltpu.SemaphoreType.DMA((N_FLOW,)),
        ],
        compiler_params=pltpu.CompilerParams(
            collective_id=0, has_side_effects=True, vmem_limit_bytes=62 * 1024 * 1024
        ),
        name="pair_grads",
    )(images, texts, ids, logit_scale, logit_bias)


def solution(mesh):
    finer = Mesh(mesh.devices.reshape(4, 2, 4, 4), AXES)
    return jax.shard_map(
        per_device,
        mesh=finer,
        in_specs=(P(AXES, None), P(AXES, None), P(AXES), P(AXES), P(), P()),
        out_specs=(P(AXES, None), P(AXES, None), P()),
        check_vma=False,
    )
```

```python
import jax
import jax.numpy as jnp
from jax import lax
from jax.experimental import pallas as pl
from jax.experimental.pallas import tpu as pltpu
from jax.sharding import Mesh
from jax.sharding import PartitionSpec as P

AXES = ("x", "core", "y", "z")
MESH = pl.DeviceIdType.MESH
EPSILON = 1e-06
ROWS = 128
BF16 = jnp.bfloat16
F32 = jnp.float32

PLACES = ((0, 0), (0, 1), (1, 0), (3, 0), (1, 1), (3, 1), (2, 0), (2, 1))
AT = {place: index for index, place in enumerate(PLACES)}
N_PLACE = len(PLACES)

HALVES = (0, 1)
HALF = ROWS // 2
GATHER = ("z", "plus_own", "minus_own", "plus_par", "minus_par", "plus_far", "minus_far", "z_far")
REDUCE = ("far_plus", "far_minus", "near_plus", "near_minus", "relay_plus", "relay_minus", "z")
FLOWS = {}
for name in GATHER:
    FLOWS["ids", name] = len(FLOWS)
    for part in HALVES:
        for kind in ("img", "txt"):
            FLOWS[kind, name, part] = len(FLOWS)
for kind in ("dimg", "dimg_s", "dtxt", "dtxt_s"):
    for name in REDUCE:
        for part in HALVES:
            FLOWS[kind, name, part] = len(FLOWS)
for place in range(N_PLACE):
    FLOWS["share", place] = len(FLOWS)
for place in range(N_PLACE):
    FLOWS["swap", place] = len(FLOWS)
FLOWS["loss_core"] = len(FLOWS)
for axis in ("x", "y", "z"):
    for step in (1, 2, 3):
        FLOWS["loss", axis, step] = len(FLOWS)
N_FLOW = len(FLOWS)


def normalize(values):
    wide = values.astype(F32)
    recip = lax.rsqrt(jnp.sum(wide * wide, axis=1, keepdims=True) + EPSILON)
    return (wide * recip, recip)


def project_back(unit, recip, grad):
    return recip * (grad - unit * jnp.sum(unit * grad, axis=1, keepdims=True))


def tile_at(index):
    table = (
        (8, lambda k: 3 - k // 2, lambda k: 1 - k % 2),
        (14, lambda k: 5 - k // 3, lambda k: 2 - k % 3),
        (18, lambda k: 3 - k, lambda k: 2),
        (26, lambda k: 7 - k // 4, lambda k: 3 - k % 4),
        (32, lambda k: 5 - k, lambda k: 3),
    )
    first = 0
    pair, group = jnp.int32(0), jnp.int32(0)
    for last, pair_of, group_of in table:
        inside = jnp.logical_and(index >= first, index < last)
        pair = jnp.where(inside, pair_of(index - first), pair)
        group = jnp.where(inside, group_of(index - first), group)
        first = last
    return pair, group


def kernel(
    img_in, txt_in, ids_in, scale_ref, bias_ref,
    img_out, txt_out, loss_out,
    img_raw, txt_raw, ids_raw, scale_raw, bias_raw,
    img, txt, ids, dimg, swap, dtxt, even, odd, sent, sent_s, got, got_s, loss_tile, loss_got,
    load_sem, send_sem, recv_sem,
):
    x, core = lax.axis_index("x"), lax.axis_index("core")
    y, z = lax.axis_index("y"), lax.axis_index("z")
    other = {"core": 1 - core}
    z_img = z + 1 - 2 * lax.rem(z, 2)
    z_txt = 3 - z
    plus = {"img": {"x": lax.rem(x + 1, 4)}, "txt": {"y": lax.rem(y + 1, 4)}}
    minus = {"img": {"x": lax.rem(x + 3, 4)}, "txt": {"y": lax.rem(y + 3, 4)}}
    across = {"img": {"z": z_img}, "txt": {"z": z_txt}}

    loads = [
        pltpu.make_async_copy(src, dst, load_sem.at[number])
        for number, (src, dst) in enumerate(
            (
                (img_in, img_raw), (txt_in, txt_raw), (ids_in, ids_raw),
                (scale_ref, scale_raw), (bias_ref, bias_raw),
            )
        )
    ]
    for load in loads:
        load.start()

    started = []

    def copy(flow, src, dst, device):
        return pltpu.make_async_remote_copy(
            src_ref=src, dst_ref=dst, send_sem=send_sem.at[flow], recv_sem=recv_sem.at[flow],
            device_id=device, device_id_type=MESH,
        )

    def launch(make):
        make().start()
        started.append(make)

    barrier = pltpu.get_barrier_semaphore()
    peers = [other]
    for axis, here in (("x", x), ("y", y), ("z", z)):
        for step in (1, 2, 3):
            peers.append({axis: lax.rem(here + step, 4)})
    for step in (1, 3):
        peers.append({"x": lax.rem(x + step, 4), "z": z_img})
        peers.append({"y": lax.rem(y + step, 4), "z": z_txt})
    for peer in peers:
        pl.semaphore_signal(barrier, inc=1, device_id=peer, device_id_type=MESH)

    def img_rows(place, which):
        return pl.ds((2 * place + which) * ROWS, ROWS)

    def rows(place):
        return pl.ds(place * ROWS, ROWS)

    for load in loads:
        load.wait()
    img[img_rows(0, 0), :] = normalize(img_raw[...])[0].astype(BF16)
    txt[rows(0), :] = normalize(txt_raw[...])[0].astype(BF16)
    ids[0] = jnp.broadcast_to(ids_raw[...], (8, ROWS))
    scale = scale_raw[0]
    bias = bias_raw[0]
    pl.semaphore_wait(barrier, len(peers))

    def gather(kind, name, part):
        ring = "img" if kind == "img" else "txt"
        src, dst, device = {
            "z": ((0, 0), (0, 1), across[ring]),
            "plus_own": ((0, 0), (3, 0), plus[ring]),
            "minus_own": ((0, 0), (1, 0), minus[ring]),
            "plus_par": ((0, 1), (3, 1), plus[ring]),
            "minus_par": ((0, 1), (1, 1), minus[ring]),
            "plus_far": ((3, 0), (2, 0), plus[ring]),
            "minus_far": ((1, 0), (2, 0), minus[ring]),
            "z_far": ((2, 0), (2, 1), across[ring]),
        }[name]
        src, dst = AT[src], AT[dst]
        if kind == "ids":
            return copy(FLOWS[kind, name], ids.at[src], ids.at[dst], device)
        ref, every = (img, 2) if kind == "img" else (txt, 1)
        return copy(
            FLOWS[kind, name, part],
            ref.at[pl.ds(src * every * ROWS + part * HALF, HALF), :],
            ref.at[pl.ds(dst * every * ROWS + part * HALF, HALF), :],
            device,
        )

    def share(place):
        return copy(
            FLOWS["share", place], img.at[img_rows(place, 0), :], img.at[img_rows(place, 1), :], other
        )

    def go(kind, name, part):
        launch(lambda: gather(kind, name, part))
        if kind == "txt" and part == 1:
            launch(lambda: gather("ids", name, 0))

    def give(place):
        launch(lambda: share(AT[place]))

    def come(kind, name, part):
        gather(kind, name, part).wait_recv()
        if kind == "txt" and part == 1:
            gather("ids", name, 0).wait_recv()

    row_iota = lax.broadcasted_iota(jnp.int32, (2 * ROWS, 1), 0)

    def span(number):
        return pl.ds(pl.multiple_of(number * (2 * ROWS), 2 * ROWS), 2 * ROWS)

    def make_coeff(pair, group):
        logits = scale * lax.dot_general(
            img[span(pair), :], txt[span(group), :], (((1,), (1,)), ((), ())),
            preferred_element_type=F32,
        ) + bias
        owner = jnp.where(pair == 0, y * 4 + z, y * 4 + z_img) * ROWS
        valid = jnp.logical_and(pair < 2, row_iota < ROWS)
        row_ids = jnp.where(valid, owner + row_iota, -1)
        column_ids = jnp.concatenate(
            [ids[2 * group, 0:1, :], ids[2 * group + 1, 0:1, :]], axis=1
        )
        same = row_ids == column_ids
        logits = jnp.where(same, -logits, logits)
        power = jnp.exp(logits)
        one_plus = 1.0 + power
        recip = 1.0 / one_plus
        sigmoid = power * recip
        softplus = jnp.log(one_plus) + (power - (one_plus - 1.0)) * recip
        folded = jnp.sum(softplus.reshape(32, 8, 256), axis=0)
        loss_tile[0] += folded[:, :128] + folded[:, 128:]
        return jnp.where(same, -sigmoid, sigmoid).astype(BF16)

    def use_coeff(half, pair, group):
        here, there = span(pair), span(group)
        dimg[here, :] += jnp.dot(half, txt[there, :], preferred_element_type=F32)
        dtxt[there, :] += lax.dot_general(
            half, img[here, :], (((0,), (0,)), ((), ())), preferred_element_type=F32
        )

    for part in HALVES:
        for name in ("z", "plus_own", "minus_own"):
            go("img", name, part)
            go("txt", name, part)
    give((0, 0))
    dimg[...] = jnp.zeros_like(dimg)
    dtxt[...] = jnp.zeros_like(dtxt)
    loss_tile[0] = jnp.zeros_like(loss_tile[0])
    for kind in ("img", "txt"):
        come(kind, "plus_own", 0)
        go(kind, "plus_far", 0)
    for kind in ("img", "txt"):
        come(kind, "z", 0)
        go(kind, "plus_par", 0)
        go(kind, "minus_par", 0)
    for kind in ("img", "txt"):
        come(kind, "minus_own", 0)
        come(kind, "minus_own", 1)
        go(kind, "minus_far", 1)
    give((1, 0))
    for kind in ("img", "txt"):
        come(kind, "z", 1)
        go(kind, "plus_par", 1)
        go(kind, "minus_par", 1)
    give((0, 1))
    for kind in ("img", "txt"):
        come(kind, "plus_own", 1)
    give((3, 0))
    for place in range(4):
        share(place).wait_recv()

    def far_on():
        for kind in ("img", "txt"):
            come(kind, "plus_far", 0)
            go(kind, "z_far", 0)
        for kind in ("img", "txt"):
            come(kind, "minus_far", 1)
            go(kind, "z_far", 1)
        give((2, 0))

    def partners_here():
        for name, place in (("minus_par", (1, 1)), ("plus_par", (3, 1))):
            for part in HALVES:
                come("img", name, part)
            give(place)
        for name in ("minus_par", "plus_par"):
            for part in HALVES:
                come("txt", name, part)
        for place in ((1, 1), (3, 1)):
            share(AT[place]).wait_recv()

    def far_here():
        for part in HALVES:
            come("img", "z_far", part)
        give((2, 1))
        for part in HALVES:
            come("txt", "z_far", part)
        for place in ((2, 0), (2, 1)):
            share(AT[place]).wait_recv()

    eye = lax.broadcasted_iota(jnp.int32, (HALF, ROWS), 0) == lax.broadcasted_iota(
        jnp.int32, (HALF, ROWS), 1
    )

    def give_back(place):
        return copy(
            FLOWS["swap", 0] + place, dimg.at[img_rows(place, 1), :], swap.at[rows(place), :], other
        )

    def slot(kind, name, part):
        number = REDUCE.index(name) + (0 if kind == "dimg" else len(REDUCE))
        return number * 2 + part

    def sum_ref(kind, place, part):
        if kind == "dimg":
            return dimg.at[pl.ds(AT[place] * 2 * ROWS + part * HALF, HALF), :]
        return dtxt.at[pl.ds(AT[place] * ROWS + part * HALF, HALF), :]

    def route(kind, name):
        ring = "img" if kind == "dimg" else "txt"
        if name == "z":
            return across[ring]
        if name == "relay_minus":
            return {**minus[ring], **across[ring]}
        return plus[ring] if name.endswith("plus") else minus[ring]

    def values(kind, name, part):
        s = slot(kind, name, part)
        return copy(FLOWS[kind, name, part], sent.at[s], got.at[s], route(kind, name))

    def units(kind, name, part):
        s = slot(kind, name, part)
        return copy(FLOWS[kind + "_s", name, part], sent_s.at[s], got_s.at[s], route(kind, name))

    def send(kind, name, place, part):
        ref = sum_ref(kind, place, part)
        s = slot(kind, name, part)
        top = jnp.maximum(jnp.max(jnp.abs(ref[...]), axis=1, keepdims=True), 1e-30)
        across_lanes = jnp.sum(jnp.where(eye, top * (1.0 / 32767.0), 0.0), axis=0, keepdims=True)
        sent_s[s] = jnp.broadcast_to(across_lanes, (8, ROWS))
        sent[s] = jnp.round(ref[...] * (32767.0 / top)).astype(jnp.int32).astype(jnp.int16)
        launch(lambda: values(kind, name, part))
        launch(lambda: units(kind, name, part))

    def take(kind, name, part):
        s = slot(kind, name, part)
        values(kind, name, part).wait_recv()
        units(kind, name, part).wait_recv()
        unit = jnp.sum(jnp.where(eye, got_s[s, 0:1, :], 0.0), axis=1, keepdims=True)
        return got[s].astype(jnp.int32).astype(F32) * unit

    def add(kind, name, place, part):
        sum_ref(kind, place, part)[...] += take(kind, name, part)

    def merge(place):
        give_back(AT[place]).wait_recv()
        dimg[img_rows(AT[place], 0), :] += swap[rows(AT[place]), :]

    def relay(kind, way, place):
        for part in HALVES:
            add(kind, "far_" + way, place, part)
            send(kind, "relay_" + way, place, part)

    def send_all(kind, name, place):
        for part in HALVES:
            send(kind, name, place, part)

    def pass_back(place):
        launch(lambda: give_back(place))

    def far_dimg():
        merge((2, 1))
        send_all("dimg", "far_minus", (2, 1))
        merge((2, 0))
        send_all("dimg", "far_plus", (2, 0))

    def far_dtxt():
        send_all("dtxt", "far_minus", (2, 1))
        send_all("dtxt", "far_plus", (2, 0))

    def loss_send(axis, here, number):
        loss_got[number, here] = loss_tile[number]
        for stride in (1, 2, 3):
            launch(
                lambda stride=stride: copy(
                    FLOWS["loss", axis, stride], loss_tile.at[number], loss_got.at[number, here],
                    {axis: lax.rem(here + stride, 4)},
                )
            )

    def loss_take(axis, here, number):
        for stride in (1, 2, 3):
            source = lax.rem(here + 4 - stride, 4)
            copy(
                FLOWS["loss", axis, stride], loss_tile.at[number], loss_got.at[number, source],
                {axis: lax.rem(here + stride, 4)},
            ).wait_recv()
        loss_tile[number + 1] = (loss_got[number, 0] + loss_got[number, 1]) + (
            loss_got[number, 2] + loss_got[number, 3]
        )

    def loss_swap():
        return copy(FLOWS["loss_core"], loss_tile.at[0], loss_got.at[0, 0], other)

    def near_dtxt(part):
        send("dtxt", "near_plus", (1, 1), part)
        send("dtxt", "near_minus", (3, 0), part)

    def two_back(place):
        pass_back(place)
        pass_back(place - 1)

    def sixth_back():
        pass_back(6)
        near_dtxt(0)

    def third_back():
        two_back(3)
        far_dimg()

    events = {
        0: far_on,
        2: partners_here,
        7: far_here,
        10: lambda: pass_back(7),
        12: sixth_back,
        13: lambda: two_back(5),
        14: third_back,
    }

    def make(index, buffer):
        buffer[...] = make_coeff(*tile_at(index))

    def use(index, buffer):
        use_coeff(buffer[...], *tile_at(index))

    make(jnp.int32(0), even)

    def step(index, carry):
        make(2 * index + 1, odd)
        use(2 * index, even)
        make(2 * index + 2, even)
        use(2 * index + 1, odd)
        for moment, event in events.items():
            pl.when(index == moment)(event)
        return carry

    lax.fori_loop(0, 15, step, 0)
    make(jnp.int32(31), odd)
    launch(loss_swap)
    use(jnp.int32(30), even)
    use(jnp.int32(31), odd)
    two_back(1)

    far_dtxt()
    loss_swap().wait_recv()
    loss_tile[1] = loss_tile[0] + loss_got[0, 0]
    loss_send("z", z, 1)
    merge((1, 1))
    send_all("dimg", "near_plus", (1, 1))
    merge((3, 0))
    send_all("dimg", "near_minus", (3, 0))
    merge((3, 1))
    merge((1, 0))
    merge((0, 1))
    merge((0, 0))
    loss_take("z", z, 1)
    loss_send("x", x, 2)
    add("dtxt", "near_plus", (0, 1), 0)
    send("dtxt", "z", (0, 1), 0)
    relay("dimg", "minus", (3, 1))
    relay("dimg", "plus", (1, 0))
    relay("dtxt", "minus", (3, 1))
    relay("dtxt", "plus", (1, 0))
    near_dtxt(1)
    for part in HALVES:
        add("dimg", "near_plus", (0, 1), part)
        send("dimg", "z", (0, 1), part)
    loss_take("x", x, 2)
    loss_send("y", y, 3)
    add("dtxt", "near_minus", (0, 0), 0)
    for part in HALVES:
        add("dimg", "near_minus", (0, 0), part)
    add("dtxt", "near_plus", (0, 1), 1)
    send("dtxt", "z", (0, 1), 1)
    for name in ("relay_plus", "relay_minus"):
        for kind in ("dimg", "dtxt"):
            for part in HALVES:
                add(kind, name, (0, 0), part)
    add("dtxt", "near_minus", (0, 0), 1)
    loss_take("y", y, 3)
    count = F32(ROWS * 128)
    loss_out[0] = jnp.sum(loss_tile[4]) / (count * count)
    for kind, source, out in (("dimg", img_raw, img_out), ("dtxt", txt_raw, txt_out)):
        for part in HALVES:
            ref = sum_ref(kind, (0, 0), part)
            piece = pl.ds(part * HALF, HALF)
            ref[...] = scale * (ref[...] + take(kind, "z", part))
            unit, recip = normalize(source[piece, :])
            out[piece, :] = project_back(unit, recip, ref[...])

    for make in started:
        make().wait_send()


def per_device(images, texts, lang_order, position, logit_scale, logit_bias):
    rows, width = images.shape
    ids = lang_order.reshape(1, rows)
    whole = pl.BlockSpec(memory_space=pl.ANY)
    vmem = pl.BlockSpec(memory_space=pltpu.VMEM)
    smem = pl.BlockSpec(memory_space=pltpu.SMEM)
    return pl.pallas_call(
        kernel,
        out_shape=(
            jax.ShapeDtypeStruct((rows, width), F32),
            jax.ShapeDtypeStruct((rows, width), F32),
            jax.ShapeDtypeStruct((1,), F32),
        ),
        in_specs=[whole] * 5,
        out_specs=(vmem, vmem, smem),
        scratch_shapes=[
            pltpu.VMEM((rows, width), BF16),
            pltpu.VMEM((rows, width), BF16),
            pltpu.VMEM((1, rows), jnp.int32),
            pltpu.SMEM((1,), F32),
            pltpu.SMEM((1,), F32),
            pltpu.VMEM((16 * rows, width), BF16),
            pltpu.VMEM((8 * rows, width), BF16),
            pltpu.VMEM((8, 8, rows), jnp.int32),
            pltpu.VMEM((16 * rows, width), F32),
            pltpu.VMEM((8 * rows, width), F32),
            pltpu.VMEM((8 * rows, width), F32),
            pltpu.VMEM((2 * rows, 2 * rows), BF16),
            pltpu.VMEM((2 * rows, 2 * rows), BF16),
            pltpu.VMEM((28, HALF, width), jnp.int16),
            pltpu.VMEM((28, 8, rows), F32),
            pltpu.VMEM((28, HALF, width), jnp.int16),
            pltpu.VMEM((28, 8, rows), F32),
            pltpu.VMEM((5, 8, 128), F32),
            pltpu.VMEM((4, 4, 8, 128), F32),
            pltpu.SemaphoreType.DMA((5,)),
            pltpu.SemaphoreType.DMA((N_FLOW,)),
            pltpu.SemaphoreType.DMA((N_FLOW,)),
        ],
        compiler_params=pltpu.CompilerParams(
            collective_id=0, has_side_effects=True, vmem_limit_bytes=62 * 1024 * 1024
        ),
        name="pair_grads",
    )(images, texts, ids, logit_scale, logit_bias)


def solution(mesh):
    finer = Mesh(mesh.devices.reshape(4, 2, 4, 4), AXES)
    return jax.shard_map(
        per_device,
        mesh=finer,
        in_specs=(P(AXES, None), P(AXES, None), P(AXES), P(AXES), P(), P()),
        out_specs=(P(AXES, None), P(AXES, None), P()),
        check_vma=False,
    )
```

```python
import jax
import jax.numpy as jnp
from jax import lax
from jax.experimental import pallas as pl
from jax.experimental.pallas import tpu as pltpu
from jax.sharding import Mesh
from jax.sharding import PartitionSpec as P

AXES = ("x", "core", "y", "z")
MESH = pl.DeviceIdType.MESH
EPSILON = 1e-06
ROWS = 128
WIDTH = 1152
BF16 = jnp.bfloat16
F32 = jnp.float32

PLACES = (0b000, 0b001, 0b010, 0b100, 0b011, 0b101, 0b110, 0b111)
AT = {place: index for index, place in enumerate(PLACES)}
N_PLACE = len(PLACES)
THIRDS = (0, 1, 2)
ORDER = ((0, 1, 2), (1, 2, 0), (2, 0, 1))


def level(third, place):
    return max((n for n, axis in enumerate(ORDER[third]) if place >> axis & 1), default=-1)


def onward(third, place):
    return [place | 1 << axis for axis in ORDER[third][level(third, place) + 1 :]]


FLOWS = {}
for place in PLACES[1:]:
    FLOWS["ids", place] = len(FLOWS)
    for kind in ("img", "txt", "dimg", "dimg_s", "dtxt", "dtxt_s"):
        for third in THIRDS:
            FLOWS[kind, third, place] = len(FLOWS)
for place in range(N_PLACE):
    FLOWS["share", place] = len(FLOWS)
for place in range(N_PLACE):
    FLOWS["swap", place] = len(FLOWS)
FLOWS["loss_core"] = len(FLOWS)
for axis in ("x", "y", "z"):
    for step in (1, 2, 3):
        FLOWS["loss", axis, step] = len(FLOWS)
N_FLOW = len(FLOWS)


def normalize(values):
    wide = values.astype(F32)
    recip = lax.rsqrt(jnp.sum(wide * wide, axis=1, keepdims=True) + EPSILON)
    return (wide * recip, recip)


def project_back(unit, recip, grad):
    return recip * (grad - unit * jnp.sum(unit * grad, axis=1, keepdims=True))


def tile_at(index):
    table = (
        (8, lambda k: 3 - k // 2, lambda k: 1 - k % 2),
        (16, lambda k: 7 - k // 4, lambda k: 3 - k % 4),
        (22, lambda k: 5 - k, lambda k: 3),
        (28, lambda k: 5 - k // 3, lambda k: 2 - k % 3),
        (32, lambda k: 3 - k, lambda k: 2),
    )
    first = 0
    pair, group = jnp.int32(0), jnp.int32(0)
    for last, pair_of, group_of in table:
        inside = jnp.logical_and(index >= first, index < last)
        pair = jnp.where(inside, pair_of(index - first), pair)
        group = jnp.where(inside, group_of(index - first), group)
        first = last
    return pair, group


def kernel(
    img_in, txt_in, ids_in, scale_ref, bias_ref,
    img_out, txt_out, loss_out,
    img_raw, txt_raw, ids_raw, scale_raw, bias_raw,
    img, txt, ids, dimg, swap, dtxt, even, odd, sent, sent_s, got, got_s, loss_tile, loss_got,
    load_sem, send_sem, recv_sem,
):
    x, core = lax.axis_index("x"), lax.axis_index("core")
    y, z = lax.axis_index("y"), lax.axis_index("z")
    other = {"core": 1 - core}
    here = {"x": x, "y": y, "z": z}
    partner = {
        "img": [{axis: at + 1 - 2 * lax.rem(at, 2)} for axis, at in here.items()],
        "txt": [{axis: 3 - at} for axis, at in here.items()],
    }
    partner["dimg"] = partner["img"]
    partner["dtxt"] = partner["ids"] = partner["txt"]

    loads = [
        pltpu.make_async_copy(src, dst, load_sem.at[number])
        for number, (src, dst) in enumerate(
            (
                (img_in, img_raw), (txt_in, txt_raw), (ids_in, ids_raw),
                (scale_ref, scale_raw), (bias_ref, bias_raw),
            )
        )
    ]
    for load in loads:
        load.start()

    started = []

    def copy(flow, src, dst, device):
        return pltpu.make_async_remote_copy(
            src_ref=src, dst_ref=dst, send_sem=send_sem.at[flow], recv_sem=recv_sem.at[flow],
            device_id=device, device_id_type=MESH,
        )

    def launch(make):
        make().start()
        started.append(make)

    barrier = pltpu.get_barrier_semaphore()
    peers = [other]
    for axis, here in (("x", x), ("y", y), ("z", z)):
        for step in (1, 2, 3):
            peers.append({axis: lax.rem(here + step, 4)})
    for peer in peers:
        pl.semaphore_signal(barrier, inc=1, device_id=peer, device_id_type=MESH)

    def img_rows(place, which):
        return pl.ds((2 * place + which) * ROWS, ROWS)

    def rows(place):
        return pl.ds(place * ROWS, ROWS)

    for load in loads:
        load.wait()
    img[img_rows(0, 0), :] = normalize(img_raw[...])[0].astype(BF16)
    txt[rows(0), :] = normalize(txt_raw[...])[0].astype(BF16)
    ids[0] = jnp.broadcast_to(ids_raw[...], (8, ROWS)) + x * (16 * ROWS)
    scale = scale_raw[0]
    bias = bias_raw[0]
    pl.semaphore_wait(barrier, len(peers))

    def columns(third):
        return pl.ds(third * (WIDTH // 3), WIDTH // 3)

    def route(kind, third, place):
        return partner[kind][ORDER[third][level(third, place)]]

    def before(third, place):
        return place ^ 1 << ORDER[third][level(third, place)]

    def gather(kind, third, place):
        src, dst = AT[before(third, place)], AT[place]
        device = route(kind, third, place)
        if kind == "ids":
            return copy(FLOWS[kind, place], ids.at[src], ids.at[dst], device)
        ref, every = (img, 2) if kind == "img" else (txt, 1)
        return copy(
            FLOWS[kind, third, place],
            ref.at[pl.ds(src * every * ROWS, ROWS), columns(third)],
            ref.at[pl.ds(dst * every * ROWS, ROWS), columns(third)],
            device,
        )

    def share(place):
        return copy(
            FLOWS["share", place], img.at[img_rows(place, 0), :], img.at[img_rows(place, 1), :], other
        )

    def go(kind, third, place):
        launch(lambda: gather(kind, third, place))
        if kind == "txt" and third == 0:
            launch(lambda: gather("ids", third, place))

    def give(place):
        launch(lambda: share(AT[place]))

    def come(third, place):
        for kind in ("img", "txt"):
            gather(kind, third, place).wait_recv()
            if kind == "txt" and third == 0:
                gather("ids", third, place).wait_recv()
            for later in onward(third, place):
                go(kind, third, later)

    row_iota = lax.broadcasted_iota(jnp.int32, (2 * ROWS, 1), 0)

    def span(number):
        return pl.ds(pl.multiple_of(number * (2 * ROWS), 2 * ROWS), 2 * ROWS)

    def make_coeff(pair, group):
        logits = scale * lax.dot_general(
            img[span(pair), :], txt[span(group), :], (((1,), (1,)), ((), ())),
            preferred_element_type=F32,
        ) + bias
        with_y = jnp.logical_or(pair == AT[0b010], pair == AT[0b110])
        with_z = jnp.logical_or(pair == AT[0b100], pair == AT[0b110])
        owner = (
            x * 16
            + jnp.where(with_y, partner["img"][1]["y"], y) * 4
            + jnp.where(with_z, partner["img"][2]["z"], z)
        ) * ROWS
        same_x = jnp.logical_or(pair == 0, jnp.logical_or(with_y, with_z))
        valid = jnp.logical_and(same_x, row_iota < ROWS)
        row_ids = jnp.where(valid, owner + row_iota, -1)
        column_ids = jnp.concatenate(
            [ids[2 * group, 0:1, :], ids[2 * group + 1, 0:1, :]], axis=1
        )
        same = row_ids == column_ids
        logits = jnp.where(same, -logits, logits)
        power = jnp.exp(logits)
        one_plus = 1.0 + power
        recip = 1.0 / one_plus
        sigmoid = power * recip
        softplus = jnp.log(one_plus) + (power - (one_plus - 1.0)) * recip
        folded = jnp.sum(softplus.reshape(32, 8, 256), axis=0)
        loss_tile[0] += folded[:, :128] + folded[:, 128:]
        return jnp.where(same, -sigmoid, sigmoid).astype(BF16)

    def use_coeff(half, pair, group):
        here, there = span(pair), span(group)
        dimg[here, :] += jnp.dot(half, txt[there, :], preferred_element_type=F32)
        dtxt[there, :] += lax.dot_general(
            half, img[here, :], (((0,), (0,)), ((), ())), preferred_element_type=F32
        )

    for turn in range(3):
        for axis in range(3):
            for kind in ("img", "txt"):
                go(kind, (axis - turn) % 3, 1 << axis)
    give(0)
    dimg[...] = jnp.zeros_like(dimg)
    dtxt[...] = jnp.zeros_like(dtxt)
    loss_tile[0] = jnp.zeros_like(loss_tile[0])
    for turn in range(3):
        for axis in range(3):
            come((axis - turn) % 3, 1 << axis)
    for axis in range(3):
        give(1 << axis)
    for place in range(4):
        share(place).wait_recv()

    def firsts(third):
        return 1 << ORDER[third][0] | 1 << ORDER[third][1]

    def pass_on():
        for third in THIRDS:
            come(third, firsts(third))

    def all_here():
        for place in (0b111, 0b110, 0b101, 0b011):
            for third in THIRDS:
                if place != firsts(third):
                    come(third, place)
            give(place)
        for place in (0b111, 0b110, 0b101, 0b011):
            share(AT[place]).wait_recv()

    eye = lax.broadcasted_iota(jnp.int32, (ROWS, ROWS), 0) == lax.broadcasted_iota(
        jnp.int32, (ROWS, ROWS), 1
    )

    def give_back(place):
        return copy(
            FLOWS["swap", 0] + place, dimg.at[img_rows(place, 1), :], swap.at[rows(place), :], other
        )

    def slot(kind, third, place):
        return ((place - 1) * 3 + third) * 2 + (kind == "dtxt")

    def sum_ref(kind, third, place):
        if kind == "dimg":
            return dimg.at[pl.ds(AT[place] * 2 * ROWS, ROWS), columns(third)]
        return dtxt.at[pl.ds(AT[place] * ROWS, ROWS), columns(third)]

    def values(kind, third, place):
        s = slot(kind, third, place)
        return copy(FLOWS[kind, third, place], sent.at[s], got.at[s], route(kind, third, place))

    def units(kind, third, place):
        s = slot(kind, third, place)
        return copy(
            FLOWS[kind + "_s", third, place], sent_s.at[s], got_s.at[s], route(kind, third, place)
        )

    def send(kind, third, place):
        for child in onward(third, place):
            add(kind, third, child)
        ref = sum_ref(kind, third, place)
        s = slot(kind, third, place)
        top = jnp.maximum(jnp.max(jnp.abs(ref[...]), axis=1, keepdims=True), 1e-30)
        across_lanes = jnp.sum(jnp.where(eye, top * (1.0 / 32767.0), 0.0), axis=0, keepdims=True)
        sent_s[s] = jnp.broadcast_to(across_lanes, (8, ROWS))
        sent[s] = jnp.round(ref[...] * (32767.0 / top)).astype(jnp.int32).astype(jnp.int16)
        launch(lambda: values(kind, third, place))
        launch(lambda: units(kind, third, place))

    def take(kind, third, place):
        s = slot(kind, third, place)
        values(kind, third, place).wait_recv()
        units(kind, third, place).wait_recv()
        unit = jnp.sum(jnp.where(eye, got_s[s, 0:1, :], 0.0), axis=1, keepdims=True)
        return got[s].astype(jnp.int32).astype(F32) * unit

    def add(kind, third, place):
        sum_ref(kind, third, before(third, place))[...] += take(kind, third, place)

    def merge(place):
        give_back(AT[place]).wait_recv()
        dimg[img_rows(AT[place], 0), :] += swap[rows(AT[place]), :]

    def send_now(kind, place):
        for third in THIRDS:
            if not onward(third, place):
                send(kind, third, place)

    def pass_back(place):
        launch(lambda: give_back(place))

    def loss_send(axis, here, number):
        loss_got[number, here] = loss_tile[number]
        for stride in (1, 2, 3):
            launch(
                lambda stride=stride: copy(
                    FLOWS["loss", axis, stride], loss_tile.at[number], loss_got.at[number, here],
                    {axis: lax.rem(here + stride, 4)},
                )
            )

    def loss_take(axis, here, number):
        for stride in (1, 2, 3):
            source = lax.rem(here + 4 - stride, 4)
            copy(
                FLOWS["loss", axis, stride], loss_tile.at[number], loss_got.at[number, source],
                {axis: lax.rem(here + stride, 4)},
            ).wait_recv()
        loss_tile[number + 1] = (loss_got[number, 0] + loss_got[number, 1]) + (
            loss_got[number, 2] + loss_got[number, 3]
        )

    def loss_swap():
        return copy(FLOWS["loss_core"], loss_tile.at[0], loss_got.at[0, 0], other)

    def two_back(place):
        pass_back(place)
        pass_back(place - 1)

    def after_7():
        pass_back(6)
        merge(0b111)
        send_now("dimg", 0b111)

    def after_9():
        merge(0b110)
        send_now("dimg", 0b110)

    def after_10():
        send_now("dtxt", 0b111)
        send_now("dtxt", 0b110)

    def after_13():
        pass_back(4)
        for axis in range(3):
            send_now("dtxt", 1 << axis)

    def after_14():
        two_back(3)
        merge(0b101)
        send_now("dimg", 0b101)

    events = {
        0: pass_on,
        2: all_here,
        5: lambda: pass_back(7),
        7: after_7,
        9: after_9,
        10: after_10,
        12: lambda: pass_back(5),
        13: after_13,
        14: after_14,
    }

    def make(index, buffer):
        buffer[...] = make_coeff(*tile_at(index))

    def use(index, buffer):
        use_coeff(buffer[...], *tile_at(index))

    make(jnp.int32(0), even)

    def step(index, carry):
        make(2 * index + 1, odd)
        use(2 * index, even)
        make(2 * index + 2, even)
        use(2 * index + 1, odd)
        for moment, event in events.items():
            pl.when(index == moment)(event)
        return carry

    lax.fori_loop(0, 15, step, 0)
    make(jnp.int32(31), odd)
    launch(loss_swap)
    use(jnp.int32(30), even)
    use(jnp.int32(31), odd)
    two_back(1)

    send_now("dtxt", 0b101)
    send_now("dtxt", 0b011)
    merge(0b011)
    send_now("dimg", 0b011)
    loss_swap().wait_recv()
    loss_tile[1] = loss_tile[0] + loss_got[0, 0]
    loss_send("z", z, 1)
    for third in THIRDS:
        for kind in ("dimg", "dtxt"):
            send(kind, third, firsts(third))
    for axis in range(3):
        merge(1 << axis)
        send_now("dimg", 1 << axis)
    merge(0)
    loss_take("z", z, 1)
    loss_send("x", x, 2)
    for third in THIRDS:
        for kind in ("dtxt", "dimg"):
            send(kind, third, 1 << ORDER[third][1])
    loss_take("x", x, 2)
    loss_send("y", y, 3)
    for third in THIRDS:
        for kind in ("dtxt", "dimg"):
            send(kind, third, 1 << ORDER[third][0])
    for turn in (2, 1, 0):
        for third in THIRDS:
            for kind in ("dtxt", "dimg"):
                add(kind, third, 1 << ORDER[third][turn])
    loss_take("y", y, 3)
    count = F32(ROWS * 128)
    loss_out[0] = jnp.sum(loss_tile[4]) / (count * count)
    for kind, source, out in (("dtxt", txt_raw, txt_out), ("dimg", img_raw, img_out)):
        own = pl.ds(0, ROWS)
        grad = scale * (dimg if kind == "dimg" else dtxt)[own, :]
        unit, recip = normalize(source[...])
        out[...] = project_back(unit, recip, grad)

    for make in started:
        make().wait_send()


def per_device(images, texts, lang_order, position, logit_scale, logit_bias):
    rows, width = images.shape
    ids = lang_order.reshape(1, rows)
    whole = pl.BlockSpec(memory_space=pl.ANY)
    vmem = pl.BlockSpec(memory_space=pltpu.VMEM)
    smem = pl.BlockSpec(memory_space=pltpu.SMEM)
    return pl.pallas_call(
        kernel,
        out_shape=(
            jax.ShapeDtypeStruct((rows, width), F32),
            jax.ShapeDtypeStruct((rows, width), F32),
            jax.ShapeDtypeStruct((1,), F32),
        ),
        in_specs=[whole] * 5,
        out_specs=(vmem, vmem, smem),
        scratch_shapes=[
            pltpu.VMEM((rows, width), BF16),
            pltpu.VMEM((rows, width), BF16),
            pltpu.VMEM((1, rows), jnp.int32),
            pltpu.SMEM((1,), F32),
            pltpu.SMEM((1,), F32),
            pltpu.VMEM((16 * rows, width), BF16),
            pltpu.VMEM((8 * rows, width), BF16),
            pltpu.VMEM((8, 8, rows), jnp.int32),
            pltpu.VMEM((16 * rows, width), F32),
            pltpu.VMEM((8 * rows, width), F32),
            pltpu.VMEM((8 * rows, width), F32),
            pltpu.VMEM((2 * rows, 2 * rows), BF16),
            pltpu.VMEM((2 * rows, 2 * rows), BF16),
            pltpu.VMEM((42, rows, width // 3), jnp.int16),
            pltpu.VMEM((42, 8, rows), F32),
            pltpu.VMEM((42, rows, width // 3), jnp.int16),
            pltpu.VMEM((42, 8, rows), F32),
            pltpu.VMEM((5, 8, 128), F32),
            pltpu.VMEM((4, 4, 8, 128), F32),
            pltpu.SemaphoreType.DMA((5,)),
            pltpu.SemaphoreType.DMA((N_FLOW,)),
            pltpu.SemaphoreType.DMA((N_FLOW,)),
        ],
        compiler_params=pltpu.CompilerParams(
            collective_id=0, has_side_effects=True, vmem_limit_bytes=62 * 1024 * 1024
        ),
        name="pair_grads",
    )(images, texts, ids, logit_scale, logit_bias)


def solution(mesh):
    finer = Mesh(mesh.devices.reshape(4, 2, 4, 4), AXES)
    return jax.shard_map(
        per_device,
        mesh=finer,
        in_specs=(P(AXES, None), P(AXES, None), P(AXES), P(AXES), P(), P()),
        out_specs=(P(AXES, None), P(AXES, None), P()),
        check_vma=False,
    )
```

```python
import jax
import jax.numpy as jnp
from jax import lax
from jax.experimental import pallas as pl
from jax.experimental.pallas import tpu as pltpu
from jax.sharding import Mesh
from jax.sharding import PartitionSpec as P

AXES = ("x", "core", "y", "z")
MESH = pl.DeviceIdType.MESH
EPSILON = 1e-06
ROWS = 128
WIDTH = 1152
BF16 = jnp.bfloat16
F32 = jnp.float32

PLACES = (0b000, 0b001, 0b010, 0b100, 0b011, 0b101, 0b110, 0b111)
AT = {place: index for index, place in enumerate(PLACES)}
N_PLACE = len(PLACES)
THIRDS = (0, 1, 2)
ORDER = ((0, 1, 2), (1, 2, 0), (2, 0, 1))


def level(third, place):
    return max((n for n, axis in enumerate(ORDER[third]) if place >> axis & 1), default=-1)


def onward(third, place):
    return [place | 1 << axis for axis in ORDER[third][level(third, place) + 1 :]]


FLOWS = {}
for place in PLACES[1:]:
    FLOWS["ids", place] = len(FLOWS)
    for kind in ("img", "txt", "dimg", "dimg_s", "dtxt", "dtxt_s"):
        for third in THIRDS:
            FLOWS[kind, third, place] = len(FLOWS)
for place in range(N_PLACE):
    FLOWS["share", place] = len(FLOWS)
for place in range(N_PLACE):
    FLOWS["swap", place] = len(FLOWS)
FLOWS["loss_core"] = len(FLOWS)
for axis in ("x", "y", "z"):
    for step in (1, 2, 3):
        FLOWS["loss", axis, step] = len(FLOWS)
N_FLOW = len(FLOWS)


def normalize(values):
    wide = values.astype(F32)
    recip = lax.rsqrt(jnp.sum(wide * wide, axis=1, keepdims=True) + EPSILON)
    return (wide * recip, recip)


def project_back(unit, recip, grad):
    return recip * (grad - unit * jnp.sum(unit * grad, axis=1, keepdims=True))


def tile_at(index):
    table = (
        (4, lambda k: 1 - k // 2, lambda k: 1 - k % 2),
        (6, lambda k: 2, lambda k: 1 - k),
        (7, lambda k: 2, lambda k: 2),
        (11, lambda k: 3, lambda k: 3 - k),
        (14, lambda k: 2 - k, lambda k: 3),
        (16, lambda k: 1 - k, lambda k: 2),
    )
    first = 0
    pair, group = jnp.int32(0), jnp.int32(0)
    for last, pair_of, group_of in table:
        inside = jnp.logical_and(index >= first, index < last)
        pair = jnp.where(inside, pair_of(index - first), pair)
        group = jnp.where(inside, group_of(index - first), group)
        first = last
    return pair, group


def kernel(
    img_in, txt_in, ids_in, scale_ref, bias_ref,
    img_out, txt_out, loss_out,
    img_raw, txt_raw, ids_raw, scale_raw, bias_raw,
    img, txt, ids, dimg, swap, dtxt, even, odd, sent, sent_s, got, got_s, loss_tile, loss_got,
    load_sem, send_sem, recv_sem,
):
    x, core = lax.axis_index("x"), lax.axis_index("core")
    y, z = lax.axis_index("y"), lax.axis_index("z")
    other = {"core": 1 - core}
    here = {"x": x, "y": y, "z": z}
    partner = {
        "img": [{axis: at + 1 - 2 * lax.rem(at, 2)} for axis, at in here.items()],
        "txt": [{axis: 3 - at} for axis, at in here.items()],
    }
    partner["dimg"] = partner["img"]
    partner["dtxt"] = partner["ids"] = partner["txt"]

    loads = [
        pltpu.make_async_copy(src, dst, load_sem.at[number])
        for number, (src, dst) in enumerate(
            (
                (img_in, img_raw), (txt_in, txt_raw), (ids_in, ids_raw),
                (scale_ref, scale_raw), (bias_ref, bias_raw),
            )
        )
    ]
    for load in loads:
        load.start()

    started = []

    def copy(flow, src, dst, device):
        return pltpu.make_async_remote_copy(
            src_ref=src, dst_ref=dst, send_sem=send_sem.at[flow], recv_sem=recv_sem.at[flow],
            device_id=device, device_id_type=MESH,
        )

    def launch(make):
        make().start()
        started.append(make)

    barrier = pltpu.get_barrier_semaphore()
    peers = [other]
    for axis, here in (("x", x), ("y", y), ("z", z)):
        for step in (1, 2, 3):
            peers.append({axis: lax.rem(here + step, 4)})
    for peer in peers:
        pl.semaphore_signal(barrier, inc=1, device_id=peer, device_id_type=MESH)

    def img_rows(place, which):
        return pl.ds((2 * place + which) * ROWS, ROWS)

    def rows(place):
        return pl.ds(place * ROWS, ROWS)

    for load in loads:
        load.wait()
    img[img_rows(0, 0), :] = normalize(img_raw[...])[0].astype(BF16)
    txt[rows(0), :] = normalize(txt_raw[...])[0].astype(BF16)
    ids[0] = jnp.broadcast_to(ids_raw[...], (8, ROWS)) + x * (16 * ROWS)
    scale = scale_raw[0]
    bias = bias_raw[0]
    pl.semaphore_wait(barrier, len(peers))

    def columns(third):
        return pl.ds(third * (WIDTH // 3), WIDTH // 3)

    def route(kind, third, place):
        return partner[kind][ORDER[third][level(third, place)]]

    def before(third, place):
        return place ^ 1 << ORDER[third][level(third, place)]

    def gather(kind, third, place):
        src, dst = AT[before(third, place)], AT[place]
        device = route(kind, third, place)
        if kind == "ids":
            return copy(FLOWS[kind, place], ids.at[src], ids.at[dst], device)
        ref, every = (img, 2) if kind == "img" else (txt, 1)
        return copy(
            FLOWS[kind, third, place],
            ref.at[pl.ds(src * every * ROWS, ROWS), columns(third)],
            ref.at[pl.ds(dst * every * ROWS, ROWS), columns(third)],
            device,
        )

    def share(place):
        return copy(
            FLOWS["share", place], img.at[img_rows(place, 0), :], img.at[img_rows(place, 1), :], other
        )

    def go(kind, third, place):
        launch(lambda: gather(kind, third, place))
        if kind == "txt" and third == 0:
            launch(lambda: gather("ids", third, place))

    def give(place):
        launch(lambda: share(AT[place]))

    def come(third, place):
        for kind in ("img", "txt"):
            gather(kind, third, place).wait_recv()
            if kind == "txt" and third == 0:
                gather("ids", third, place).wait_recv()
            for later in onward(third, place):
                go(kind, third, later)

    tall = 4 * ROWS
    row_iota = lax.broadcasted_iota(jnp.int32, (tall, 1), 0)

    def span(number):
        return pl.ds(pl.multiple_of(number * (2 * ROWS), 2 * ROWS), 2 * ROWS)

    def tall_span(number):
        return pl.ds(pl.multiple_of(number * tall, tall), tall)

    def make_coeff(pair, group):
        logits = scale * lax.dot_general(
            img[tall_span(pair), :], txt[span(group), :], (((1,), (1,)), ((), ())),
            preferred_element_type=F32,
        ) + bias
        lower = row_iota < 2 * ROWS
        place_at = 2 * pair + jnp.where(lower, 0, 1)
        with_y = jnp.logical_or(place_at == AT[0b010], place_at == AT[0b110])
        with_z = jnp.logical_or(place_at == AT[0b100], place_at == AT[0b110])
        owner = (
            x * 16
            + jnp.where(with_y, partner["img"][1]["y"], y) * 4
            + jnp.where(with_z, partner["img"][2]["z"], z)
        ) * ROWS
        within = row_iota - jnp.where(lower, 0, 2 * ROWS)
        same_x = jnp.logical_or(place_at == 0, jnp.logical_or(with_y, with_z))
        valid = jnp.logical_and(same_x, within < ROWS)
        row_ids = jnp.where(valid, owner + within, -1)
        column_ids = jnp.concatenate(
            [ids[2 * group, 0:1, :], ids[2 * group + 1, 0:1, :]], axis=1
        )
        same = row_ids == column_ids
        logits = jnp.where(same, -logits, logits)
        power = jnp.exp(logits)
        one_plus = 1.0 + power
        recip = 1.0 / one_plus
        sigmoid = power * recip
        lost = (power - (one_plus - 1.0)) * recip
        half = tall // 2
        softplus = jnp.log(one_plus[:half] * one_plus[half:]) + (lost[:half] + lost[half:])
        folded = jnp.sum(softplus.reshape(32, 8, 256), axis=0)
        loss_tile[0] += folded[:, :128] + folded[:, 128:]
        return jnp.where(same, -sigmoid, sigmoid).astype(BF16)

    def use_coeff(half, pair, group):
        here, there = tall_span(pair), span(group)
        dimg[here, :] += jnp.dot(half, txt[there, :], preferred_element_type=F32)
        dtxt[there, :] += lax.dot_general(
            half, img[here, :], (((0,), (0,)), ((), ())), preferred_element_type=F32
        )

    for turn in range(3):
        for axis in range(3):
            for kind in ("img", "txt"):
                go(kind, (axis - turn) % 3, 1 << axis)
    give(0)
    dimg[...] = jnp.zeros_like(dimg)
    dtxt[...] = jnp.zeros_like(dtxt)
    loss_tile[0] = jnp.zeros_like(loss_tile[0])
    for turn in range(3):
        for axis in range(3):
            come((axis - turn) % 3, 1 << axis)
    for axis in range(3):
        give(1 << axis)
    for place in range(4):
        share(place).wait_recv()

    def firsts(third):
        return 1 << ORDER[third][0] | 1 << ORDER[third][1]

    def pass_on():
        for third in THIRDS:
            come(third, firsts(third))

    def partners_here():
        for place in (0b011, 0b101):
            for third in THIRDS:
                if place != firsts(third):
                    come(third, place)
            give(place)
        for place in (0b011, 0b101):
            share(AT[place]).wait_recv()

    def all_here():
        for place in (0b110, 0b111):
            for third in THIRDS:
                if place != firsts(third):
                    come(third, place)
            give(place)
        for place in (0b110, 0b111):
            share(AT[place]).wait_recv()

    eye = lax.broadcasted_iota(jnp.int32, (ROWS, ROWS), 0) == lax.broadcasted_iota(
        jnp.int32, (ROWS, ROWS), 1
    )

    def give_back(place):
        return copy(
            FLOWS["swap", 0] + place, dimg.at[img_rows(place, 1), :], swap.at[rows(place), :], other
        )

    def slot(kind, third, place):
        return ((place - 1) * 3 + third) * 2 + (kind == "dtxt")

    def sum_ref(kind, third, place):
        if kind == "dimg":
            return dimg.at[pl.ds(AT[place] * 2 * ROWS, ROWS), columns(third)]
        return dtxt.at[pl.ds(AT[place] * ROWS, ROWS), columns(third)]

    def values(kind, third, place):
        s = slot(kind, third, place)
        return copy(FLOWS[kind, third, place], sent.at[s], got.at[s], route(kind, third, place))

    def units(kind, third, place):
        s = slot(kind, third, place)
        return copy(
            FLOWS[kind + "_s", third, place], sent_s.at[s], got_s.at[s], route(kind, third, place)
        )

    def send(kind, third, place):
        for child in onward(third, place):
            add(kind, third, child)
        ref = sum_ref(kind, third, place)
        s = slot(kind, third, place)
        top = jnp.maximum(jnp.max(jnp.abs(ref[...]), axis=1, keepdims=True), 1e-30)
        across_lanes = jnp.sum(jnp.where(eye, top * (1.0 / 32767.0), 0.0), axis=0, keepdims=True)
        sent_s[s] = jnp.broadcast_to(across_lanes, (8, ROWS))
        sent[s] = ((ref[...] * (32767.0 / top) + 32768.5).astype(jnp.int32) - 32768).astype(jnp.int16)
        launch(lambda: values(kind, third, place))
        launch(lambda: units(kind, third, place))

    def take(kind, third, place):
        s = slot(kind, third, place)
        values(kind, third, place).wait_recv()
        units(kind, third, place).wait_recv()
        unit = jnp.sum(jnp.where(eye, got_s[s, 0:1, :], 0.0), axis=1, keepdims=True)
        return got[s].astype(jnp.int32).astype(F32) * unit

    def add(kind, third, place):
        sum_ref(kind, third, before(third, place))[...] += take(kind, third, place)

    def merge(place):
        give_back(AT[place]).wait_recv()
        dimg[img_rows(AT[place], 0), :] += swap[rows(AT[place]), :]

    def send_now(kind, place):
        for third in THIRDS:
            if not onward(third, place):
                send(kind, third, place)

    def pass_back(place):
        launch(lambda: give_back(place))

    def loss_send(axis, here, number):
        loss_got[number, here] = loss_tile[number]
        for stride in (1, 2, 3):
            launch(
                lambda stride=stride: copy(
                    FLOWS["loss", axis, stride], loss_tile.at[number], loss_got.at[number, here],
                    {axis: lax.rem(here + stride, 4)},
                )
            )

    def loss_take(axis, here, number):
        for stride in (1, 2, 3):
            source = lax.rem(here + 4 - stride, 4)
            copy(
                FLOWS["loss", axis, stride], loss_tile.at[number], loss_got.at[number, source],
                {axis: lax.rem(here + stride, 4)},
            ).wait_recv()
        loss_tile[number + 1] = (loss_got[number, 0] + loss_got[number, 1]) + (
            loss_got[number, 2] + loss_got[number, 3]
        )

    def loss_swap():
        return copy(FLOWS["loss_core"], loss_tile.at[0], loss_got.at[0, 0], other)

    def two_back(place):
        pass_back(place)
        pass_back(place - 1)

    def far_dimg():
        for place in (0b111, 0b110):
            merge(place)
            send_now("dimg", place)

    def far_dtxt():
        for place in (0b111, 0b110):
            send_now("dtxt", place)

    def near_dtxt():
        for axis in range(3):
            send_now("dtxt", 1 << axis)

    def partner_dimg():
        for place in (0b101, 0b011):
            merge(place)
            send_now("dimg", place)

    def far_back():
        two_back(7)
        near_dtxt()

    def partner_out():
        far_dtxt()
        partner_dimg()

    events = {
        0: pass_on,
        2: partners_here,
        5: all_here,
        10: far_back,
        11: lambda: two_back(5),
        12: far_dimg,
        13: partner_out,
    }

    def make(index, buffer):
        buffer[...] = make_coeff(*tile_at(index))

    def use(index, buffer):
        use_coeff(buffer[...], *tile_at(index))

    make(jnp.int32(0), even)

    def step(index, carry):
        for half, (new, old) in enumerate(((odd, even), (even, odd))):
            make(2 * index + 1 + half, new)
            use(2 * index + half, old)
            for moment, event in events.items():
                if moment % 2 == half:
                    pl.when(index == moment // 2)(event)
        return carry

    lax.fori_loop(0, 7, step, 0)
    make(jnp.int32(15), odd)
    launch(loss_swap)
    use(jnp.int32(14), even)
    two_back(3)
    loss_swap().wait_recv()
    loss_tile[1] = loss_tile[0] + loss_got[0, 0]
    loss_send("z", z, 1)
    use(jnp.int32(15), odd)
    two_back(1)

    send_now("dtxt", 0b101)
    send_now("dtxt", 0b011)
    loss_take("z", z, 1)
    loss_send("x", x, 2)
    for third in THIRDS:
        for kind in ("dimg", "dtxt"):
            send(kind, third, firsts(third))
    for axis in range(3):
        merge(1 << axis)
        send_now("dimg", 1 << axis)
    merge(0)
    loss_take("x", x, 2)
    loss_send("y", y, 3)
    for third in THIRDS:
        for kind in ("dtxt", "dimg"):
            send(kind, third, 1 << ORDER[third][1])
    for third in THIRDS:
        for kind in ("dtxt", "dimg"):
            send(kind, third, 1 << ORDER[third][0])
    for turn in (2, 1, 0):
        for third in THIRDS:
            for kind in ("dtxt", "dimg"):
                add(kind, third, 1 << ORDER[third][turn])
    loss_take("y", y, 3)
    count = F32(ROWS * 128)
    loss_out[0] = jnp.sum(loss_tile[4]) / (count * count)
    for kind, source, out in (("dtxt", txt_raw, txt_out), ("dimg", img_raw, img_out)):
        own = pl.ds(0, ROWS)
        grad = scale * (dimg if kind == "dimg" else dtxt)[own, :]
        unit, recip = normalize(source[...])
        out[...] = project_back(unit, recip, grad)

    for make in started:
        make().wait_send()


def per_device(images, texts, lang_order, position, logit_scale, logit_bias):
    rows, width = images.shape
    ids = lang_order.reshape(1, rows)
    whole = pl.BlockSpec(memory_space=pl.ANY)
    vmem = pl.BlockSpec(memory_space=pltpu.VMEM)
    smem = pl.BlockSpec(memory_space=pltpu.SMEM)
    return pl.pallas_call(
        kernel,
        out_shape=(
            jax.ShapeDtypeStruct((rows, width), F32),
            jax.ShapeDtypeStruct((rows, width), F32),
            jax.ShapeDtypeStruct((1,), F32),
        ),
        in_specs=[whole] * 5,
        out_specs=(vmem, vmem, smem),
        scratch_shapes=[
            pltpu.VMEM((rows, width), BF16),
            pltpu.VMEM((rows, width), BF16),
            pltpu.VMEM((1, rows), jnp.int32),
            pltpu.SMEM((1,), F32),
            pltpu.SMEM((1,), F32),
            pltpu.VMEM((16 * rows, width), BF16),
            pltpu.VMEM((8 * rows, width), BF16),
            pltpu.VMEM((8, 8, rows), jnp.int32),
            pltpu.VMEM((16 * rows, width), F32),
            pltpu.VMEM((8 * rows, width), F32),
            pltpu.VMEM((8 * rows, width), F32),
            pltpu.VMEM((4 * rows, 2 * rows), BF16),
            pltpu.VMEM((4 * rows, 2 * rows), BF16),
            pltpu.VMEM((42, rows, width // 3), jnp.int16),
            pltpu.VMEM((42, 8, rows), F32),
            pltpu.VMEM((42, rows, width // 3), jnp.int16),
            pltpu.VMEM((42, 8, rows), F32),
            pltpu.VMEM((5, 8, 128), F32),
            pltpu.VMEM((4, 4, 8, 128), F32),
            pltpu.SemaphoreType.DMA((5,)),
            pltpu.SemaphoreType.DMA((N_FLOW,)),
            pltpu.SemaphoreType.DMA((N_FLOW,)),
        ],
        compiler_params=pltpu.CompilerParams(
            collective_id=0, has_side_effects=True, vmem_limit_bytes=62 * 1024 * 1024
        ),
        name="pair_grads",
    )(images, texts, ids, logit_scale, logit_bias)


def solution(mesh):
    finer = Mesh(mesh.devices.reshape(4, 2, 4, 4), AXES)
    return jax.shard_map(
        per_device,
        mesh=finer,
        in_specs=(P(AXES, None), P(AXES, None), P(AXES), P(AXES), P(), P()),
        out_specs=(P(AXES, None), P(AXES, None), P()),
        check_vma=False,
    )
```

```python
import jax
import jax.numpy as jnp
from jax import lax
from jax.experimental import pallas as pl
from jax.experimental.pallas import tpu as pltpu
from jax.sharding import Mesh
from jax.sharding import PartitionSpec as P

AXES = ("x", "core", "y", "z")
MESH = pl.DeviceIdType.MESH
EPSILON = 1e-06
ROWS = 128
WIDTH = 1152
BF16 = jnp.bfloat16
F32 = jnp.float32

PLACES = (0b000, 0b001, 0b010, 0b100, 0b011, 0b101, 0b110, 0b111)
AT = {place: index for index, place in enumerate(PLACES)}
N_PLACE = len(PLACES)
THIRDS = (0, 1, 2)
ORDER = ((0, 1, 2), (1, 2, 0), (2, 0, 1))


def level(third, place):
    return max((n for n, axis in enumerate(ORDER[third]) if place >> axis & 1), default=-1)


def onward(third, place):
    return [place | 1 << axis for axis in ORDER[third][level(third, place) + 1 :]]


FLOWS = {}
for place in PLACES[1:]:
    for kind in ("img", "txt", "dimg", "dtxt"):
        for third in THIRDS:
            FLOWS[kind, third, place] = len(FLOWS)
for place in range(N_PLACE):
    FLOWS["share", place] = len(FLOWS)
for place in range(N_PLACE):
    FLOWS["swap", place] = len(FLOWS)
FLOWS["loss_core"] = len(FLOWS)
for axis in ("x", "y", "z"):
    for step in (1, 2, 3):
        FLOWS["loss", axis, step] = len(FLOWS)
N_FLOW = len(FLOWS)
SENT = ("img", "txt", "ids", "values", "units", "share", "swap", "loss_core", "loss")


def normalize(values):
    wide = values.astype(F32)
    recip = lax.rsqrt(jnp.sum(wide * wide, axis=1, keepdims=True) + EPSILON)
    return (wide * recip, recip)


def project_back(unit, recip, grad):
    return recip * (grad - unit * jnp.sum(unit * grad, axis=1, keepdims=True))


def tile_at(index):
    table = (
        (4, lambda k: 1 - k // 2, lambda k: 1 - k % 2),
        (6, lambda k: 2, lambda k: 1 - k),
        (7, lambda k: 2, lambda k: 2),
        (11, lambda k: 3, lambda k: 3 - k),
        (14, lambda k: 2 - k, lambda k: 3),
        (16, lambda k: 1 - k, lambda k: 2),
    )
    first = 0
    pair, group = jnp.int32(0), jnp.int32(0)
    for last, pair_of, group_of in table:
        inside = jnp.logical_and(index >= first, index < last)
        pair = jnp.where(inside, pair_of(index - first), pair)
        group = jnp.where(inside, group_of(index - first), group)
        first = last
    return pair, group


def kernel(
    img_in, txt_in, ids_in, scale_ref, bias_ref,
    img_out, txt_out, loss_out,
    img_raw, txt_raw, ids_raw, scale_raw, bias_raw,
    img, txt, ids, dimg, swap, dtxt, even, odd, sent, sent_s, got, got_s, loss_tile, loss_got,
    both, load_sem, send_sem, recv_sem,
):
    x, core = lax.axis_index("x"), lax.axis_index("core")
    y, z = lax.axis_index("y"), lax.axis_index("z")
    other = {"core": 1 - core}
    here = {"x": x, "y": y, "z": z}
    partner = {
        "img": [{axis: at + 1 - 2 * lax.rem(at, 2)} for axis, at in here.items()],
        "txt": [{axis: 3 - at} for axis, at in here.items()],
    }
    partner["dimg"] = partner["img"]
    partner["dtxt"] = partner["ids"] = partner["txt"]

    loads = [
        pltpu.make_async_copy(src, dst, load_sem.at[number])
        for number, (src, dst) in enumerate(
            (
                (img_in, img_raw), (txt_in, txt_raw), (ids_in, ids_raw),
                (scale_ref, scale_raw), (bias_ref, bias_raw),
            )
        )
    ]
    for load in loads:
        load.start()

    def copy(kind, flow, src, dst, device):
        return pltpu.make_async_remote_copy(
            src_ref=src, dst_ref=dst, send_sem=send_sem.at[SENT.index(kind)],
            recv_sem=recv_sem.at[flow], device_id=device, device_id_type=MESH,
        )

    def both_here(flow):
        copy("ids", flow, both, both, other).wait_recv()

    def launch(make):
        make().start()

    barrier = pltpu.get_barrier_semaphore()
    peers = [other]
    for axis, here in (("x", x), ("y", y), ("z", z)):
        for step in (1, 2, 3):
            peers.append({axis: lax.rem(here + step, 4)})
    for peer in peers:
        pl.semaphore_signal(barrier, inc=1, device_id=peer, device_id_type=MESH)

    def img_rows(place, which):
        return pl.ds((2 * place + which) * ROWS, ROWS)

    def rows(place):
        return pl.ds(place * ROWS, ROWS)

    for load in loads:
        load.wait()
    img[img_rows(0, 0), :] = normalize(img_raw[...])[0].astype(BF16)
    txt[rows(0), :] = normalize(txt_raw[...])[0].astype(BF16)
    ids[0] = jnp.broadcast_to(ids_raw[...], (8, ROWS)) + x * (16 * ROWS)
    scale = scale_raw[0]
    bias = bias_raw[0]
    pl.semaphore_wait(barrier, len(peers))

    def columns(third):
        return pl.ds(third * (WIDTH // 3), WIDTH // 3)

    def route(kind, third, place):
        return partner[kind][ORDER[third][level(third, place)]]

    def before(third, place):
        return place ^ 1 << ORDER[third][level(third, place)]

    def gather(kind, third, place):
        src, dst = AT[before(third, place)], AT[place]
        device = route(kind, third, place)
        if kind == "ids":
            return copy(kind, FLOWS["txt", 0, place], ids.at[src], ids.at[dst], device)
        ref, every = (img, 2) if kind == "img" else (txt, 1)
        return copy(
            kind,
            FLOWS[kind, third, place],
            ref.at[pl.ds(src * every * ROWS, ROWS), columns(third)],
            ref.at[pl.ds(dst * every * ROWS, ROWS), columns(third)],
            device,
        )

    def share(place):
        return copy(
            "share", FLOWS["share", place], img.at[img_rows(place, 0), :], img.at[img_rows(place, 1), :], other
        )

    def go(kind, third, place):
        launch(lambda: gather(kind, third, place))
        if kind == "txt" and third == 0:
            launch(lambda: gather("ids", third, place))

    def give(place):
        launch(lambda: share(AT[place]))

    def come(third, place):
        for kind in ("img", "txt"):
            if kind == "txt" and third == 0:
                both_here(FLOWS[kind, third, place])
            else:
                gather(kind, third, place).wait_recv()
            for later in onward(third, place):
                go(kind, third, later)

    tall = 4 * ROWS
    row_iota = lax.broadcasted_iota(jnp.int32, (tall, 1), 0)

    def span(number):
        return pl.ds(pl.multiple_of(number * (2 * ROWS), 2 * ROWS), 2 * ROWS)

    def tall_span(number):
        return pl.ds(pl.multiple_of(number * tall, tall), tall)

    def make_coeff(pair, group):
        logits = scale * lax.dot_general(
            img[tall_span(pair), :], txt[span(group), :], (((1,), (1,)), ((), ())),
            preferred_element_type=F32,
        ) + bias
        lower = row_iota < 2 * ROWS
        place_at = 2 * pair + jnp.where(lower, 0, 1)
        with_y = jnp.logical_or(place_at == AT[0b010], place_at == AT[0b110])
        with_z = jnp.logical_or(place_at == AT[0b100], place_at == AT[0b110])
        owner = (
            x * 16
            + jnp.where(with_y, partner["img"][1]["y"], y) * 4
            + jnp.where(with_z, partner["img"][2]["z"], z)
        ) * ROWS
        within = row_iota - jnp.where(lower, 0, 2 * ROWS)
        same_x = jnp.logical_or(place_at == 0, jnp.logical_or(with_y, with_z))
        valid = jnp.logical_and(same_x, within < ROWS)
        row_ids = jnp.where(valid, owner + within, -1)
        column_ids = jnp.concatenate(
            [ids[2 * group, 0:1, :], ids[2 * group + 1, 0:1, :]], axis=1
        )
        same = row_ids == column_ids
        logits = jnp.where(same, -logits, logits)
        power = jnp.exp(logits)
        one_plus = 1.0 + power
        recip = 1.0 / one_plus
        sigmoid = power * recip
        lost = (power - (one_plus - 1.0)) * recip
        half = tall // 2
        softplus = jnp.log(one_plus[:half] * one_plus[half:]) + (lost[:half] + lost[half:])
        folded = jnp.sum(softplus.reshape(32, 8, 256), axis=0)
        loss_tile[0] += folded[:, :128] + folded[:, 128:]
        return jnp.where(same, -sigmoid, sigmoid).astype(BF16)

    def use_coeff(half, pair, group):
        here, there = tall_span(pair), span(group)
        dimg[here, :] += jnp.dot(half, txt[there, :], preferred_element_type=F32)
        dtxt[there, :] += lax.dot_general(
            half, img[here, :], (((0,), (0,)), ((), ())), preferred_element_type=F32
        )

    for turn in range(3):
        for axis in range(3):
            for kind in ("img", "txt"):
                go(kind, (axis - turn) % 3, 1 << axis)
    give(0)
    dimg[...] = jnp.zeros_like(dimg)
    dtxt[...] = jnp.zeros_like(dtxt)
    loss_tile[0] = jnp.zeros_like(loss_tile[0])
    for turn in range(3):
        for axis in range(3):
            come((axis - turn) % 3, 1 << axis)
    for axis in range(3):
        give(1 << axis)
    for place in range(4):
        share(place).wait_recv()

    def firsts(third):
        return 1 << ORDER[third][0] | 1 << ORDER[third][1]

    def pass_on():
        for third in THIRDS:
            come(third, firsts(third))

    def partners_here():
        for place in (0b011, 0b101):
            for third in THIRDS:
                if place != firsts(third):
                    come(third, place)
            give(place)
        for place in (0b011, 0b101):
            share(AT[place]).wait_recv()

    def all_here():
        for place in (0b110, 0b111):
            for third in THIRDS:
                if place != firsts(third):
                    come(third, place)
            give(place)
        for place in (0b110, 0b111):
            share(AT[place]).wait_recv()

    eye = lax.broadcasted_iota(jnp.int32, (ROWS, ROWS), 0) == lax.broadcasted_iota(
        jnp.int32, (ROWS, ROWS), 1
    )

    def give_back(place):
        return copy(
            "swap", FLOWS["swap", 0] + place, dimg.at[img_rows(place, 1), :], swap.at[rows(place), :], other
        )

    def slot(kind, third, place):
        return ((place - 1) * 3 + third) * 2 + (kind == "dtxt")

    def sum_ref(kind, third, place):
        if kind == "dimg":
            return dimg.at[pl.ds(AT[place] * 2 * ROWS, ROWS), columns(third)]
        return dtxt.at[pl.ds(AT[place] * ROWS, ROWS), columns(third)]

    def values(kind, third, place):
        s = slot(kind, third, place)
        return copy(
            "values", FLOWS[kind, third, place], sent.at[s], got.at[s], route(kind, third, place)
        )

    def units(kind, third, place):
        s = slot(kind, third, place)
        return copy(
            "units", FLOWS[kind, third, place], sent_s.at[s], got_s.at[s], route(kind, third, place)
        )

    def send(kind, third, place):
        for child in onward(third, place):
            add(kind, third, child)
        ref = sum_ref(kind, third, place)
        s = slot(kind, third, place)
        top = jnp.maximum(jnp.max(jnp.abs(ref[...]), axis=1, keepdims=True), 1e-30)
        across_lanes = jnp.sum(jnp.where(eye, top * (1.0 / 32767.0), 0.0), axis=0, keepdims=True)
        sent_s[s] = jnp.broadcast_to(across_lanes, (8, ROWS))
        sent[s] = ((ref[...] * (32767.0 / top) + 32768.5).astype(jnp.int32) - 32768).astype(jnp.int16)
        launch(lambda: values(kind, third, place))
        launch(lambda: units(kind, third, place))

    def take(kind, third, place):
        s = slot(kind, third, place)
        both_here(FLOWS[kind, third, place])
        unit = jnp.sum(jnp.where(eye, got_s[s, 0:1, :], 0.0), axis=1, keepdims=True)
        return got[s].astype(jnp.int32).astype(F32) * unit

    def add(kind, third, place):
        sum_ref(kind, third, before(third, place))[...] += take(kind, third, place)

    def merge(place):
        give_back(AT[place]).wait_recv()
        dimg[img_rows(AT[place], 0), :] += swap[rows(AT[place]), :]

    def send_now(kind, place):
        for third in THIRDS:
            if not onward(third, place):
                send(kind, third, place)

    def pass_back(place):
        launch(lambda: give_back(place))

    def loss_send(axis, here, number):
        loss_got[number, here] = loss_tile[number]
        for stride in (1, 2, 3):
            launch(
                lambda stride=stride: copy(
                    "loss", FLOWS["loss", axis, stride], loss_tile.at[number], loss_got.at[number, here],
                    {axis: lax.rem(here + stride, 4)},
                )
            )

    def loss_take(axis, here, number):
        for stride in (1, 2, 3):
            source = lax.rem(here + 4 - stride, 4)
            copy(
                "loss", FLOWS["loss", axis, stride], loss_tile.at[number], loss_got.at[number, source],
                {axis: lax.rem(here + stride, 4)},
            ).wait_recv()
        loss_tile[number + 1] = (loss_got[number, 0] + loss_got[number, 1]) + (
            loss_got[number, 2] + loss_got[number, 3]
        )

    def loss_swap():
        return copy("loss_core", FLOWS["loss_core"], loss_tile.at[0], loss_got.at[0, 0], other)

    def two_back(place):
        pass_back(place)
        pass_back(place - 1)

    def far_dimg():
        for place in (0b111, 0b110):
            merge(place)
            send_now("dimg", place)

    def far_dtxt():
        for place in (0b111, 0b110):
            send_now("dtxt", place)

    def near_dtxt():
        for axis in range(3):
            send_now("dtxt", 1 << axis)

    def partner_dimg():
        for place in (0b101, 0b011):
            merge(place)
            send_now("dimg", place)

    def far_back():
        two_back(7)
        near_dtxt()

    def partner_out():
        far_dtxt()
        partner_dimg()

    events = {
        0: pass_on,
        2: partners_here,
        5: all_here,
        10: far_back,
        11: lambda: two_back(5),
        12: far_dimg,
        13: partner_out,
    }

    def make(index, buffer):
        buffer[...] = make_coeff(*tile_at(index))

    def use(index, buffer):
        use_coeff(buffer[...], *tile_at(index))

    make(jnp.int32(0), even)

    def step(index, carry):
        for half, (new, old) in enumerate(((odd, even), (even, odd))):
            make(2 * index + 1 + half, new)
            use(2 * index + half, old)
            for moment, event in events.items():
                if moment % 2 == half:
                    pl.when(index == moment // 2)(event)
        return carry

    lax.fori_loop(0, 7, step, 0)
    make(jnp.int32(15), odd)
    launch(loss_swap)
    use(jnp.int32(14), even)
    two_back(3)
    loss_swap().wait_recv()
    loss_tile[1] = loss_tile[0] + loss_got[0, 0]
    loss_send("z", z, 1)
    use(jnp.int32(15), odd)
    two_back(1)

    send_now("dtxt", 0b101)
    send_now("dtxt", 0b011)
    for third in THIRDS:
        for kind in ("dimg", "dtxt"):
            send(kind, third, firsts(third))
    loss_take("z", z, 1)
    loss_send("x", x, 2)
    for axis in range(3):
        merge(1 << axis)
        send_now("dimg", 1 << axis)
    merge(0)
    for third in THIRDS:
        for kind in ("dtxt", "dimg"):
            send(kind, third, 1 << ORDER[third][1])
    loss_take("x", x, 2)
    loss_send("y", y, 3)
    for third in THIRDS:
        for kind in ("dtxt", "dimg"):
            send(kind, third, 1 << ORDER[third][0])
    for turn in (2, 1, 0):
        for third in THIRDS:
            for kind in ("dtxt", "dimg"):
                add(kind, third, 1 << ORDER[third][turn])
    loss_take("y", y, 3)
    count = F32(ROWS * 128)
    loss_out[0] = jnp.sum(loss_tile[4]) / (count * count)
    for kind, source, out in (("dtxt", txt_raw, txt_out), ("dimg", img_raw, img_out)):
        own = pl.ds(0, ROWS)
        grad = scale * (dimg if kind == "dimg" else dtxt)[own, :]
        unit, recip = normalize(source[...])
        out[...] = project_back(unit, recip, grad)

    sevens = pl.ds(0, 7 * ROWS)
    for kind, every in (
        ("img", txt.at[sevens, :]), ("txt", txt.at[sevens, :]), ("ids", ids.at[pl.ds(0, 7)]),
        ("values", sent), ("units", sent_s), ("share", txt), ("swap", swap),
        ("loss_core", loss_tile.at[0]), ("loss", sent_s.at[pl.ds(0, 9)]),
    ):
        copy(kind, 0, every, every, other).wait_send()


def per_device(images, texts, lang_order, position, logit_scale, logit_bias):
    rows, width = images.shape
    ids = lang_order.reshape(1, rows)
    whole = pl.BlockSpec(memory_space=pl.ANY)
    vmem = pl.BlockSpec(memory_space=pltpu.VMEM)
    smem = pl.BlockSpec(memory_space=pltpu.SMEM)
    return pl.pallas_call(
        kernel,
        out_shape=(
            jax.ShapeDtypeStruct((rows, width), F32),
            jax.ShapeDtypeStruct((rows, width), F32),
            jax.ShapeDtypeStruct((1,), F32),
        ),
        in_specs=[whole] * 5,
        out_specs=(vmem, vmem, smem),
        scratch_shapes=[
            pltpu.VMEM((rows, width), BF16),
            pltpu.VMEM((rows, width), BF16),
            pltpu.VMEM((1, rows), jnp.int32),
            pltpu.SMEM((1,), F32),
            pltpu.SMEM((1,), F32),
            pltpu.VMEM((16 * rows, width), BF16),
            pltpu.VMEM((8 * rows, width), BF16),
            pltpu.VMEM((8, 8, rows), jnp.int32),
            pltpu.VMEM((16 * rows, width), F32),
            pltpu.VMEM((8 * rows, width), F32),
            pltpu.VMEM((8 * rows, width), F32),
            pltpu.VMEM((4 * rows, 2 * rows), BF16),
            pltpu.VMEM((4 * rows, 2 * rows), BF16),
            pltpu.VMEM((42, rows, width // 3), jnp.int16),
            pltpu.VMEM((42, 8, rows), F32),
            pltpu.VMEM((42, rows, width // 3), jnp.int16),
            pltpu.VMEM((42, 8, rows), F32),
            pltpu.VMEM((5, 8, 128), F32),
            pltpu.VMEM((4, 4, 8, 128), F32),
            pltpu.VMEM((200, 128), F32),
            pltpu.SemaphoreType.DMA((5,)),
            pltpu.SemaphoreType.DMA((len(SENT),)),
            pltpu.SemaphoreType.DMA((N_FLOW,)),
        ],
        compiler_params=pltpu.CompilerParams(
            collective_id=0, has_side_effects=True, vmem_limit_bytes=62 * 1024 * 1024
        ),
        name="pair_grads",
    )(images, texts, ids, logit_scale, logit_bias)


def solution(mesh):
    finer = Mesh(mesh.devices.reshape(4, 2, 4, 4), AXES)
    return jax.shard_map(
        per_device,
        mesh=finer,
        in_specs=(P(AXES, None), P(AXES, None), P(AXES), P(AXES), P(), P()),
        out_specs=(P(AXES, None), P(AXES, None), P()),
        check_vma=False,
    )
```

```python
import jax
import jax.numpy as jnp
from jax import lax
from jax.experimental import pallas as pl
from jax.experimental.pallas import tpu as pltpu
from jax.sharding import Mesh
from jax.sharding import PartitionSpec as P

AXES = ("x", "core", "y", "z")
MESH = pl.DeviceIdType.MESH
EPSILON = 1e-06
ROWS = 128
WIDTH = 1152
BF16 = jnp.bfloat16
F32 = jnp.float32

PLACES = (0b000, 0b001, 0b010, 0b100, 0b011, 0b101, 0b110, 0b111)
AT = {place: index for index, place in enumerate(PLACES)}
N_PLACE = len(PLACES)
THIRDS = (0, 1, 2)
ORDER = ((0, 1, 2), (1, 2, 0), (2, 0, 1))


def level(third, place):
    return max((n for n, axis in enumerate(ORDER[third]) if place >> axis & 1), default=-1)


def onward(third, place):
    return [place | 1 << axis for axis in ORDER[third][level(third, place) + 1 :]]


FLOWS = {}
for place in PLACES[1:]:
    for kind in ("img", "txt", "dimg", "dtxt"):
        for third in THIRDS:
            FLOWS[kind, third, place] = len(FLOWS)
for place in range(N_PLACE):
    FLOWS["share", place] = len(FLOWS)
for place in range(N_PLACE):
    FLOWS["swap", place] = len(FLOWS)
FLOWS["loss_core"] = len(FLOWS)
for axis in ("x", "y", "z"):
    for step in (1, 2, 3):
        FLOWS["loss", axis, step] = len(FLOWS)
N_FLOW = len(FLOWS)
SENT = ("img", "txt", "ids", "values", "units", "share", "swap", "loss_core", "loss")


def normalize(values):
    wide = values.astype(F32)
    recip = lax.rsqrt(jnp.sum(wide * wide, axis=1, keepdims=True) + EPSILON)
    return (wide * recip, recip)


def project_back(unit, recip, grad):
    return recip * (grad - unit * jnp.sum(unit * grad, axis=1, keepdims=True))


def tile_at(index):
    table = (
        (4, lambda k: 1 - k // 2, lambda k: 1 - k % 2),
        (6, lambda k: 2, lambda k: 1 - k),
        (7, lambda k: 2, lambda k: 2),
        (11, lambda k: 3, lambda k: 3 - k),
        (14, lambda k: 2 - k, lambda k: 3),
        (16, lambda k: 1 - k, lambda k: 2),
    )
    first = 0
    pair, group = jnp.int32(0), jnp.int32(0)
    for last, pair_of, group_of in table:
        inside = jnp.logical_and(index >= first, index < last)
        pair = jnp.where(inside, pair_of(index - first), pair)
        group = jnp.where(inside, group_of(index - first), group)
        first = last
    return pair, group


def kernel(
    img_in, txt_in, ids_in, scale_ref, bias_ref,
    img_out, txt_out, loss_out,
    img_raw, txt_raw, ids_raw, scale_raw, bias_raw,
    img, txt, ids, dimg, swap, dtxt, even, odd, spare, sent, sent_s, got, got_s, loss_tile, loss_got,
    both, load_sem, send_sem, recv_sem,
):
    x, core = lax.axis_index("x"), lax.axis_index("core")
    y, z = lax.axis_index("y"), lax.axis_index("z")
    other = {"core": 1 - core}
    here = {"x": x, "y": y, "z": z}
    partner = {
        "img": [{axis: at + 1 - 2 * lax.rem(at, 2)} for axis, at in here.items()],
        "txt": [{axis: 3 - at} for axis, at in here.items()],
    }
    partner["dimg"] = partner["img"]
    partner["dtxt"] = partner["ids"] = partner["txt"]

    loads = [
        pltpu.make_async_copy(src, dst, load_sem.at[number])
        for number, (src, dst) in enumerate(
            (
                (img_in, img_raw), (txt_in, txt_raw), (ids_in, ids_raw),
                (scale_ref, scale_raw), (bias_ref, bias_raw),
            )
        )
    ]
    for load in loads:
        load.start()

    def copy(kind, flow, src, dst, device):
        return pltpu.make_async_remote_copy(
            src_ref=src, dst_ref=dst, send_sem=send_sem.at[SENT.index(kind)],
            recv_sem=recv_sem.at[flow], device_id=device, device_id_type=MESH,
        )

    def both_here(flow):
        copy("ids", flow, both, both, other).wait_recv()

    def launch(make):
        make().start()

    barrier = pltpu.get_barrier_semaphore()
    peers = [other]
    for axis, here in (("x", x), ("y", y), ("z", z)):
        for step in (1, 2, 3):
            peers.append({axis: lax.rem(here + step, 4)})
    for peer in peers:
        pl.semaphore_signal(barrier, inc=1, device_id=peer, device_id_type=MESH)

    def img_rows(place, which):
        return pl.ds((2 * place + which) * ROWS, ROWS)

    def rows(place):
        return pl.ds(place * ROWS, ROWS)

    for load in loads:
        load.wait()
    img[img_rows(0, 0), :] = normalize(img_raw[...])[0].astype(BF16)
    txt[rows(0), :] = normalize(txt_raw[...])[0].astype(BF16)
    ids[0] = jnp.broadcast_to(ids_raw[...], (8, ROWS)) + x * (16 * ROWS)
    scale = scale_raw[0]
    bias = bias_raw[0]
    pl.semaphore_wait(barrier, len(peers))

    def columns(third):
        return pl.ds(third * (WIDTH // 3), WIDTH // 3)

    def route(kind, third, place):
        return partner[kind][ORDER[third][level(third, place)]]

    def before(third, place):
        return place ^ 1 << ORDER[third][level(third, place)]

    def gather(kind, third, place):
        src, dst = AT[before(third, place)], AT[place]
        device = route(kind, third, place)
        if kind == "ids":
            return copy(kind, FLOWS["txt", 0, place], ids.at[src], ids.at[dst], device)
        ref, every = (img, 2) if kind == "img" else (txt, 1)
        return copy(
            kind,
            FLOWS[kind, third, place],
            ref.at[pl.ds(src * every * ROWS, ROWS), columns(third)],
            ref.at[pl.ds(dst * every * ROWS, ROWS), columns(third)],
            device,
        )

    def share(place):
        return copy(
            "share", FLOWS["share", place], img.at[img_rows(place, 0), :], img.at[img_rows(place, 1), :], other
        )

    def go(kind, third, place):
        launch(lambda: gather(kind, third, place))
        if kind == "txt" and third == 0:
            launch(lambda: gather("ids", third, place))

    def give(place):
        launch(lambda: share(AT[place]))

    def come(third, place):
        for kind in ("img", "txt"):
            if kind == "txt" and third == 0:
                both_here(FLOWS[kind, third, place])
            else:
                gather(kind, third, place).wait_recv()
            for later in onward(third, place):
                go(kind, third, later)

    tall = 4 * ROWS
    row_iota = lax.broadcasted_iota(jnp.int32, (tall, 1), 0)

    def span(number):
        return pl.ds(pl.multiple_of(number * (2 * ROWS), 2 * ROWS), 2 * ROWS)

    def tall_span(number):
        return pl.ds(pl.multiple_of(number * tall, tall), tall)

    def make_coeff(pair, group):
        logits = scale * lax.dot_general(
            img[tall_span(pair), :], txt[span(group), :], (((1,), (1,)), ((), ())),
            preferred_element_type=F32,
        ) + bias
        lower = row_iota < 2 * ROWS
        place_at = 2 * pair + jnp.where(lower, 0, 1)
        with_y = jnp.logical_or(place_at == AT[0b010], place_at == AT[0b110])
        with_z = jnp.logical_or(place_at == AT[0b100], place_at == AT[0b110])
        owner = (
            x * 16
            + jnp.where(with_y, partner["img"][1]["y"], y) * 4
            + jnp.where(with_z, partner["img"][2]["z"], z)
        ) * ROWS
        within = row_iota - jnp.where(lower, 0, 2 * ROWS)
        same_x = jnp.logical_or(place_at == 0, jnp.logical_or(with_y, with_z))
        valid = jnp.logical_and(same_x, within < ROWS)
        row_ids = jnp.where(valid, owner + within, -1)
        column_ids = jnp.concatenate(
            [ids[2 * group, 0:1, :], ids[2 * group + 1, 0:1, :]], axis=1
        )
        same = row_ids == column_ids
        logits = jnp.where(same, -logits, logits)
        power = jnp.exp(logits)
        one_plus = 1.0 + power
        recip = 1.0 / one_plus
        sigmoid = power * recip
        lost = (power - (one_plus - 1.0)) * recip
        half = tall // 2
        softplus = jnp.log(one_plus[:half] * one_plus[half:]) + (lost[:half] + lost[half:])
        folded = jnp.sum(softplus.reshape(32, 8, 256), axis=0)
        loss_tile[0] += folded[:, :128] + folded[:, 128:]
        return jnp.where(same, -sigmoid, sigmoid).astype(BF16)

    def use_coeff(half, pair, group):
        here, there = tall_span(pair), span(group)
        dimg[here, :] += jnp.dot(half, txt[there, :], preferred_element_type=F32)
        dtxt[there, :] += lax.dot_general(
            half, img[here, :], (((0,), (0,)), ((), ())), preferred_element_type=F32
        )

    for turn in range(3):
        for axis in range(3):
            for kind in ("img", "txt"):
                go(kind, (axis - turn) % 3, 1 << axis)
    give(0)
    dimg[...] = jnp.zeros_like(dimg)
    dtxt[...] = jnp.zeros_like(dtxt)
    loss_tile[0] = jnp.zeros_like(loss_tile[0])
    for turn in range(3):
        for axis in range(3):
            come((axis - turn) % 3, 1 << axis)
    for axis in range(3):
        give(1 << axis)
    for place in range(4):
        share(place).wait_recv()

    def firsts(third):
        return 1 << ORDER[third][0] | 1 << ORDER[third][1]

    def pass_on():
        for third in THIRDS:
            come(third, firsts(third))

    def partners_here():
        for place in (0b011, 0b101):
            for third in THIRDS:
                if place != firsts(third):
                    come(third, place)
            give(place)
        for place in (0b011, 0b101):
            share(AT[place]).wait_recv()

    def all_here():
        for place in (0b110, 0b111):
            for third in THIRDS:
                if place != firsts(third):
                    come(third, place)
            give(place)
        for place in (0b110, 0b111):
            share(AT[place]).wait_recv()

    eye = lax.broadcasted_iota(jnp.int32, (ROWS, ROWS), 0) == lax.broadcasted_iota(
        jnp.int32, (ROWS, ROWS), 1
    )

    def give_back(place):
        return copy(
            "swap", FLOWS["swap", 0] + place, dimg.at[img_rows(place, 1), :], swap.at[rows(place), :], other
        )

    def slot(kind, third, place):
        return ((place - 1) * 3 + third) * 2 + (kind == "dtxt")

    def sum_ref(kind, third, place):
        if kind == "dimg":
            return dimg.at[pl.ds(AT[place] * 2 * ROWS, ROWS), columns(third)]
        return dtxt.at[pl.ds(AT[place] * ROWS, ROWS), columns(third)]

    def values(kind, third, place):
        s = slot(kind, third, place)
        return copy(
            "values", FLOWS[kind, third, place], sent.at[s], got.at[s], route(kind, third, place)
        )

    def units(kind, third, place):
        s = slot(kind, third, place)
        return copy(
            "units", FLOWS[kind, third, place], sent_s.at[s], got_s.at[s], route(kind, third, place)
        )

    def send(kind, third, place):
        for child in onward(third, place):
            add(kind, third, child)
        ref = sum_ref(kind, third, place)
        s = slot(kind, third, place)
        top = jnp.maximum(jnp.max(jnp.abs(ref[...]), axis=1, keepdims=True), 1e-30)
        across_lanes = jnp.sum(jnp.where(eye, top * (1.0 / 32767.0), 0.0), axis=0, keepdims=True)
        sent_s[s] = jnp.broadcast_to(across_lanes, (8, ROWS))
        sent[s] = ((ref[...] * (32767.0 / top) + 32768.5).astype(jnp.int32) - 32768).astype(jnp.int16)
        launch(lambda: values(kind, third, place))
        launch(lambda: units(kind, third, place))

    def take(kind, third, place):
        s = slot(kind, third, place)
        both_here(FLOWS[kind, third, place])
        unit = jnp.sum(jnp.where(eye, got_s[s, 0:1, :], 0.0), axis=1, keepdims=True)
        return got[s].astype(jnp.int32).astype(F32) * unit

    def add(kind, third, place):
        sum_ref(kind, third, before(third, place))[...] += take(kind, third, place)

    def merge(place):
        give_back(AT[place]).wait_recv()
        dimg[img_rows(AT[place], 0), :] += swap[rows(AT[place]), :]

    def send_now(kind, place):
        for third in THIRDS:
            if not onward(third, place):
                send(kind, third, place)

    def pass_back(place):
        launch(lambda: give_back(place))

    def loss_send(axis, here, number):
        loss_got[number, here] = loss_tile[number]
        for stride in (1, 2, 3):
            launch(
                lambda stride=stride: copy(
                    "loss", FLOWS["loss", axis, stride], loss_tile.at[number], loss_got.at[number, here],
                    {axis: lax.rem(here + stride, 4)},
                )
            )

    def loss_take(axis, here, number):
        for stride in (1, 2, 3):
            source = lax.rem(here + 4 - stride, 4)
            copy(
                "loss", FLOWS["loss", axis, stride], loss_tile.at[number], loss_got.at[number, source],
                {axis: lax.rem(here + stride, 4)},
            ).wait_recv()
        loss_tile[number + 1] = (loss_got[number, 0] + loss_got[number, 1]) + (
            loss_got[number, 2] + loss_got[number, 3]
        )

    def loss_swap():
        return copy("loss_core", FLOWS["loss_core"], loss_tile.at[0], loss_got.at[0, 0], other)

    def two_back(place):
        pass_back(place)
        pass_back(place - 1)

    def far_dimg():
        for place in (0b111, 0b110):
            merge(place)
            send_now("dimg", place)

    def far_dtxt():
        for place in (0b111, 0b110):
            send_now("dtxt", place)

    def near_dtxt():
        for axis in range(3):
            send_now("dtxt", 1 << axis)

    def partner_dimg():
        for place in (0b101, 0b011):
            merge(place)
            send_now("dimg", place)

    def far_back():
        two_back(7)
        near_dtxt()

    def partner_out():
        far_dtxt()
        partner_dimg()

    events = {
        0: pass_on,
        2: partners_here,
        5: all_here,
        10: far_back,
        11: lambda: two_back(5),
    }

    def make(index, buffer):
        buffer[...] = make_coeff(*tile_at(index))

    def use(index, buffer):
        use_coeff(buffer[...], *tile_at(index))

    make(jnp.int32(0), even)

    def step(index, carry):
        for half, (new, old) in enumerate(((odd, even), (even, odd))):
            make(2 * index + 1 + half, new)
            use(2 * index + half, old)
            for moment, event in events.items():
                if moment % 2 == half:
                    pl.when(index == moment // 2)(event)
        return carry

    lax.fori_loop(0, 6, step, 0)
    make(jnp.int32(13), odd)
    use(jnp.int32(12), even)
    far_dimg()
    make(jnp.int32(14), even)
    make(jnp.int32(15), spare)
    launch(loss_swap)
    use(jnp.int32(13), odd)
    loss_swap().wait_recv()
    loss_tile[1] = loss_tile[0] + loss_got[0, 0]
    loss_send("z", z, 1)
    partner_out()
    use(jnp.int32(14), even)
    two_back(3)
    loss_take("z", z, 1)
    loss_send("x", x, 2)
    use(jnp.int32(15), spare)
    two_back(1)

    send_now("dtxt", 0b101)
    send_now("dtxt", 0b011)
    for third in THIRDS:
        for kind in ("dimg", "dtxt"):
            send(kind, third, firsts(third))
    for axis in range(3):
        merge(1 << axis)
        send_now("dimg", 1 << axis)
    merge(0)
    loss_take("x", x, 2)
    loss_send("y", y, 3)
    for third in THIRDS:
        for kind in ("dtxt", "dimg"):
            send(kind, third, 1 << ORDER[third][1])
    for third in THIRDS:
        for kind in ("dtxt", "dimg"):
            send(kind, third, 1 << ORDER[third][0])
    for turn in (2, 1, 0):
        for third in THIRDS:
            for kind in ("dtxt", "dimg"):
                add(kind, third, 1 << ORDER[third][turn])
    loss_take("y", y, 3)
    count = F32(ROWS * 128)
    loss_out[0] = jnp.sum(loss_tile[4]) / (count * count)
    for kind, source, out in (("dtxt", txt_raw, txt_out), ("dimg", img_raw, img_out)):
        own = pl.ds(0, ROWS)
        grad = scale * (dimg if kind == "dimg" else dtxt)[own, :]
        unit, recip = normalize(source[...])
        out[...] = project_back(unit, recip, grad)

    sevens = pl.ds(0, 7 * ROWS)
    for kind, every in (
        ("img", txt.at[sevens, :]), ("txt", txt.at[sevens, :]), ("ids", ids.at[pl.ds(0, 7)]),
        ("values", sent), ("units", sent_s), ("share", txt), ("swap", swap),
        ("loss_core", loss_tile.at[0]), ("loss", sent_s.at[pl.ds(0, 9)]),
    ):
        copy(kind, 0, every, every, other).wait_send()


def per_device(images, texts, lang_order, position, logit_scale, logit_bias):
    rows, width = images.shape
    ids = lang_order.reshape(1, rows)
    whole = pl.BlockSpec(memory_space=pl.ANY)
    vmem = pl.BlockSpec(memory_space=pltpu.VMEM)
    smem = pl.BlockSpec(memory_space=pltpu.SMEM)
    return pl.pallas_call(
        kernel,
        out_shape=(
            jax.ShapeDtypeStruct((rows, width), F32),
            jax.ShapeDtypeStruct((rows, width), F32),
            jax.ShapeDtypeStruct((1,), F32),
        ),
        in_specs=[whole] * 5,
        out_specs=(vmem, vmem, smem),
        scratch_shapes=[
            pltpu.VMEM((rows, width), BF16),
            pltpu.VMEM((rows, width), BF16),
            pltpu.VMEM((1, rows), jnp.int32),
            pltpu.SMEM((1,), F32),
            pltpu.SMEM((1,), F32),
            pltpu.VMEM((16 * rows, width), BF16),
            pltpu.VMEM((8 * rows, width), BF16),
            pltpu.VMEM((8, 8, rows), jnp.int32),
            pltpu.VMEM((16 * rows, width), F32),
            pltpu.VMEM((8 * rows, width), F32),
            pltpu.VMEM((8 * rows, width), F32),
            pltpu.VMEM((4 * rows, 2 * rows), BF16),
            pltpu.VMEM((4 * rows, 2 * rows), BF16),
            pltpu.VMEM((4 * rows, 2 * rows), BF16),
            pltpu.VMEM((42, rows, width // 3), jnp.int16),
            pltpu.VMEM((42, 8, rows), F32),
            pltpu.VMEM((42, rows, width // 3), jnp.int16),
            pltpu.VMEM((42, 8, rows), F32),
            pltpu.VMEM((5, 8, 128), F32),
            pltpu.VMEM((4, 4, 8, 128), F32),
            pltpu.VMEM((200, 128), F32),
            pltpu.SemaphoreType.DMA((5,)),
            pltpu.SemaphoreType.DMA((len(SENT),)),
            pltpu.SemaphoreType.DMA((N_FLOW,)),
        ],
        compiler_params=pltpu.CompilerParams(
            collective_id=0, has_side_effects=True, vmem_limit_bytes=62 * 1024 * 1024
        ),
        name="pair_grads",
    )(images, texts, ids, logit_scale, logit_bias)


def solution(mesh):
    finer = Mesh(mesh.devices.reshape(4, 2, 4, 4), AXES)
    return jax.shard_map(
        per_device,
        mesh=finer,
        in_specs=(P(AXES, None), P(AXES, None), P(AXES), P(AXES), P(), P()),
        out_specs=(P(AXES, None), P(AXES, None), P()),
        check_vma=False,
    )
```

```python
import jax
import jax.numpy as jnp
from jax import lax
from jax.experimental import pallas as pl
from jax.experimental.pallas import tpu as pltpu
from jax.sharding import Mesh
from jax.sharding import PartitionSpec as P

AXES = ("x", "core", "y", "z")
MESH = pl.DeviceIdType.MESH
EPSILON = 1e-06
ROWS = 128
WIDTH = 1152
BF16 = jnp.bfloat16
F32 = jnp.float32

PLACES = (0b000, 0b001, 0b010, 0b100, 0b011, 0b101, 0b110, 0b111)
AT = {place: index for index, place in enumerate(PLACES)}
N_PLACE = len(PLACES)
THIRDS = (0, 1, 2)
ORDER = ((0, 1, 2), (1, 2, 0), (2, 0, 1))


def level(third, place):
    return max((n for n, axis in enumerate(ORDER[third]) if place >> axis & 1), default=-1)


def onward(third, place):
    return [place | 1 << axis for axis in ORDER[third][level(third, place) + 1 :]]


FLOWS = {}
for place in PLACES[1:]:
    for kind in ("img", "txt", "dimg", "dtxt"):
        for third in THIRDS:
            FLOWS[kind, third, place] = len(FLOWS)
for place in range(N_PLACE):
    FLOWS["share", place] = len(FLOWS)
for place in range(N_PLACE):
    FLOWS["swap", place] = len(FLOWS)
FLOWS["loss_core"] = len(FLOWS)
for axis in ("x", "y", "z"):
    for step in (1, 2, 3):
        FLOWS["loss", axis, step] = len(FLOWS)
N_FLOW = len(FLOWS)
SENT = ("img", "txt", "ids", "values", "units", "share", "swap", "loss_core", "loss")


def normalize(values):
    wide = values.astype(F32)
    recip = lax.rsqrt(jnp.sum(wide * wide, axis=1, keepdims=True) + EPSILON)
    return (wide * recip, recip)


def project_back(unit, recip, grad):
    return recip * (grad - unit * jnp.sum(unit * grad, axis=1, keepdims=True))


def tile_at(index):
    table = (
        (4, lambda k: 1 - k // 2, lambda k: 1 - k % 2),
        (6, lambda k: 2, lambda k: 1 - k),
        (7, lambda k: 2, lambda k: 2),
        (11, lambda k: 3, lambda k: 3 - k),
        (14, lambda k: 2 - k, lambda k: 3),
        (16, lambda k: 1 - k, lambda k: 2),
    )
    first = 0
    pair, group = jnp.int32(0), jnp.int32(0)
    for last, pair_of, group_of in table:
        inside = jnp.logical_and(index >= first, index < last)
        pair = jnp.where(inside, pair_of(index - first), pair)
        group = jnp.where(inside, group_of(index - first), group)
        first = last
    return pair, group


def kernel(
    img_in, txt_in, ids_in, scale_ref, bias_ref,
    img_out, txt_out, loss_out,
    img_raw, txt_raw, ids_raw, scale_raw, bias_raw,
    img, txt, ids, dimg, swap, dtxt, even, odd, sent, sent_s, got, got_s, loss_tile, loss_got,
    both, load_sem, send_sem, recv_sem,
):
    x, core = lax.axis_index("x"), lax.axis_index("core")
    y, z = lax.axis_index("y"), lax.axis_index("z")
    other = {"core": 1 - core}
    here = {"x": x, "y": y, "z": z}
    partner = {
        "img": [{axis: at + 1 - 2 * lax.rem(at, 2)} for axis, at in here.items()],
        "txt": [{axis: 3 - at} for axis, at in here.items()],
    }
    partner["dimg"] = partner["img"]
    partner["dtxt"] = partner["ids"] = partner["txt"]

    loads = [
        pltpu.make_async_copy(src, dst, load_sem.at[number])
        for number, (src, dst) in enumerate(
            (
                (img_in, img_raw), (txt_in, txt_raw), (ids_in, ids_raw),
                (scale_ref, scale_raw), (bias_ref, bias_raw),
            )
        )
    ]
    for load in loads:
        load.start()

    def copy(kind, flow, src, dst, device):
        return pltpu.make_async_remote_copy(
            src_ref=src, dst_ref=dst, send_sem=send_sem.at[SENT.index(kind)],
            recv_sem=recv_sem.at[flow], device_id=device, device_id_type=MESH,
        )

    def both_here(flow):
        copy("ids", flow, both, both, other).wait_recv()

    def launch(make):
        make().start()

    barrier = pltpu.get_barrier_semaphore()
    peers = [other]
    for axis, here in (("x", x), ("y", y), ("z", z)):
        for step in (1, 2, 3):
            peers.append({axis: lax.rem(here + step, 4)})
    for peer in peers:
        pl.semaphore_signal(barrier, inc=1, device_id=peer, device_id_type=MESH)

    def img_rows(place, which):
        return pl.ds((2 * place + which) * ROWS, ROWS)

    def rows(place):
        return pl.ds(place * ROWS, ROWS)

    for load in loads:
        load.wait()
    img[img_rows(0, 0), :] = normalize(img_raw[...])[0].astype(BF16)
    txt[rows(0), :] = normalize(txt_raw[...])[0].astype(BF16)
    ids[0] = jnp.broadcast_to(ids_raw[...], (8, ROWS)) + x * (16 * ROWS)
    scale = scale_raw[0]
    bias = bias_raw[0]
    pl.semaphore_wait(barrier, len(peers))

    def columns(third):
        return pl.ds(third * (WIDTH // 3), WIDTH // 3)

    def route(kind, third, place):
        return partner[kind][ORDER[third][level(third, place)]]

    def before(third, place):
        return place ^ 1 << ORDER[third][level(third, place)]

    def gather(kind, third, place):
        src, dst = AT[before(third, place)], AT[place]
        device = route(kind, third, place)
        if kind == "ids":
            return copy(kind, FLOWS["txt", 0, place], ids.at[src], ids.at[dst], device)
        ref, every = (img, 2) if kind == "img" else (txt, 1)
        return copy(
            kind,
            FLOWS[kind, third, place],
            ref.at[pl.ds(src * every * ROWS, ROWS), columns(third)],
            ref.at[pl.ds(dst * every * ROWS, ROWS), columns(third)],
            device,
        )

    def share(place):
        return copy(
            "share", FLOWS["share", place], img.at[img_rows(place, 0), :], img.at[img_rows(place, 1), :], other
        )

    def go(kind, third, place):
        launch(lambda: gather(kind, third, place))
        if kind == "txt" and third == 0:
            launch(lambda: gather("ids", third, place))

    def give(place):
        launch(lambda: share(AT[place]))

    def come(third, place):
        for kind in ("img", "txt"):
            if kind == "txt" and third == 0:
                both_here(FLOWS[kind, third, place])
            else:
                gather(kind, third, place).wait_recv()
            for later in onward(third, place):
                go(kind, third, later)

    tall = 4 * ROWS
    row_iota = lax.broadcasted_iota(jnp.int32, (tall, 1), 0)

    def span(number):
        return pl.ds(pl.multiple_of(number * (2 * ROWS), 2 * ROWS), 2 * ROWS)

    def tall_span(number):
        return pl.ds(pl.multiple_of(number * tall, tall), tall)

    def make_coeff(pair, group):
        logits = scale * lax.dot_general(
            img[tall_span(pair), :], txt[span(group), :], (((1,), (1,)), ((), ())),
            preferred_element_type=F32,
        ) + bias
        lower = row_iota < 2 * ROWS
        place_at = 2 * pair + jnp.where(lower, 0, 1)
        with_y = jnp.logical_or(place_at == AT[0b010], place_at == AT[0b110])
        with_z = jnp.logical_or(place_at == AT[0b100], place_at == AT[0b110])
        owner = (
            x * 16
            + jnp.where(with_y, partner["img"][1]["y"], y) * 4
            + jnp.where(with_z, partner["img"][2]["z"], z)
        ) * ROWS
        within = row_iota - jnp.where(lower, 0, 2 * ROWS)
        same_x = jnp.logical_or(place_at == 0, jnp.logical_or(with_y, with_z))
        valid = jnp.logical_and(same_x, within < ROWS)
        row_ids = jnp.where(valid, owner + within, -1)
        column_ids = jnp.concatenate(
            [ids[2 * group, 0:1, :], ids[2 * group + 1, 0:1, :]], axis=1
        )
        same = row_ids == column_ids
        logits = jnp.where(same, -logits, logits)
        power = jnp.exp(logits)
        one_plus = 1.0 + power
        recip = 1.0 / one_plus
        sigmoid = power * recip
        lost = (power - (one_plus - 1.0)) * recip
        half = tall // 2
        softplus = jnp.log(one_plus[:half] * one_plus[half:]) + (lost[:half] + lost[half:])
        folded = jnp.sum(softplus.reshape(32, 8, 256), axis=0)
        loss_tile[0] += folded[:, :128] + folded[:, 128:]
        return jnp.where(same, -sigmoid, sigmoid).astype(BF16)

    def use_coeff(half, pair, group):
        here, there = tall_span(pair), span(group)
        dimg[here, :] += jnp.dot(half, txt[there, :], preferred_element_type=F32)
        dtxt[there, :] += lax.dot_general(
            half, img[here, :], (((0,), (0,)), ((), ())), preferred_element_type=F32
        )

    for turn in range(3):
        for axis in range(3):
            for kind in ("img", "txt"):
                go(kind, (axis - turn) % 3, 1 << axis)
    give(0)
    dimg[...] = jnp.zeros_like(dimg)
    dtxt[...] = jnp.zeros_like(dtxt)
    loss_tile[0] = jnp.zeros_like(loss_tile[0])
    for turn in range(3):
        for axis in range(3):
            come((axis - turn) % 3, 1 << axis)
    for axis in range(3):
        give(1 << axis)
    for place in range(4):
        share(place).wait_recv()

    def firsts(third):
        return 1 << ORDER[third][0] | 1 << ORDER[third][1]

    def pass_on():
        for third in THIRDS:
            come(third, firsts(third))

    def partners_here():
        for place in (0b011, 0b101):
            for third in THIRDS:
                if place != firsts(third):
                    come(third, place)
            give(place)
        for place in (0b011, 0b101):
            share(AT[place]).wait_recv()

    def all_here():
        for place in (0b110, 0b111):
            for third in THIRDS:
                if place != firsts(third):
                    come(third, place)
            give(place)
        for place in (0b110, 0b111):
            share(AT[place]).wait_recv()

    eye = lax.broadcasted_iota(jnp.int32, (ROWS, ROWS), 0) == lax.broadcasted_iota(
        jnp.int32, (ROWS, ROWS), 1
    )

    def give_back(place):
        return copy(
            "swap", FLOWS["swap", 0] + place, dimg.at[img_rows(place, 1), :], swap.at[rows(place), :], other
        )

    def slot(kind, third, place):
        return ((place - 1) * 3 + third) * 2 + (kind == "dtxt")

    def sum_ref(kind, third, place):
        if kind == "dimg":
            return dimg.at[pl.ds(AT[place] * 2 * ROWS, ROWS), columns(third)]
        return dtxt.at[pl.ds(AT[place] * ROWS, ROWS), columns(third)]

    def values(kind, third, place):
        s = slot(kind, third, place)
        return copy(
            "values", FLOWS[kind, third, place], sent.at[s], got.at[s], route(kind, third, place)
        )

    def units(kind, third, place):
        s = slot(kind, third, place)
        return copy(
            "units", FLOWS[kind, third, place], sent_s.at[s], got_s.at[s], route(kind, third, place)
        )

    def send(kind, third, place):
        for child in onward(third, place):
            add(kind, third, child)
        ref = sum_ref(kind, third, place)
        s = slot(kind, third, place)
        top = jnp.maximum(jnp.max(jnp.abs(ref[...]), axis=1, keepdims=True), 1e-30)
        across_lanes = jnp.sum(jnp.where(eye, top * (1.0 / 32767.0), 0.0), axis=0, keepdims=True)
        sent_s[s] = jnp.broadcast_to(across_lanes, (8, ROWS))
        sent[s] = ((ref[...] * (32767.0 / top) + 32768.5).astype(jnp.int32) - 32768).astype(jnp.int16)
        launch(lambda: values(kind, third, place))
        launch(lambda: units(kind, third, place))

    def take(kind, third, place):
        s = slot(kind, third, place)
        both_here(FLOWS[kind, third, place])
        unit = jnp.sum(jnp.where(eye, got_s[s, 0:1, :], 0.0), axis=1, keepdims=True)
        return got[s].astype(jnp.int32).astype(F32) * unit

    def add(kind, third, place):
        sum_ref(kind, third, before(third, place))[...] += take(kind, third, place)

    def merge(place):
        give_back(AT[place]).wait_recv()
        dimg[img_rows(AT[place], 0), :] += swap[rows(AT[place]), :]

    def send_now(kind, place):
        for third in THIRDS:
            if not onward(third, place):
                send(kind, third, place)

    def pass_back(place):
        launch(lambda: give_back(place))

    def loss_send(axis, here, number):
        loss_got[number, here] = loss_tile[number]
        for stride in (1, 2, 3):
            launch(
                lambda stride=stride: copy(
                    "loss", FLOWS["loss", axis, stride], loss_tile.at[number], loss_got.at[number, here],
                    {axis: lax.rem(here + stride, 4)},
                )
            )

    def loss_take(axis, here, number):
        for stride in (1, 2, 3):
            source = lax.rem(here + 4 - stride, 4)
            copy(
                "loss", FLOWS["loss", axis, stride], loss_tile.at[number], loss_got.at[number, source],
                {axis: lax.rem(here + stride, 4)},
            ).wait_recv()
        loss_tile[number + 1] = (loss_got[number, 0] + loss_got[number, 1]) + (
            loss_got[number, 2] + loss_got[number, 3]
        )

    def loss_swap():
        return copy("loss_core", FLOWS["loss_core"], loss_tile.at[0], loss_got.at[0, 0], other)

    def two_back(place):
        pass_back(place)
        pass_back(place - 1)

    def far_dimg():
        for place in (0b111, 0b110):
            merge(place)
            send_now("dimg", place)

    def far_dtxt():
        for place in (0b111, 0b110):
            send_now("dtxt", place)

    def near_dtxt():
        for axis in range(3):
            send_now("dtxt", 1 << axis)

    def partner_dimg():
        for place in (0b101, 0b011):
            merge(place)
            send_now("dimg", place)

    def far_back():
        two_back(7)
        near_dtxt()

    def partner_out():
        far_dtxt()
        partner_dimg()

    events = {
        0: pass_on,
        2: partners_here,
        5: all_here,
        10: far_back,
        11: lambda: two_back(5),
        12: far_dimg,
        13: partner_out,
    }

    def make(index, buffer):
        buffer[...] = make_coeff(*tile_at(index))

    def use(index, buffer):
        use_coeff(buffer[...], *tile_at(index))

    make(jnp.int32(0), even)

    def step(index, carry):
        for half, (new, old) in enumerate(((odd, even), (even, odd))):
            make(2 * index + 1 + half, new)
            use(2 * index + half, old)
            for moment, event in events.items():
                if moment % 2 == half:
                    pl.when(index == moment // 2)(event)
        return carry

    lax.fori_loop(0, 7, step, 0)
    make(jnp.int32(15), odd)
    launch(loss_swap)
    use(jnp.int32(14), even)
    two_back(3)
    loss_swap().wait_recv()
    loss_tile[1] = loss_tile[0] + loss_got[0, 0]
    loss_send("z", z, 1)
    use(jnp.int32(15), odd)
    two_back(1)

    send_now("dtxt", 0b101)
    send_now("dtxt", 0b011)
    for third in THIRDS:
        for kind in ("dimg", "dtxt"):
            send(kind, third, firsts(third))
    loss_take("z", z, 1)
    loss_send("x", x, 2)
    for axis in range(3):
        merge(1 << axis)
        send_now("dimg", 1 << axis)
    merge(0)
    for third in THIRDS:
        for kind in ("dtxt", "dimg"):
            send(kind, third, 1 << ORDER[third][1])
    for third in THIRDS:
        for kind in ("dtxt", "dimg"):
            send(kind, third, 1 << ORDER[third][0])
    loss_take("x", x, 2)
    loss_send("y", y, 3)
    for turn in (2, 1, 0):
        for third in THIRDS:
            for kind in ("dtxt", "dimg"):
                add(kind, third, 1 << ORDER[third][turn])
    loss_take("y", y, 3)
    count = F32(ROWS * 128)
    loss_out[0] = jnp.sum(loss_tile[4]) / (count * count)
    for kind, source, out in (("dtxt", txt_raw, txt_out), ("dimg", img_raw, img_out)):
        own = pl.ds(0, ROWS)
        grad = scale * (dimg if kind == "dimg" else dtxt)[own, :]
        unit, recip = normalize(source[...])
        out[...] = project_back(unit, recip, grad)

    sevens = pl.ds(0, 7 * ROWS)
    for kind, every in (
        ("img", txt.at[sevens, :]), ("txt", txt.at[sevens, :]), ("ids", ids.at[pl.ds(0, 7)]),
        ("values", sent), ("units", sent_s), ("share", txt), ("swap", swap),
        ("loss_core", loss_tile.at[0]), ("loss", sent_s.at[pl.ds(0, 9)]),
    ):
        copy(kind, 0, every, every, other).wait_send()


def per_device(images, texts, lang_order, position, logit_scale, logit_bias):
    rows, width = images.shape
    ids = lang_order.reshape(1, rows)
    whole = pl.BlockSpec(memory_space=pl.ANY)
    vmem = pl.BlockSpec(memory_space=pltpu.VMEM)
    smem = pl.BlockSpec(memory_space=pltpu.SMEM)
    return pl.pallas_call(
        kernel,
        out_shape=(
            jax.ShapeDtypeStruct((rows, width), F32),
            jax.ShapeDtypeStruct((rows, width), F32),
            jax.ShapeDtypeStruct((1,), F32),
        ),
        in_specs=[whole] * 5,
        out_specs=(vmem, vmem, smem),
        scratch_shapes=[
            pltpu.VMEM((rows, width), BF16),
            pltpu.VMEM((rows, width), BF16),
            pltpu.VMEM((1, rows), jnp.int32),
            pltpu.SMEM((1,), F32),
            pltpu.SMEM((1,), F32),
            pltpu.VMEM((16 * rows, width), BF16),
            pltpu.VMEM((8 * rows, width), BF16),
            pltpu.VMEM((8, 8, rows), jnp.int32),
            pltpu.VMEM((16 * rows, width), F32),
            pltpu.VMEM((8 * rows, width), F32),
            pltpu.VMEM((8 * rows, width), F32),
            pltpu.VMEM((4 * rows, 2 * rows), BF16),
            pltpu.VMEM((4 * rows, 2 * rows), BF16),
            pltpu.VMEM((42, rows, width // 3), jnp.int16),
            pltpu.VMEM((42, 8, rows), F32),
            pltpu.VMEM((42, rows, width // 3), jnp.int16),
            pltpu.VMEM((42, 8, rows), F32),
            pltpu.VMEM((5, 8, 128), F32),
            pltpu.VMEM((4, 4, 8, 128), F32),
            pltpu.VMEM((200, 128), F32),
            pltpu.SemaphoreType.DMA((5,)),
            pltpu.SemaphoreType.DMA((len(SENT),)),
            pltpu.SemaphoreType.DMA((N_FLOW,)),
        ],
        compiler_params=pltpu.CompilerParams(
            collective_id=0, has_side_effects=True, vmem_limit_bytes=62 * 1024 * 1024
        ),
        name="pair_grads",
    )(images, texts, ids, logit_scale, logit_bias)


def solution(mesh):
    finer = Mesh(mesh.devices.reshape(4, 2, 4, 4), AXES)
    return jax.shard_map(
        per_device,
        mesh=finer,
        in_specs=(P(AXES, None), P(AXES, None), P(AXES), P(AXES), P(), P()),
        out_specs=(P(AXES, None), P(AXES, None), P()),
        check_vma=False,
    )
```

```python
import jax
import jax.numpy as jnp
from jax import lax
from jax.experimental import pallas as pl
from jax.experimental.pallas import tpu as pltpu
from jax.sharding import Mesh
from jax.sharding import PartitionSpec as P

AXES = ("x", "core", "y", "z")
MESH = pl.DeviceIdType.MESH
EPSILON = 1e-06
ROWS = 128
WIDTH = 1152
BF16 = jnp.bfloat16
F32 = jnp.float32

PLACES = (0b000, 0b001, 0b010, 0b100, 0b011, 0b101, 0b110, 0b111)
AT = {place: index for index, place in enumerate(PLACES)}
N_PLACE = len(PLACES)
THIRDS = (0, 1, 2)
ORDER = ((0, 1, 2), (1, 2, 0), (2, 0, 1))


def level(third, place):
    return max((n for n, axis in enumerate(ORDER[third]) if place >> axis & 1), default=-1)


def onward(third, place):
    return [place | 1 << axis for axis in ORDER[third][level(third, place) + 1 :]]


FLOWS = {}
for place in PLACES[1:]:
    for kind in ("img", "txt", "dimg", "dtxt"):
        for third in THIRDS:
            FLOWS[kind, third, place] = len(FLOWS)
for place in range(N_PLACE):
    FLOWS["share", place] = len(FLOWS)
for place in range(N_PLACE):
    FLOWS["swap", place] = len(FLOWS)
FLOWS["loss_core"] = len(FLOWS)
for axis in ("x", "y", "z"):
    for step in (1, 2, 3):
        FLOWS["loss", axis, step] = len(FLOWS)
N_FLOW = len(FLOWS)
SENT = ("img", "txt", "ids", "values", "units", "share", "swap", "loss_core", "loss")


def normalize(values):
    wide = values.astype(F32)
    recip = lax.rsqrt(jnp.sum(wide * wide, axis=1, keepdims=True) + EPSILON)
    return (wide * recip, recip)


def project_back(unit, recip, grad):
    return recip * (grad - unit * jnp.sum(unit * grad, axis=1, keepdims=True))


def tile_at(index):
    table = (
        (4, lambda k: 1 - k // 2, lambda k: 1 - k % 2),
        (6, lambda k: 2, lambda k: 1 - k),
        (7, lambda k: 2, lambda k: 2),
        (11, lambda k: 3, lambda k: 3 - k),
        (14, lambda k: 2 - k, lambda k: 3),
        (16, lambda k: 1 - k, lambda k: 2),
    )
    first = 0
    pair, group = jnp.int32(0), jnp.int32(0)
    for last, pair_of, group_of in table:
        inside = jnp.logical_and(index >= first, index < last)
        pair = jnp.where(inside, pair_of(index - first), pair)
        group = jnp.where(inside, group_of(index - first), group)
        first = last
    return pair, group


def kernel(
    img_in, txt_in, ids_in, scale_ref, bias_ref,
    img_out, txt_out, loss_out,
    img_raw, txt_raw, ids_raw, scale_raw, bias_raw,
    img, txt, ids, dimg, swap, dtxt, even, odd, sent, sent_s, got, got_s, loss_tile, loss_got,
    both, load_sem, send_sem, recv_sem,
):
    x, core = lax.axis_index("x"), lax.axis_index("core")
    y, z = lax.axis_index("y"), lax.axis_index("z")
    other = {"core": 1 - core}
    here = {"x": x, "y": y, "z": z}
    partner = {
        "img": [{axis: at + 1 - 2 * lax.rem(at, 2)} for axis, at in here.items()],
        "txt": [{axis: 3 - at} for axis, at in here.items()],
    }
    partner["dimg"] = partner["img"]
    partner["dtxt"] = partner["ids"] = partner["txt"]

    loads = [
        pltpu.make_async_copy(src, dst, load_sem.at[number])
        for number, (src, dst) in enumerate(
            (
                (img_in, img_raw), (txt_in, txt_raw), (ids_in, ids_raw),
                (scale_ref, scale_raw), (bias_ref, bias_raw),
            )
        )
    ]
    for load in loads:
        load.start()

    def copy(kind, flow, src, dst, device):
        return pltpu.make_async_remote_copy(
            src_ref=src, dst_ref=dst, send_sem=send_sem.at[SENT.index(kind)],
            recv_sem=recv_sem.at[flow], device_id=device, device_id_type=MESH,
        )

    def both_here(flow):
        copy("ids", flow, both, both, other).wait_recv()

    def launch(make):
        make().start()

    barrier = pltpu.get_barrier_semaphore()
    peers = [other]
    for axis, here in (("x", x), ("y", y), ("z", z)):
        for step in (1, 2, 3):
            peers.append({axis: lax.rem(here + step, 4)})
    for peer in peers:
        pl.semaphore_signal(barrier, inc=1, device_id=peer, device_id_type=MESH)

    def img_rows(place, which):
        return pl.ds((2 * place + which) * ROWS, ROWS)

    def rows(place):
        return pl.ds(place * ROWS, ROWS)

    for load in loads:
        load.wait()
    img[img_rows(0, 0), :] = normalize(img_raw[...])[0].astype(BF16)
    txt[rows(0), :] = normalize(txt_raw[...])[0].astype(BF16)
    ids[0] = jnp.broadcast_to(ids_raw[...], (8, ROWS)) + x * (16 * ROWS)
    scale = scale_raw[0]
    bias = bias_raw[0]
    pl.semaphore_wait(barrier, len(peers))

    def columns(third):
        return pl.ds(third * (WIDTH // 3), WIDTH // 3)

    def route(kind, third, place):
        return partner[kind][ORDER[third][level(third, place)]]

    def before(third, place):
        return place ^ 1 << ORDER[third][level(third, place)]

    def gather(kind, third, place):
        src, dst = AT[before(third, place)], AT[place]
        device = route(kind, third, place)
        if kind == "ids":
            return copy(kind, FLOWS["txt", 0, place], ids.at[src], ids.at[dst], device)
        ref, every = (img, 2) if kind == "img" else (txt, 1)
        return copy(
            kind,
            FLOWS[kind, third, place],
            ref.at[pl.ds(src * every * ROWS, ROWS), columns(third)],
            ref.at[pl.ds(dst * every * ROWS, ROWS), columns(third)],
            device,
        )

    def share(place):
        return copy(
            "share", FLOWS["share", place], img.at[img_rows(place, 0), :], img.at[img_rows(place, 1), :], other
        )

    def go(kind, third, place):
        launch(lambda: gather(kind, third, place))
        if kind == "txt" and third == 0:
            launch(lambda: gather("ids", third, place))

    def give(place):
        launch(lambda: share(AT[place]))

    def come(third, place):
        for kind in ("img", "txt"):
            if kind == "txt" and third == 0:
                both_here(FLOWS[kind, third, place])
            else:
                gather(kind, third, place).wait_recv()
            for later in onward(third, place):
                go(kind, third, later)

    tall = 4 * ROWS
    row_iota = lax.broadcasted_iota(jnp.int32, (tall, 1), 0)

    def span(number):
        return pl.ds(pl.multiple_of(number * (2 * ROWS), 2 * ROWS), 2 * ROWS)

    def tall_span(number):
        return pl.ds(pl.multiple_of(number * tall, tall), tall)

    def make_coeff(pair, group):
        logits = scale * lax.dot_general(
            img[tall_span(pair), :], txt[span(group), :], (((1,), (1,)), ((), ())),
            preferred_element_type=F32,
        ) + bias
        lower = row_iota < 2 * ROWS
        place_at = 2 * pair + jnp.where(lower, 0, 1)
        with_y = jnp.logical_or(place_at == AT[0b010], place_at == AT[0b110])
        with_z = jnp.logical_or(place_at == AT[0b100], place_at == AT[0b110])
        owner = (
            x * 16
            + jnp.where(with_y, partner["img"][1]["y"], y) * 4
            + jnp.where(with_z, partner["img"][2]["z"], z)
        ) * ROWS
        within = row_iota - jnp.where(lower, 0, 2 * ROWS)
        same_x = jnp.logical_or(place_at == 0, jnp.logical_or(with_y, with_z))
        valid = jnp.logical_and(same_x, within < ROWS)
        row_ids = jnp.where(valid, owner + within, -1)
        column_ids = jnp.concatenate(
            [ids[2 * group, 0:1, :], ids[2 * group + 1, 0:1, :]], axis=1
        )
        same = row_ids == column_ids
        logits = jnp.where(same, -logits, logits)
        power = jnp.exp(logits)
        one_plus = 1.0 + power
        recip = 1.0 / one_plus
        sigmoid = power * recip
        lost = (power - (one_plus - 1.0)) * recip
        half = tall // 2
        softplus = jnp.log(one_plus[:half] * one_plus[half:]) + (lost[:half] + lost[half:])
        folded = jnp.sum(softplus.reshape(32, 8, 256), axis=0)
        loss_tile[0] += folded[:, :128] + folded[:, 128:]
        return jnp.where(same, -sigmoid, sigmoid).astype(BF16)

    def use_coeff(half, pair, group):
        here, there = tall_span(pair), span(group)
        dimg[here, :] += jnp.dot(half, txt[there, :], preferred_element_type=F32)
        dtxt[there, :] += lax.dot_general(
            half, img[here, :], (((0,), (0,)), ((), ())), preferred_element_type=F32
        )

    for turn in range(3):
        for axis in range(3):
            for kind in ("img", "txt"):
                go(kind, (axis - turn) % 3, 1 << axis)
    give(0)
    dimg[...] = jnp.zeros_like(dimg)
    dtxt[...] = jnp.zeros_like(dtxt)
    loss_tile[0] = jnp.zeros_like(loss_tile[0])
    for turn in range(3):
        for axis in range(3):
            come((axis - turn) % 3, 1 << axis)
    for axis in range(3):
        give(1 << axis)
    for place in range(4):
        share(place).wait_recv()

    def firsts(third):
        return 1 << ORDER[third][0] | 1 << ORDER[third][1]

    def pass_on():
        for third in THIRDS:
            come(third, firsts(third))

    def partners_here():
        for place in (0b011, 0b101):
            for third in THIRDS:
                if place != firsts(third):
                    come(third, place)
            give(place)
        for place in (0b011, 0b101):
            share(AT[place]).wait_recv()

    def all_here():
        for place in (0b110, 0b111):
            for third in THIRDS:
                if place != firsts(third):
                    come(third, place)
            give(place)
        for place in (0b110, 0b111):
            share(AT[place]).wait_recv()

    eye = lax.broadcasted_iota(jnp.int32, (ROWS, ROWS), 0) == lax.broadcasted_iota(
        jnp.int32, (ROWS, ROWS), 1
    )

    def give_back(place):
        return copy(
            "swap", FLOWS["swap", 0] + place, dimg.at[img_rows(place, 1), :], swap.at[rows(place), :], other
        )

    def slot(kind, third, place):
        return ((place - 1) * 3 + third) * 2 + (kind == "dtxt")

    def sum_ref(kind, third, place):
        if kind == "dimg":
            return dimg.at[pl.ds(AT[place] * 2 * ROWS, ROWS), columns(third)]
        return dtxt.at[pl.ds(AT[place] * ROWS, ROWS), columns(third)]

    def values(kind, third, place):
        s = slot(kind, third, place)
        return copy(
            "values", FLOWS[kind, third, place], sent.at[s], got.at[s], route(kind, third, place)
        )

    def units(kind, third, place):
        s = slot(kind, third, place)
        return copy(
            "units", FLOWS[kind, third, place], sent_s.at[s], got_s.at[s], route(kind, third, place)
        )

    def send(kind, third, place):
        ref = sum_ref(kind, third, place)
        children = onward(third, place)
        if children:
            ref[...] += sum(take(kind, third, child) for child in children)
        s = slot(kind, third, place)
        top = jnp.maximum(jnp.max(jnp.abs(ref[...]), axis=1, keepdims=True), 1e-30)
        across_lanes = jnp.sum(jnp.where(eye, top * (1.0 / 32767.0), 0.0), axis=0, keepdims=True)
        sent_s[s] = jnp.broadcast_to(across_lanes, (8, ROWS))
        sent[s] = ((ref[...] * (32767.0 / top) + 32768.5).astype(jnp.int32) - 32768).astype(jnp.int16)
        launch(lambda: values(kind, third, place))
        launch(lambda: units(kind, third, place))

    def take(kind, third, place):
        s = slot(kind, third, place)
        both_here(FLOWS[kind, third, place])
        unit = jnp.sum(jnp.where(eye, got_s[s, 0:1, :], 0.0), axis=1, keepdims=True)
        return got[s].astype(jnp.int32).astype(F32) * unit

    def add(kind, third, place):
        sum_ref(kind, third, before(third, place))[...] += take(kind, third, place)

    def merge(place):
        give_back(AT[place]).wait_recv()
        dimg[img_rows(AT[place], 0), :] += swap[rows(AT[place]), :]

    def send_now(kind, place):
        for third in THIRDS:
            if not onward(third, place):
                send(kind, third, place)

    def pass_back(place):
        launch(lambda: give_back(place))

    def loss_send(axis, here, number):
        loss_got[number, here] = loss_tile[number]
        for stride in (1, 2, 3):
            launch(
                lambda stride=stride: copy(
                    "loss", FLOWS["loss", axis, stride], loss_tile.at[number], loss_got.at[number, here],
                    {axis: lax.rem(here + stride, 4)},
                )
            )

    def loss_take(axis, here, number):
        for stride in (1, 2, 3):
            source = lax.rem(here + 4 - stride, 4)
            copy(
                "loss", FLOWS["loss", axis, stride], loss_tile.at[number], loss_got.at[number, source],
                {axis: lax.rem(here + stride, 4)},
            ).wait_recv()
        loss_tile[number + 1] = (loss_got[number, 0] + loss_got[number, 1]) + (
            loss_got[number, 2] + loss_got[number, 3]
        )

    def loss_swap():
        return copy("loss_core", FLOWS["loss_core"], loss_tile.at[0], loss_got.at[0, 0], other)

    def two_back(place):
        pass_back(place)
        pass_back(place - 1)

    def far_dimg():
        for place in (0b111, 0b110):
            merge(place)
            send_now("dimg", place)

    def far_dtxt():
        for place in (0b111, 0b110):
            send_now("dtxt", place)

    def near_dtxt():
        for axis in range(3):
            send_now("dtxt", 1 << axis)

    def partner_dimg():
        for place in (0b101, 0b011):
            merge(place)
            send_now("dimg", place)

    def far_back():
        two_back(7)
        near_dtxt()

    def partner_out():
        far_dtxt()
        partner_dimg()

    events = {
        0: pass_on,
        2: partners_here,
        5: all_here,
        10: far_back,
        11: lambda: two_back(5),
        12: far_dimg,
        13: partner_out,
    }

    def make(index, buffer):
        buffer[...] = make_coeff(*tile_at(index))

    def use(index, buffer):
        use_coeff(buffer[...], *tile_at(index))

    make(jnp.int32(0), even)

    def step(index, carry):
        for half, (new, old) in enumerate(((odd, even), (even, odd))):
            make(2 * index + 1 + half, new)
            use(2 * index + half, old)
            for moment, event in events.items():
                if moment % 2 == half:
                    pl.when(index == moment // 2)(event)
        return carry

    lax.fori_loop(0, 7, step, 0)
    make(jnp.int32(15), odd)
    launch(loss_swap)
    use(jnp.int32(14), even)
    two_back(3)
    loss_swap().wait_recv()
    loss_tile[1] = loss_tile[0] + loss_got[0, 0]
    loss_send("z", z, 1)
    for third in THIRDS:
        send("dimg", third, firsts(third))
    use(jnp.int32(15), odd)
    two_back(1)

    send_now("dtxt", 0b101)
    send_now("dtxt", 0b011)
    for third in THIRDS:
        send("dtxt", third, firsts(third))
    loss_take("z", z, 1)
    loss_send("x", x, 2)
    for axis in range(3):
        merge(1 << axis)
        send_now("dimg", 1 << axis)
    merge(0)
    for third in THIRDS:
        for kind in ("dtxt", "dimg"):
            send(kind, third, 1 << ORDER[third][1])
    for third in THIRDS:
        for kind in ("dtxt", "dimg"):
            send(kind, third, 1 << ORDER[third][0])
    loss_take("x", x, 2)
    loss_send("y", y, 3)
    for turn in (2, 1, 0):
        for third in THIRDS:
            for kind in ("dtxt", "dimg"):
                add(kind, third, 1 << ORDER[third][turn])
    loss_take("y", y, 3)
    count = F32(ROWS * 128)
    loss_out[0] = jnp.sum(loss_tile[4]) / (count * count)
    for kind, source, out in (("dtxt", txt_raw, txt_out), ("dimg", img_raw, img_out)):
        own = pl.ds(0, ROWS)
        grad = scale * (dimg if kind == "dimg" else dtxt)[own, :]
        unit, recip = normalize(source[...])
        out[...] = project_back(unit, recip, grad)

    sevens = pl.ds(0, 7 * ROWS)
    for kind, every in (
        ("img", txt.at[sevens, :]), ("txt", txt.at[sevens, :]), ("ids", ids.at[pl.ds(0, 7)]),
        ("values", sent), ("units", sent_s), ("share", txt), ("swap", swap),
        ("loss_core", loss_tile.at[0]), ("loss", sent_s.at[pl.ds(0, 9)]),
    ):
        copy(kind, 0, every, every, other).wait_send()


def per_device(images, texts, lang_order, position, logit_scale, logit_bias):
    rows, width = images.shape
    ids = lang_order.reshape(1, rows)
    whole = pl.BlockSpec(memory_space=pl.ANY)
    vmem = pl.BlockSpec(memory_space=pltpu.VMEM)
    smem = pl.BlockSpec(memory_space=pltpu.SMEM)
    return pl.pallas_call(
        kernel,
        out_shape=(
            jax.ShapeDtypeStruct((rows, width), F32),
            jax.ShapeDtypeStruct((rows, width), F32),
            jax.ShapeDtypeStruct((1,), F32),
        ),
        in_specs=[whole] * 5,
        out_specs=(vmem, vmem, smem),
        scratch_shapes=[
            pltpu.VMEM((rows, width), BF16),
            pltpu.VMEM((rows, width), BF16),
            pltpu.VMEM((1, rows), jnp.int32),
            pltpu.SMEM((1,), F32),
            pltpu.SMEM((1,), F32),
            pltpu.VMEM((16 * rows, width), BF16),
            pltpu.VMEM((8 * rows, width), BF16),
            pltpu.VMEM((8, 8, rows), jnp.int32),
            pltpu.VMEM((16 * rows, width), F32),
            pltpu.VMEM((8 * rows, width), F32),
            pltpu.VMEM((8 * rows, width), F32),
            pltpu.VMEM((4 * rows, 2 * rows), BF16),
            pltpu.VMEM((4 * rows, 2 * rows), BF16),
            pltpu.VMEM((42, rows, width // 3), jnp.int16),
            pltpu.VMEM((42, 8, rows), F32),
            pltpu.VMEM((42, rows, width // 3), jnp.int16),
            pltpu.VMEM((42, 8, rows), F32),
            pltpu.VMEM((5, 8, 128), F32),
            pltpu.VMEM((4, 4, 8, 128), F32),
            pltpu.VMEM((200, 128), F32),
            pltpu.SemaphoreType.DMA((5,)),
            pltpu.SemaphoreType.DMA((len(SENT),)),
            pltpu.SemaphoreType.DMA((N_FLOW,)),
        ],
        compiler_params=pltpu.CompilerParams(
            collective_id=0, has_side_effects=True, vmem_limit_bytes=62 * 1024 * 1024
        ),
        name="pair_grads",
    )(images, texts, ids, logit_scale, logit_bias)


def solution(mesh):
    finer = Mesh(mesh.devices.reshape(4, 2, 4, 4), AXES)
    return jax.shard_map(
        per_device,
        mesh=finer,
        in_specs=(P(AXES, None), P(AXES, None), P(AXES), P(AXES), P(), P()),
        out_specs=(P(AXES, None), P(AXES, None), P()),
        check_vma=False,
    )
```
